128 devices in a mesh: dev: 128 (over z, x, y, core).
Axes of the slice: x: 4, y: 4, z: 4, core: 2. Of those that a mesh axis runs over, the one named last changes fastest.
Arguments:
- state: float32 [2, 4194304], P(None, 'dev'), as said below
- angles: float32 [22, 3], replicated, may hold values from -3.140625 to 3.140625
- sample_high: int32 [1048576, 1], P('dev'), may hold values from 0 to 127; in each aligned block of 8192 rows (0 to 8191, 8192 to 16383, ...) at most 256 rows name the same one
- sample_low: int32 [1048576], P('dev'), may hold values from 0 to 32767
- marginal_qubits: int32 [10], replicated, may hold values from 0 to 21, as said below
Outputs:
- sample_probs: float32 [1048576], P('dev')
- histogram: float32 [1024], P('dev')
- fidelity: float32 [], replicated
The draws below stay inside these ranges and needn't reach their ends.
Inputs may be any that keep to these rules, and one draw needn't show every extreme that they name: The state is unit noise times a product over qubits of factors between exp(-0.2) and exp(0.2). `marginal_qubits`: 10 different qubit numbers. `sample_high`: among the rows of one device no value occurs more than 256 times, and in some devices one value occurs exactly 256 times.
All inputs are finite; a program needn't handle non-finite values.
Results may differ from the reference program's by a relative error of at most 0.00075.
Values sent between devices are 32-bit elements.
A program may use at most 64 MiB of HBM per device.

```python
import math
import jax
import jax.numpy as jnp
import numpy as np

QUBITS = 22
AMPS_DEV = 32768
AMPS = 4194304
SAMP_DEV = 8192
SAMPLES = 1048576
OWNERS = 128
CAP = 256
MARG = 10
MARG_BINS = 1024


def draw_state(key, part):
    key_envelope = jax.random.fold_in(key, 11)
    key_noise = jax.random.fold_in(key, 12)
    factors = jax.random.uniform(key_envelope, (QUBITS,), jnp.float32, -0.15, 0.15)
    noise = jax.random.normal(key_noise, (2, AMPS), jnp.float32)
    index = jnp.arange(AMPS, dtype=jnp.int32)
    exponent = jnp.zeros((AMPS,), jnp.float32)
    for qubit in range(QUBITS):
        exponent = exponent + factors[qubit] * (index >> qubit & 1).astype(jnp.float32)
    return noise * jnp.exp(exponent)[None, :]


def draw_marginal_qubits(key, part):
    return jax.random.permutation(jax.random.fold_in(key, 21), QUBITS)[:MARG].astype(jnp.int32)


def set_ends(values, rng, least, top_value):
    spot = [jax.random.randint(jax.random.fold_in(rng, axis), (), 0, length) for axis, length in enumerate(values.shape)]
    widest = values.shape.index(max(values.shape))
    neighbour = spot[:widest] + [(spot[widest] + 1) % values.shape[widest]] + spot[widest + 1:]
    return values.at[tuple(spot)].set(least).at[tuple(neighbour)].set(top_value)


def rank_bounds(amount, lean):
    loads = [(1 << 20) // math.isqrt(standing ** lean) + 1 for standing in range(1, amount + 1)]
    deviation = 1 + sum(loads) // (1 << 30)
    return np.cumsum(np.array([max(1, weight // deviation) for weight in loads]))


def ranked_ids(stream_key, shape, number_of, skew):
    grid = rank_bounds(number_of, skew)
    pick = jax.random.randint(jax.random.fold_in(stream_key, 1), shape, 0, int(grid[number_of - 1]))
    standing = jnp.searchsorted(jnp.asarray(grid, jnp.int32), pick, side="right")
    return jax.random.permutation(jax.random.fold_in(stream_key, 2), number_of)[standing].astype(jnp.int32)


def assign_block(stream_key, own, number, rows, count, top, bound, skew):
    ranking = jax.random.permutation(stream_key, count)
    heavy_load, ordinary = portions_of(count, rows * top, bound, skew, True), portions_of(count, rows * top, bound, skew, False)
    places = jnp.arange(count)

    def named(lengths, offset_by):
        used = int((lengths > 0).sum())
        fixed = max(1, used // 4)
        passed = fixed + (places - fixed + offset_by * (used - fixed)) % max(1, count - fixed)
        return jnp.zeros((count,), jnp.int32).at[ranking[jnp.where(places < fixed, places, passed)]].set(jnp.asarray(lengths, jnp.int32))

    lengths = jnp.where(number % 4 == 0, named(heavy_load, number // 4), named(ordinary, number - number // 4 - 1))
    mixed = jax.random.permutation(jax.random.fold_in(own, 3), count)
    source_of, taker = mixed[0:count // 2 * 2:2], mixed[1:count // 2 * 2:2]
    margin = jnp.minimum(lengths[source_of] - 1, bound - lengths[taker]) // 2
    margin = jnp.where((source_of == ranking[0]) | (taker == ranking[0]) | (lengths[taker] == 0), 0, jnp.maximum(margin, 0))
    passed = jax.random.randint(jax.random.fold_in(own, 4), (count // 2,), 0, 1 << 20) % (margin + 1)
    lengths = lengths.at[source_of].add(-passed).at[taker].add(passed)
    items = jnp.searchsorted(jnp.cumsum(lengths), jnp.arange(rows * top), side="right").astype(jnp.int32)
    grid = items.reshape(top, rows).T
    grid = grid[jax.random.permutation(jax.random.fold_in(own, 1), rows)]
    offset_by = jax.random.randint(jax.random.fold_in(own, 2), (rows, 1), 0, top)
    return jnp.take_along_axis(grid, (jnp.arange(top)[None, :] + offset_by) % top, axis=1)


def portions_of(count, total, bound, skew, full):
    loads = [(1 << 20) // math.isqrt(grade ** skew) + 1 for grade in range(1, count + 1)]
    largest = bound if full else min(bound, max(-(-total // count), total * loads[0] // sum(loads)))
    least = 1 if total - largest >= count - 1 else 0
    counts, spare = [largest] + [least] * (count - 1), total - largest - least * (count - 1)
    while spare > 0:
        candidates = [i for i in range(1, count) if counts[i] < largest] or [i for i in range(1, count) if counts[i] < bound]
        whole, left = sum([loads[i] for i in candidates]), spare
        for i in candidates:
            more = min(bound - counts[i], max(1, left * loads[i] // whole), spare)
            counts[i] = counts[i] + more
            spare = spare - more
    return np.array(counts)


def setup_inputs(seed: int = 0) -> dict:
    keys = jax.random.split(jax.random.key(seed), 6)
    state = draw_state(jax.random.fold_in(keys[5], 71), 0)
    angles = jnp.clip(jax.random.uniform(keys[1], (QUBITS, 3), jnp.float32, -3.140625, 3.140625), -3.140625, 3.140625)
    sample_high_keys = jax.random.split(jax.random.fold_in(keys[2], 1), SAMPLES // SAMP_DEV)
    sample_high_turns = jax.random.permutation(jax.random.fold_in(keys[2], 3), SAMPLES // SAMP_DEV)
    sample_high = jax.vmap(lambda own, number: assign_block(jax.random.fold_in(keys[2], 2), own, number, SAMP_DEV, OWNERS, 1, CAP, 2))(sample_high_keys, sample_high_turns).reshape((SAMPLES, 1))
    sample_low = set_ends(ranked_ids(keys[3], (SAMPLES,), AMPS_DEV, 2), jax.random.fold_in(keys[3], 3), 0, AMPS_DEV - 1).astype(jnp.int32)
    marginal_qubits = draw_marginal_qubits(jax.random.fold_in(keys[5], 71), 0)
    return {"state": state, "angles": angles, "sample_high": sample_high, "sample_low": sample_low, "marginal_qubits": marginal_qubits}


def gate_parts(angles):
    theta = angles[:, 0]
    first = angles[:, 1]
    second = angles[:, 2]
    cosine = jnp.cos(theta)
    sine = jnp.sin(theta)
    zeros = jnp.zeros_like(cosine)
    real_part = jnp.stack([jnp.stack([cosine, -jnp.cos(second) * sine], -1),
                           jnp.stack([jnp.cos(first) * sine, jnp.cos(first + second) * cosine], -1)], -2)
    imag_part = jnp.stack([jnp.stack([zeros, -jnp.sin(second) * sine], -1),
                           jnp.stack([jnp.sin(first) * sine, jnp.sin(first + second) * cosine], -1)], -2)
    return real_part, imag_part


def reference(state, angles, sample_high, sample_low, marginal_qubits):
    gate_real, gate_imag = gate_parts(angles)
    real_part = state[0]
    imag_part = state[1]
    for qubit in range(QUBITS):
        shape = (AMPS // (2 * 2 ** qubit), 2, 2 ** qubit)
        field_real = real_part.reshape(shape)
        field_imag = imag_part.reshape(shape)
        zero_real, zero_imag = field_real[:, 0], field_imag[:, 0]
        one_real, one_imag = field_real[:, 1], field_imag[:, 1]
        outputs_real = []
        outputs_imag = []
        for row in range(2):
            ar, ai = gate_real[qubit, row, 0], gate_imag[qubit, row, 0]
            br, bi = gate_real[qubit, row, 1], gate_imag[qubit, row, 1]
            outputs_real.append(ar * zero_real - ai * zero_imag + br * one_real - bi * one_imag)
            outputs_imag.append(ar * zero_imag + ai * zero_real + br * one_imag + bi * one_real)
        real_part = jnp.stack(outputs_real, 1).reshape(AMPS)
        imag_part = jnp.stack(outputs_imag, 1).reshape(AMPS)
    weight = real_part * real_part + imag_part * imag_part
    norm = jnp.sum(weight)
    bitstring = sample_high[:, 0] * AMPS_DEV + sample_low
    sample_probs = AMPS * (jnp.take(weight, bitstring) / norm)
    fidelity = jnp.mean(sample_probs) - 1.0
    index = jnp.arange(AMPS, dtype=jnp.int32)
    bins = jnp.zeros((AMPS,), jnp.int32)
    for place in range(MARG):
        bins = bins + (((index >> marginal_qubits[place]) & 1) << place)
    totals = jax.ops.segment_sum(weight, bins, num_segments=MARG_BINS)
    histogram = MARG_BINS * (totals / norm)
    return sample_probs, histogram, fidelity
```

```python
import functools

import jax
import jax.numpy as jnp
from jax import lax
from jax.experimental import pallas as pl
from jax.experimental.pallas import tpu as pltpu
from jax.sharding import PartitionSpec as P

LANES = 128
SUBLANES = 8
f32 = jnp.float32
bf16 = jnp.bfloat16
i32 = jnp.int32


def iota(shape, dim):
    return lax.broadcasted_iota(i32, shape, dim)


def gate_rows(angles, qubits):
    sub = iota((SUBLANES, LANES), 0)

    def column(j):
        blocks = []
        for first in range(0, qubits, SUBLANES):
            block = jnp.zeros((SUBLANES, LANES), f32)
            for q in range(first, min(first + SUBLANES, qubits)):
                block = jnp.where(sub == q - first, angles[j, q], block)
            blocks.append(block)
        return jnp.concatenate(blocks, axis=0)

    theta, first, second = column(0), column(1), column(2)
    cosine, sine = jnp.cos(theta), jnp.sin(theta)
    joint = first + second
    return [
        cosine,
        jnp.zeros_like(cosine),
        -jnp.cos(second) * sine,
        -jnp.sin(second) * sine,
        jnp.cos(first) * sine,
        jnp.sin(first) * sine,
        jnp.cos(joint) * cosine,
        jnp.sin(joint) * cosine,
    ]


def leading_gate(xr, xi, bit, u):
    n, s, lanes = xr.shape
    shape = (n >> (bit + 1), 2, 1 << bit, s, lanes)
    xr, xi = xr.reshape(shape), xi.reshape(shape)
    ar, ai, br, bi = xr[:, 0], xi[:, 0], xr[:, 1], xi[:, 1]
    outs_r, outs_i = [], []
    for row in range(2):
        pr, pi, qr, qi = u[4 * row : 4 * row + 4]
        outs_r.append(pr * ar - pi * ai + (qr * br - qi * bi))
        outs_i.append(pr * ai + pi * ar + (qr * bi + qi * br))
    return (
        jnp.stack(outs_r, 1).reshape(n, s, lanes),
        jnp.stack(outs_i, 1).reshape(n, s, lanes),
    )


def sublane_gate(xr, xi, bit, u):
    step = 1 << bit
    high = ((iota((SUBLANES, LANES), 0) >> bit) & 1) == 1

    def swap(x):
        down = pltpu.roll(x, step, 1)
        if 2 * step == SUBLANES:
            return down
        return jnp.where(high[None], down, pltpu.roll(x, SUBLANES - step, 1))

    keep_r = jnp.where(high, u[6], u[0])[None]
    keep_i = jnp.where(high, u[7], u[1])[None]
    cross_r = jnp.where(high, u[4], u[2])[None]
    cross_i = jnp.where(high, u[5], u[3])[None]
    yr, yi = swap(xr), swap(xi)
    return (
        keep_r * xr - keep_i * xi + (cross_r * yr - cross_i * yi),
        keep_r * xi + keep_i * xr + (cross_r * yi + cross_i * yr),
    )


def lane_matrix(units):
    shape = (LANES, LANES)
    row, col = iota(shape, 0), iota(shape, 1)
    mr = mi = None
    for bit, u in enumerate(units):
        rb, cb = ((row >> bit) & 1) == 1, ((col >> bit) & 1) == 1
        gr = jnp.where(cb, jnp.where(rb, u[6], u[4]), jnp.where(rb, u[2], u[0]))
        gi = jnp.where(cb, jnp.where(rb, u[7], u[5]), jnp.where(rb, u[3], u[1]))
        if mr is None:
            mr, mi = gr, gi
        else:
            mr, mi = mr * gr - mi * gi, mr * gi + mi * gr
    return mr, mi


def row_matrix(units):
    shape = (LANES, LANES)
    row, col = iota(shape, 0), iota(shape, 1)
    mr = mi = None
    for bit, u in enumerate(units):
        rb, cb = ((row >> bit) & 1) == 1, ((col >> bit) & 1) == 1
        gr = jnp.where(rb, jnp.where(cb, u[6], u[4]), jnp.where(cb, u[2], u[0]))
        gi = jnp.where(rb, jnp.where(cb, u[7], u[5]), jnp.where(cb, u[3], u[1]))
        if mr is None:
            mr, mi = gr, gi
        else:
            mr, mi = mr * gr - mi * gi, mr * gi + mi * gr
    return mr, mi


def cut(x, depth):
    rows = x.shape[0]
    x = x.reshape(rows // SUBLANES, SUBLANES, LANES)
    per = SUBLANES // depth
    if per == 1:
        return x
    parts = [x[:, k * depth : (k + 1) * depth] for k in range(per)]
    return jnp.stack(parts, 1).reshape(rows // depth, depth, LANES)


def join(x):
    n, depth, _ = x.shape
    per = SUBLANES // depth
    if per > 1:
        x = x.reshape(n // per, per, depth, LANES)
        x = jnp.concatenate([x[:, k] for k in range(per)], axis=1)
    return x.reshape(n * depth, LANES)


def halves(x):
    top = x.astype(bf16)
    return top, (x - top.astype(f32)).astype(bf16)


def one_hot(row, count):
    wide = jnp.broadcast_to(row.astype(f32), (16, LANES)).astype(bf16)
    ids = iota((count, LANES), 0).astype(f32).astype(bf16).reshape(count // 16, 16, LANES)
    hot = jnp.where(ids == wide[None], jnp.ones((), bf16), jnp.zeros((), bf16))
    return hot.reshape(count, LANES)


def split_table(table):
    flipped = table.T
    top, rest = halves(flipped)
    return jnp.concatenate([top, rest], axis=0)


def lookup(table, upper, lower):
    rows = upper.shape[0]
    count = table.shape[1]
    hot = jnp.concatenate([one_hot(upper[r : r + 1], count) for r in range(rows)], axis=1)
    both = jnp.dot(table, hot, preferred_element_type=f32)
    sub = iota((SUBLANES, LANES), 0)
    found = []
    for r in range(rows):
        part = slice(r * LANES, (r + 1) * LANES)
        value = (both[:LANES, part] + both[LANES:, part]).reshape(LANES // SUBLANES, SUBLANES, LANES)
        low = jnp.broadcast_to(lower[r : r + 1], (SUBLANES, LANES))
        for bit in (6, 5, 4, 3):
            half = value.shape[0] // 2
            value = jnp.where((((low >> bit) & 1) == 1)[None], value[half:], value[:half])
        value = jnp.where(sub == (low & (SUBLANES - 1)), value[0], 0.0)
        found.append(jnp.sum(value, axis=0, keepdims=True))
    return jnp.concatenate(found, axis=0)


def kernel(
    sizes,
    angles,
    marg,
    state,
    owner_ref,
    low_ref,
    probs_ref,
    hist_ref,
    fid_ref,
    amp_out,
    amp_in,
    wt_out,
    wt_in,
    ans_out,
    ans_in,
    his_out,
    his_in,
    tot_out,
    tot_in,
    code_ref,
    rank_ref,
    req_ref,
    table_ref,
    global_ref,
    gates,
    sends,
    recvs,
):
    devices, depth, capacity_rows, marg_count = sizes
    me = lax.axis_index("dev")
    global_bits = devices.bit_length() - 1
    rows = state.shape[0] // 2
    row_bits = rows.bit_length() - 1
    local_bits = row_bits + 7
    codes = devices * capacity_rows

    def peer(k):
        return lax.rem(me + k, devices)

    def copy(channel, src, dst, target):
        return pltpu.make_async_remote_copy(
            src_ref=src,
            dst_ref=dst,
            send_sem=sends.at[channel],
            recv_sem=recvs.at[channel],
            device_id=(target,),
            device_id_type=pl.DeviceIdType.MESH,
        )

    def scatter(channel, out, into):
        @pl.loop(1, devices)
        def _(k):
            target = peer(k)
            copy(channel, out.at[target], into.at[me], target).start()

        into[me] = out[me]

    def spread(channel, out, into):
        @pl.loop(1, devices)
        def _(k):
            copy(channel, out.at[0], into.at[me], peer(k)).start()

        into[me] = out[0]

    def all_of(channel, into):
        many = into.at[pl.ds(0, devices - 1)]
        return copy(channel, many, many, peer(1))

    barrier = pltpu.get_barrier_semaphore()

    @pl.loop(1, devices)
    def _(k):
        pl.semaphore_signal(
            barrier, inc=1, device_id=(peer(k),), device_id_type=pl.DeviceIdType.MESH
        )

    for e, entry in enumerate(gate_rows(angles, global_bits + local_bits)):
        gates[e] = entry

    def unit(qubit):
        return [gates[e, qubit : qubit + 1] for e in range(8)]

    mr, mi = lane_matrix([unit(q) for q in range(7)])
    mixed = jnp.concatenate(
        [jnp.concatenate([mr, mi], axis=1), jnp.concatenate([-mi, mr], axis=1)], axis=0
    )
    both = jnp.concatenate(
        [state[pl.ds(0, rows, stride=2)], state[pl.ds(1, rows, stride=2)]], axis=1
    )
    both = jnp.dot(both, mixed, precision=lax.Precision.HIGHEST, preferred_element_type=f32)
    xr = both[:, :LANES].reshape(rows // SUBLANES, SUBLANES, LANES)
    xi = both[:, LANES:].reshape(rows // SUBLANES, SUBLANES, LANES)
    for bit in range(3):
        xr, xi = sublane_gate(xr, xi, bit, unit(7 + bit))
    for bit in range(row_bits - 3):
        xr, xi = leading_gate(xr, xi, bit, unit(10 + bit))
    amp_out[:, 0] = cut(xr.reshape(rows, LANES), depth)
    amp_out[:, 1] = cut(xi.reshape(rows, LANES), depth)

    mr, mi = row_matrix([unit(local_bits + q) for q in range(global_bits)])
    mixed = jnp.concatenate(
        [jnp.concatenate([mr, -mi], axis=1), jnp.concatenate([mi, mr], axis=1)], axis=0
    )
    global_ref[0], global_ref[1] = halves(mixed)
    pl.semaphore_wait(barrier, devices - 1)
    scatter(0, amp_out, amp_in)

    samp_rows = owner_ref.shape[0]
    owner = owner_ref[...]
    owner_ids = iota((devices, LANES), 0)
    chunks = samp_rows // 2
    hot_rows = [(owner_ids == owner[r : r + 1]) for r in range(samp_rows)]
    pieces = [h.astype(f32).astype(bf16) for h in hot_rows]
    stacked = jnp.concatenate(
        [jnp.concatenate(pieces[2 * c : 2 * c + 2], axis=1) for c in range(chunks)], axis=0
    )
    tri_shape = (2 * LANES, 3 * LANES)
    tri_row, tri_col = iota(tri_shape, 0), iota(tri_shape, 1)
    tri = ((tri_row < tri_col) | (tri_col >= 2 * LANES)).astype(f32).astype(bf16)
    counts = jnp.dot(stacked, tri, preferred_element_type=f32)
    before = jnp.zeros((devices, LANES), f32)
    ranks = []
    for c in range(chunks):
        block = counts[c * devices : (c + 1) * devices]
        for h in range(2):
            spot = block[:, h * LANES : (h + 1) * LANES] + before
            mine = owner_ids == owner[2 * c + h : 2 * c + h + 1]
            ranks.append(jnp.sum(jnp.where(mine, spot, 0.0), axis=0, keepdims=True))
        before = before + block[:, 2 * LANES :]
    ranking = jnp.concatenate(ranks, axis=0).astype(i32)
    code_ref[...] = owner * capacity_rows + (ranking >> 7)
    rank_ref[...] = ranking & (LANES - 1)

    lane_ids = iota((LANES, LANES), 0)
    steps = samp_rows // SUBLANES

    def place(t, placed):
        window = pl.ds(pl.multiple_of(t * SUBLANES, SUBLANES), SUBLANES)
        code, rank, low = code_ref[window], rank_ref[window], low_ref[window] + 1
        low_top = (low >> 8).astype(f32)
        low_rest = (low & 255).astype(f32)
        hot = jnp.concatenate([one_hot(code[r : r + 1], codes) for r in range(SUBLANES)], axis=1)
        tops, rests = [], []
        for r in range(SUBLANES):
            here = lane_ids == rank[r : r + 1]
            tops.append(jnp.where(here, low_top[r : r + 1], 0.0).astype(bf16))
            rests.append(jnp.where(here, low_rest[r : r + 1], 0.0).astype(bf16))
        values = jnp.concatenate(
            [jnp.concatenate(tops, axis=1), jnp.concatenate(rests, axis=1)], axis=0
        )
        return placed + lax.dot_general(
            hot, values, (((1,), (1,)), ((), ())), preferred_element_type=f32
        )

    placed = lax.fori_loop(0, steps, place, jnp.zeros((codes, 2 * LANES), f32))
    wanted = placed[:, :LANES] * 256.0 + placed[:, LANES:] - 1.0
    wt_out[:, depth:] = cut(wanted, capacity_rows)

    all_of(0, amp_in).wait_recv()
    both = jnp.concatenate(
        [
            jnp.concatenate([amp_in[:, part, d] for d in range(depth)], axis=1)
            for part in range(2)
        ],
        axis=0,
    )
    top, rest = halves(both)
    both = jnp.dot(global_ref[0], top, preferred_element_type=f32) + (
        jnp.dot(global_ref[0], rest, preferred_element_type=f32)
        + jnp.dot(global_ref[1], top, preferred_element_type=f32)
    )
    xr, xi = both[:devices], both[devices:]
    weight = xr * xr + xi * xi
    weights = [weight[:, d * LANES : (d + 1) * LANES] for d in range(depth)]
    for d in range(depth):
        wt_out[:, d] = weights[d]
    scatter(1, wt_out, wt_in)

    weight = jnp.concatenate(weights, axis=0)
    norm_part = jnp.sum(weight, axis=0, keepdims=True)
    owner_bits = devices.bit_length() - 1
    code_shape = (rows, LANES)
    row_id = iota(code_shape, 0)
    row_value = (
        ((row_id & (devices - 1)) << local_bits)
        + me * (depth * LANES)
        + ((row_id >> owner_bits) << 7)
    )
    lane_value = iota((LANES, LANES), 0)
    row_code = jnp.zeros(code_shape, i32)
    lane_code = jnp.zeros((LANES, LANES), i32)
    lane_mask = jnp.zeros((), i32)
    for k in range(marg_count):
        qubit = marg[0, k]
        row_code = row_code + (((row_value >> qubit) & 1) << k)
        lane_code = lane_code + (((lane_value >> qubit) & 1) << k)
        lane_mask = lane_mask + jnp.where(qubit < 7, 1 << k, 0)
    bins = 2**marg_count
    top, rest = halves(weight)
    split = jnp.concatenate([top, rest], axis=0)
    @pl.loop(0, bins // LANES)
    def _(c):
        bin_id = c * LANES + iota((1, LANES), 1)
        lane_part = bin_id & lane_mask
        lane_hot = (lane_code == lane_part).astype(f32).astype(bf16)
        folded = jnp.dot(split, lane_hot, preferred_element_type=f32)
        folded = folded[:rows] + folded[rows:]
        picked = jnp.where(row_code == bin_id - lane_part, folded, 0.0)
        his_out[c, 0:1] = jnp.sum(picked, axis=0, keepdims=True)
    for c in range(bins // LANES):
        his_out[c, 1:2] = norm_part

    bin_share = devices * LANES // bins

    @pl.loop(1, devices)
    def _(k):
        target = peer(k)
        copy(3, his_out.at[target // bin_share], his_in.at[me], target).start()

    his_in[me] = his_out[me // bin_share]

    all_of(1, wt_in).wait_recv()
    table_ref[:, 0:rows] = split_table(join(wt_in[:, 0:depth]))
    req_ref[...] = join(wt_in[:, depth:]).astype(i32)
    group = 32 // capacity_rows
    groups = devices // group
    mine, spot = me // group, me % group

    def answer(turn):
        first = lax.rem(mine + turn, groups) * group
        window = pl.ds(pl.multiple_of(first * capacity_rows, SUBLANES), group * capacity_rows)
        wanted = req_ref[window]
        found = lookup(table_ref[:, 0:rows], wanted >> 7, wanted & (LANES - 1))
        ans_out[pl.ds(first, group)] = cut(found, capacity_rows)
        return first, jnp.sum(found, axis=0, keepdims=True)

    def reply(first, count):
        for j in range(1, count + 1):
            target = first + lax.rem(spot + j, group)
            copy(2, ans_out.at[target], ans_in.at[me], target).start()

    def step(turn, total):
        first, part = answer(turn)
        reply(first, group)
        return total + part

    total = lax.fori_loop(1, groups, step, jnp.zeros((1, LANES), f32))
    first, part = answer(0)
    reply(first, group - 1)
    ans_in[me] = ans_out[me]
    tot_out[0] = total + part
    spread(4, tot_out, tot_in)

    all_of(2, ans_in).wait_recv()
    table_ref[:, 0:codes] = split_table(join(ans_in[...]))
    for first in range(0, samp_rows, 32):
        window = slice(first, first + 32)
        probs_ref[window] = lookup(table_ref[:, 0:codes], code_ref[window], rank_ref[window])
    all_of(4, tot_in).wait_recv()
    all_of(3, his_in).wait_recv()
    hist_ref[...] = jnp.sum(his_in[...], axis=0)
    fid_ref[...] = jnp.sum(tot_in[...], axis=0)

    for channel, into in enumerate((amp_in, wt_in, ans_in, his_in, tot_in)):
        all_of(channel, into).wait_send()


def finish(sizes, values, hist, totals, probs_ref, mine_ref, fid_ref):
    amps_total, samples, bins = sizes
    mine = mine_ref.shape[1]
    start = lax.axis_index("dev") * mine
    total = jnp.sum(totals[...], axis=1, keepdims=True)
    norm = jnp.sum(hist[1:2], axis=1, keepdims=True)
    probs_ref[...] = amps_total * (values[...] / norm)
    line = jnp.broadcast_to(hist[0:1], (SUBLANES, LANES))
    line = pltpu.roll(line, (LANES - start % LANES) % LANES, 1)
    mine_ref[...] = bins * (line[0:1, :mine] / norm)
    fid_ref[...] = amps_total * (total / norm) / samples - 1.0


def shards(state, angles, sample_high, sample_low, marginal_qubits):
    devices = lax.axis_size("dev")
    amps_local = state.shape[1]
    samp_local = sample_low.shape[0]
    marg_count = marginal_qubits.shape[0]
    bins = 2**marg_count
    depth = amps_local // devices // LANES
    capacity_rows = 4 * samp_local // devices // LANES
    rows = amps_local // LANES
    samp_rows = samp_local // LANES
    sizes = (
        devices,
        depth,
        capacity_rows,
        marg_count,
    )
    vmem = pl.BlockSpec(memory_space=pltpu.VMEM)
    smem = pl.BlockSpec(memory_space=pltpu.SMEM)
    codes = devices * capacity_rows
    bin_rows = bins // LANES
    values, hist, totals = pl.pallas_call(
        functools.partial(kernel, sizes),
        out_shape=(
            jax.ShapeDtypeStruct((samp_rows, LANES), f32),
            jax.ShapeDtypeStruct((2, LANES), f32),
            jax.ShapeDtypeStruct((1, LANES), f32),
        ),
        in_specs=[smem, smem, vmem, vmem, vmem],
        out_specs=(vmem, vmem, vmem),
        scratch_shapes=[
            pltpu.VMEM((devices, 2, depth, LANES), f32),
            pltpu.VMEM((devices, 2, depth, LANES), f32),
            pltpu.VMEM((devices, depth + capacity_rows, LANES), f32),
            pltpu.VMEM((devices, depth + capacity_rows, LANES), f32),
            pltpu.VMEM((devices, capacity_rows, LANES), f32),
            pltpu.VMEM((devices, capacity_rows, LANES), f32),
            pltpu.VMEM((bin_rows, 2, LANES), f32),
            pltpu.VMEM((devices, 2, LANES), f32),
            pltpu.VMEM((1, 1, LANES), f32),
            pltpu.VMEM((devices, 1, LANES), f32),
            pltpu.VMEM((samp_rows, LANES), i32),
            pltpu.VMEM((samp_rows, LANES), i32),
            pltpu.VMEM((codes, LANES), i32),
            pltpu.VMEM((2 * LANES, max(rows, codes)), bf16),
            pltpu.VMEM((2, 2 * devices, 2 * devices), bf16),
            pltpu.VMEM((8, -(-angles.shape[0] // SUBLANES) * SUBLANES, LANES), f32),
            pltpu.SemaphoreType.DMA((5,)),
            pltpu.SemaphoreType.DMA((5,)),
        ],
        compiler_params=pltpu.CompilerParams(collective_id=0, has_side_effects=True),
        name="circuit",
    )(
        angles.T,
        marginal_qubits.reshape(1, marg_count),
        state.reshape(2, rows, LANES).transpose(1, 0, 2).reshape(2 * rows, LANES),
        sample_high.reshape(samp_rows, LANES),
        sample_low.reshape(samp_rows, LANES),
    )
    probs, mine, fid = pl.pallas_call(
        functools.partial(
            finish, (float(amps_local * devices), float(samp_local * devices), float(bins))
        ),
        out_shape=(
            jax.ShapeDtypeStruct((samp_rows, LANES), f32),
            jax.ShapeDtypeStruct((1, bins // devices), f32),
            jax.ShapeDtypeStruct((1, 1), f32),
        ),
        in_specs=[vmem, vmem, vmem],
        out_specs=(vmem, vmem, vmem),
        name="finish",
    )(values, hist, totals)
    return probs.reshape(samp_local), mine.reshape(bins // devices), fid.reshape(())


def solution(mesh):
    return jax.shard_map(
        shards,
        mesh=mesh,
        in_specs=(P(None, "dev"), P(), P("dev", None), P("dev"), P()),
        out_specs=(P("dev"), P("dev"), P()),
        check_vma=False,
    )
```

```python
import functools
import itertools

import jax
import jax.numpy as jnp
from jax import lax
from jax.experimental import pallas as pl
from jax.experimental.pallas import tpu as pltpu
from jax.sharding import PartitionSpec as P

LANES = 128
SUBLANES = 8
TORUS = (4, 4, 4, 2)
f32 = jnp.float32
bf16 = jnp.bfloat16
i32 = jnp.int32


def iota(shape, dim):
    return lax.broadcasted_iota(i32, shape, dim)


def gate_rows(angles, qubits):
    sub = iota((SUBLANES, LANES), 0)

    def column(j):
        blocks = []
        for first in range(0, qubits, SUBLANES):
            block = jnp.zeros((SUBLANES, LANES), f32)
            for q in range(first, min(first + SUBLANES, qubits)):
                block = jnp.where(sub == q - first, angles[j, q], block)
            blocks.append(block)
        return jnp.concatenate(blocks, axis=0)

    theta, first, second = column(0), column(1), column(2)
    cosine, sine = jnp.cos(theta), jnp.sin(theta)
    joint = first + second
    return [
        cosine,
        jnp.zeros_like(cosine),
        -jnp.cos(second) * sine,
        -jnp.sin(second) * sine,
        jnp.cos(first) * sine,
        jnp.sin(first) * sine,
        jnp.cos(joint) * cosine,
        jnp.sin(joint) * cosine,
    ]


def leading_gate(xr, xi, bit, u):
    n, s, lanes = xr.shape
    shape = (n >> (bit + 1), 2, 1 << bit, s, lanes)
    xr, xi = xr.reshape(shape), xi.reshape(shape)
    ar, ai, br, bi = xr[:, 0], xi[:, 0], xr[:, 1], xi[:, 1]
    outs_r, outs_i = [], []
    for row in range(2):
        pr, pi, qr, qi = u[4 * row : 4 * row + 4]
        outs_r.append(pr * ar - pi * ai + (qr * br - qi * bi))
        outs_i.append(pr * ai + pi * ar + (qr * bi + qi * br))
    return (
        jnp.stack(outs_r, 1).reshape(n, s, lanes),
        jnp.stack(outs_i, 1).reshape(n, s, lanes),
    )


def sublane_gate(xr, xi, bit, u):
    step = 1 << bit
    high = ((iota((SUBLANES, LANES), 0) >> bit) & 1) == 1

    def swap(x):
        down = pltpu.roll(x, step, 1)
        if 2 * step == SUBLANES:
            return down
        return jnp.where(high[None], down, pltpu.roll(x, SUBLANES - step, 1))

    keep_r = jnp.where(high, u[6], u[0])[None]
    keep_i = jnp.where(high, u[7], u[1])[None]
    cross_r = jnp.where(high, u[4], u[2])[None]
    cross_i = jnp.where(high, u[5], u[3])[None]
    yr, yi = swap(xr), swap(xi)
    return (
        keep_r * xr - keep_i * xi + (cross_r * yr - cross_i * yi),
        keep_r * xi + keep_i * xr + (cross_r * yi + cross_i * yr),
    )


def lane_matrix(units):
    shape = (LANES, LANES)
    row, col = iota(shape, 0), iota(shape, 1)
    mr = mi = None
    for bit, u in enumerate(units):
        rb, cb = ((row >> bit) & 1) == 1, ((col >> bit) & 1) == 1
        gr = jnp.where(cb, jnp.where(rb, u[6], u[4]), jnp.where(rb, u[2], u[0]))
        gi = jnp.where(cb, jnp.where(rb, u[7], u[5]), jnp.where(rb, u[3], u[1]))
        if mr is None:
            mr, mi = gr, gi
        else:
            mr, mi = mr * gr - mi * gi, mr * gi + mi * gr
    return mr, mi


def row_matrix(units):
    shape = (LANES, LANES)
    row, col = iota(shape, 0), iota(shape, 1)
    mr = mi = None
    for bit, u in enumerate(units):
        rb, cb = ((row >> bit) & 1) == 1, ((col >> bit) & 1) == 1
        gr = jnp.where(rb, jnp.where(cb, u[6], u[4]), jnp.where(cb, u[2], u[0]))
        gi = jnp.where(rb, jnp.where(cb, u[7], u[5]), jnp.where(cb, u[3], u[1]))
        if mr is None:
            mr, mi = gr, gi
        else:
            mr, mi = mr * gr - mi * gi, mr * gi + mi * gr
    return mr, mi


def cut(x, depth):
    rows = x.shape[0]
    x = x.reshape(rows // SUBLANES, SUBLANES, LANES)
    per = SUBLANES // depth
    if per == 1:
        return x
    parts = [x[:, k * depth : (k + 1) * depth] for k in range(per)]
    return jnp.stack(parts, 1).reshape(rows // depth, depth, LANES)


def join(x):
    n, depth, _ = x.shape
    per = SUBLANES // depth
    if per > 1:
        x = x.reshape(n // per, per, depth, LANES)
        x = jnp.concatenate([x[:, k] for k in range(per)], axis=1)
    return x.reshape(n * depth, LANES)


def halves(x):
    top = x.astype(bf16)
    return top, (x - top.astype(f32)).astype(bf16)


def one_hot(row, count):
    wide = jnp.broadcast_to(row.astype(f32), (16, LANES)).astype(bf16)
    ids = iota((count, LANES), 0).astype(f32).astype(bf16).reshape(count // 16, 16, LANES)
    hot = jnp.where(ids == wide[None], jnp.ones((), bf16), jnp.zeros((), bf16))
    return hot.reshape(count, LANES)


def split_table(table):
    flipped = table.T
    top, rest = halves(flipped)
    return jnp.concatenate([top, rest], axis=0)


def lookup(table, upper, lower):
    rows = upper.shape[0]
    count = table.shape[1]
    hot = jnp.concatenate([one_hot(upper[r : r + 1], count) for r in range(rows)], axis=1)
    both = jnp.dot(table, hot, preferred_element_type=f32)
    sub = iota((SUBLANES, LANES), 0)
    found = []
    for r in range(rows):
        part = slice(r * LANES, (r + 1) * LANES)
        value = (both[:LANES, part] + both[LANES:, part]).reshape(LANES // SUBLANES, SUBLANES, LANES)
        low = jnp.broadcast_to(lower[r : r + 1], (SUBLANES, LANES))
        for bit in (6, 5, 4, 3):
            half = value.shape[0] // 2
            value = jnp.where((((low >> bit) & 1) == 1)[None], value[half:], value[:half])
        value = jnp.where(sub == (low & (SUBLANES - 1)), value[0], 0.0)
        found.append(jnp.sum(value, axis=0, keepdims=True))
    return jnp.concatenate(found, axis=0)


def routes(me):
    parts = []
    rest = me
    for size in reversed(TORUS):
        parts.insert(0, lax.rem(rest, size))
        rest = rest // size
    scale = 1
    tables = []
    for part, size in zip(reversed(parts), reversed(TORUS)):
        tables.insert(0, [lax.rem(part + step, size) * scale for step in range(size)])
        scale *= size
    steps = list(itertools.product(*[range(size) for size in TORUS]))
    steps.sort(key=lambda step: -sum(min(d, n - d) for d, n in zip(step[:3], TORUS[:3])))
    upper = {(a, b): tables[0][a] + tables[1][b] for a in range(TORUS[0]) for b in range(TORUS[1])}
    lower = {(a, b): tables[2][a] + tables[3][b] for a in range(TORUS[2]) for b in range(TORUS[3])}
    return [upper[step[:2]] + lower[step[2:]] for step in steps if any(step)]


def kernel(
    sizes,
    angles_hbm,
    marg_hbm,
    state_hbm,
    owner_hbm,
    low_hbm,
    probs_ref,
    hist_ref,
    fid_ref,
    amp_out,
    amp_in,
    wt_out,
    wt_in,
    ans_out,
    ans_in,
    his_out,
    his_in,
    tot_out,
    tot_in,
    code_ref,
    rank_ref,
    req_ref,
    table_ref,
    global_ref,
    gates,
    angles,
    marg,
    state,
    owner_ref,
    low_ref,
    sends,
    recvs,
    loads,
):
    devices, depth, capacity_rows, marg_count = sizes
    me = lax.axis_index("dev")
    global_bits = devices.bit_length() - 1
    rows = state.shape[0] // 2
    row_bits = rows.bit_length() - 1
    local_bits = row_bits + 7
    codes = devices * capacity_rows

    peers = routes(me)
    inputs = [
        pltpu.make_async_copy(src, dst, loads.at[n])
        for n, (src, dst) in enumerate(
            (
                (angles_hbm, angles),
                (state_hbm, state),
                (owner_hbm, owner_ref),
                (low_hbm, low_ref),
                (marg_hbm, marg),
            )
        )
    ]
    for load in inputs:
        load.start()

    def copy(channel, src, dst, target):
        return pltpu.make_async_remote_copy(
            src_ref=src,
            dst_ref=dst,
            send_sem=sends.at[channel],
            recv_sem=recvs.at[channel],
            device_id=(target,),
            device_id_type=pl.DeviceIdType.MESH,
        )

    def scatter(channel, out, into):
        for target in peers:
            copy(channel, out.at[target], into.at[me], target).start()
        into[me] = out[me]

    def spread(channel, out, into):
        for target in peers:
            copy(channel, out.at[0], into.at[me], target).start()
        into[me] = out[0]

    def all_of(channel, into):
        many = into.at[pl.ds(0, devices - 1)]
        return copy(channel, many, many, peers[-1])

    barrier = pltpu.get_barrier_semaphore()

    for target in peers:
        pl.semaphore_signal(
            barrier, inc=1, device_id=(target,), device_id_type=pl.DeviceIdType.MESH
        )

    inputs[0].wait()
    for e, entry in enumerate(gate_rows(angles, global_bits + local_bits)):
        gates[e] = entry

    def unit(qubit):
        return [gates[e, qubit : qubit + 1] for e in range(8)]

    mr, mi = lane_matrix([unit(q) for q in range(7)])
    mixed = jnp.concatenate(
        [jnp.concatenate([mr, mi], axis=1), jnp.concatenate([-mi, mr], axis=1)], axis=0
    )
    inputs[1].wait()
    both = jnp.concatenate(
        [state[pl.ds(0, rows, stride=2)], state[pl.ds(1, rows, stride=2)]], axis=1
    )
    both = jnp.dot(both, mixed, precision=lax.Precision.HIGHEST, preferred_element_type=f32)
    xr = both[:, :LANES].reshape(rows // SUBLANES, SUBLANES, LANES)
    xi = both[:, LANES:].reshape(rows // SUBLANES, SUBLANES, LANES)
    for bit in range(3):
        xr, xi = sublane_gate(xr, xi, bit, unit(7 + bit))
    for bit in range(row_bits - 3):
        xr, xi = leading_gate(xr, xi, bit, unit(10 + bit))
    amp_out[:, 0] = cut(xr.reshape(rows, LANES), depth)
    amp_out[:, 1] = cut(xi.reshape(rows, LANES), depth)

    mr, mi = row_matrix([unit(local_bits + q) for q in range(global_bits)])
    mixed = jnp.concatenate(
        [jnp.concatenate([mr, -mi], axis=1), jnp.concatenate([mi, mr], axis=1)], axis=0
    )
    global_ref[0], global_ref[1] = halves(mixed)
    pl.semaphore_wait(barrier, devices - 1)
    scatter(0, amp_out, amp_in)

    samp_rows = owner_ref.shape[0]
    for load in inputs[2:]:
        load.wait()
    owner = owner_ref[...]
    owner_ids = iota((devices, LANES), 0)
    chunks = samp_rows // 2
    hot_rows = [(owner_ids == owner[r : r + 1]) for r in range(samp_rows)]
    pieces = [h.astype(f32).astype(bf16) for h in hot_rows]
    stacked = jnp.concatenate(
        [jnp.concatenate(pieces[2 * c : 2 * c + 2], axis=1) for c in range(chunks)], axis=0
    )
    tri_shape = (2 * LANES, 3 * LANES)
    tri_row, tri_col = iota(tri_shape, 0), iota(tri_shape, 1)
    tri = ((tri_row < tri_col) | (tri_col >= 2 * LANES)).astype(f32).astype(bf16)
    counts = jnp.dot(stacked, tri, preferred_element_type=f32)
    before = jnp.zeros((devices, LANES), f32)
    ranks = []
    for c in range(chunks):
        block = counts[c * devices : (c + 1) * devices]
        for h in range(2):
            spot = block[:, h * LANES : (h + 1) * LANES] + before
            mine = owner_ids == owner[2 * c + h : 2 * c + h + 1]
            ranks.append(jnp.sum(jnp.where(mine, spot, 0.0), axis=0, keepdims=True))
        before = before + block[:, 2 * LANES :]
    ranking = jnp.concatenate(ranks, axis=0).astype(i32)
    code_ref[...] = owner * capacity_rows + (ranking >> 7)
    rank_ref[...] = ranking & (LANES - 1)

    lane_ids = iota((LANES, LANES), 0)
    steps = samp_rows // SUBLANES

    def place(t, placed):
        window = pl.ds(pl.multiple_of(t * SUBLANES, SUBLANES), SUBLANES)
        code, rank, low = code_ref[window], rank_ref[window], low_ref[window] + 1
        low_top = (low >> 8).astype(f32)
        low_rest = (low & 255).astype(f32)
        hot = jnp.concatenate([one_hot(code[r : r + 1], codes) for r in range(SUBLANES)], axis=1)
        tops, rests = [], []
        for r in range(SUBLANES):
            here = lane_ids == rank[r : r + 1]
            tops.append(jnp.where(here, low_top[r : r + 1], 0.0).astype(bf16))
            rests.append(jnp.where(here, low_rest[r : r + 1], 0.0).astype(bf16))
        values = jnp.concatenate(
            [jnp.concatenate(tops, axis=1), jnp.concatenate(rests, axis=1)], axis=0
        )
        return placed + lax.dot_general(
            hot, values, (((1,), (1,)), ((), ())), preferred_element_type=f32
        )

    placed = lax.fori_loop(0, steps, place, jnp.zeros((codes, 2 * LANES), f32))
    wanted = placed[:, :LANES] * 256.0 + placed[:, LANES:] - 1.0
    wt_out[:, depth:] = cut(wanted, capacity_rows)

    all_of(0, amp_in).wait_recv()
    both = jnp.concatenate(
        [
            jnp.concatenate([amp_in[:, part, d] for d in range(depth)], axis=1)
            for part in range(2)
        ],
        axis=0,
    )
    top, rest = halves(both)
    both = jnp.dot(global_ref[0], top, preferred_element_type=f32) + (
        jnp.dot(global_ref[0], rest, preferred_element_type=f32)
        + jnp.dot(global_ref[1], top, preferred_element_type=f32)
    )
    xr, xi = both[:devices], both[devices:]
    weight = xr * xr + xi * xi
    weights = [weight[:, d * LANES : (d + 1) * LANES] for d in range(depth)]
    for d in range(depth):
        wt_out[:, d] = weights[d]
    scatter(1, wt_out, wt_in)

    weight = jnp.concatenate(weights, axis=0)
    norm_part = jnp.sum(weight, axis=0, keepdims=True)
    owner_bits = devices.bit_length() - 1
    code_shape = (rows, LANES)
    row_id = iota(code_shape, 0)
    row_value = (
        ((row_id & (devices - 1)) << local_bits)
        + me * (depth * LANES)
        + ((row_id >> owner_bits) << 7)
    )
    lane_value = iota((LANES, LANES), 0)
    row_code = jnp.zeros(code_shape, i32)
    lane_code = jnp.zeros((LANES, LANES), i32)
    lane_mask = jnp.zeros((), i32)
    for k in range(marg_count):
        qubit = marg[0, k]
        row_code = row_code + (((row_value >> qubit) & 1) << k)
        lane_code = lane_code + (((lane_value >> qubit) & 1) << k)
        lane_mask = lane_mask + jnp.where(qubit < 7, 1 << k, 0)
    bins = 2**marg_count
    top, rest = halves(weight)
    split = jnp.concatenate([top, rest], axis=0)
    @pl.loop(0, bins // LANES)
    def _(c):
        bin_id = c * LANES + iota((1, LANES), 1)
        lane_part = bin_id & lane_mask
        lane_hot = (lane_code == lane_part).astype(f32).astype(bf16)
        folded = jnp.dot(split, lane_hot, preferred_element_type=f32)
        folded = folded[:rows] + folded[rows:]
        picked = jnp.where(row_code == bin_id - lane_part, folded, 0.0)
        his_out[c, 0:1] = jnp.sum(picked, axis=0, keepdims=True)
    for c in range(bins // LANES):
        his_out[c, 1:2] = norm_part

    bin_share = devices * LANES // bins

    for target in peers:
        copy(3, his_out.at[target // bin_share], his_in.at[me], target).start()

    his_in[me] = his_out[me // bin_share]

    all_of(1, wt_in).wait_recv()
    table_ref[:, 0:rows] = split_table(join(wt_in[:, 0:depth]))
    req_ref[...] = join(wt_in[:, depth:]).astype(i32)
    group = 32 // capacity_rows
    groups = devices // group
    mine, spot = me // group, me % group

    def answer(turn):
        first = lax.rem(mine + turn, groups) * group
        window = pl.ds(pl.multiple_of(first * capacity_rows, SUBLANES), group * capacity_rows)
        wanted = req_ref[window]
        found = lookup(table_ref[:, 0:rows], wanted >> 7, wanted & (LANES - 1))
        ans_out[pl.ds(first, group)] = cut(found, capacity_rows)
        return first, jnp.sum(found, axis=0, keepdims=True)

    def reply(first, count):
        for j in range(1, count + 1):
            target = first + lax.rem(spot + j, group)
            copy(2, ans_out.at[target], ans_in.at[me], target).start()

    def step(turn, total):
        first, part = answer(turn)
        reply(first, group)
        return total + part

    total = lax.fori_loop(1, groups, step, jnp.zeros((1, LANES), f32))
    first, part = answer(0)
    reply(first, group - 1)
    ans_in[me] = ans_out[me]
    tot_out[0] = total + part
    spread(4, tot_out, tot_in)

    all_of(2, ans_in).wait_recv()
    table_ref[:, 0:codes] = split_table(join(ans_in[...]))
    for first in range(0, samp_rows, 32):
        window = slice(first, first + 32)
        probs_ref[window] = lookup(table_ref[:, 0:codes], code_ref[window], rank_ref[window])
    all_of(4, tot_in).wait_recv()
    all_of(3, his_in).wait_recv()
    hist_ref[...] = jnp.sum(his_in[...], axis=0)
    fid_ref[...] = jnp.sum(tot_in[...], axis=0)

    for channel, into in enumerate((amp_in, wt_in, ans_in, his_in, tot_in)):
        all_of(channel, into).wait_send()


def finish(sizes, values, hist, totals, probs_ref, mine_ref, fid_ref):
    amps_total, samples, bins = sizes
    mine = mine_ref.shape[1]
    start = lax.axis_index("dev") * mine
    total = jnp.sum(totals[...], axis=1, keepdims=True)
    norm = jnp.sum(hist[1:2], axis=1, keepdims=True)
    probs_ref[...] = amps_total * (values[...] / norm)
    line = jnp.broadcast_to(hist[0:1], (SUBLANES, LANES))
    line = pltpu.roll(line, (LANES - start % LANES) % LANES, 1)
    mine_ref[...] = bins * (line[0:1, :mine] / norm)
    fid_ref[...] = amps_total * (total / norm) / samples - 1.0


def shards(state, angles, sample_high, sample_low, marginal_qubits):
    devices = lax.axis_size("dev")
    amps_local = state.shape[1]
    samp_local = sample_low.shape[0]
    marg_count = marginal_qubits.shape[0]
    bins = 2**marg_count
    depth = amps_local // devices // LANES
    capacity_rows = 4 * samp_local // devices // LANES
    rows = amps_local // LANES
    samp_rows = samp_local // LANES
    sizes = (
        devices,
        depth,
        capacity_rows,
        marg_count,
    )
    vmem = pl.BlockSpec(memory_space=pltpu.VMEM)
    codes = devices * capacity_rows
    bin_rows = bins // LANES
    values, hist, totals = pl.pallas_call(
        functools.partial(kernel, sizes),
        out_shape=(
            jax.ShapeDtypeStruct((samp_rows, LANES), f32),
            jax.ShapeDtypeStruct((2, LANES), f32),
            jax.ShapeDtypeStruct((1, LANES), f32),
        ),
        in_specs=[pl.BlockSpec(memory_space=pl.ANY)] * 5,
        out_specs=(vmem, vmem, vmem),
        scratch_shapes=[
            pltpu.VMEM((devices, 2, depth, LANES), f32),
            pltpu.VMEM((devices, 2, depth, LANES), f32),
            pltpu.VMEM((devices, depth + capacity_rows, LANES), f32),
            pltpu.VMEM((devices, depth + capacity_rows, LANES), f32),
            pltpu.VMEM((devices, capacity_rows, LANES), f32),
            pltpu.VMEM((devices, capacity_rows, LANES), f32),
            pltpu.VMEM((bin_rows, 2, LANES), f32),
            pltpu.VMEM((devices, 2, LANES), f32),
            pltpu.VMEM((1, 1, LANES), f32),
            pltpu.VMEM((devices, 1, LANES), f32),
            pltpu.VMEM((samp_rows, LANES), i32),
            pltpu.VMEM((samp_rows, LANES), i32),
            pltpu.VMEM((codes, LANES), i32),
            pltpu.VMEM((2 * LANES, max(rows, codes)), bf16),
            pltpu.VMEM((2, 2 * devices, 2 * devices), bf16),
            pltpu.VMEM((8, -(-angles.shape[0] // SUBLANES) * SUBLANES, LANES), f32),
            pltpu.SMEM((angles.shape[1], angles.shape[0]), f32),
            pltpu.SMEM((1, marg_count), i32),
            pltpu.VMEM((2 * rows, LANES), f32),
            pltpu.VMEM((samp_rows, LANES), i32),
            pltpu.VMEM((samp_rows, LANES), i32),
            pltpu.SemaphoreType.DMA((5,)),
            pltpu.SemaphoreType.DMA((5,)),
            pltpu.SemaphoreType.DMA((5,)),
        ],
        compiler_params=pltpu.CompilerParams(collective_id=0, has_side_effects=True),
        name="circuit",
    )(
        angles.T,
        marginal_qubits.reshape(1, marg_count),
        state.reshape(2, rows, LANES).transpose(1, 0, 2).reshape(2 * rows, LANES),
        sample_high.reshape(samp_rows, LANES),
        sample_low.reshape(samp_rows, LANES),
    )
    probs, mine, fid = pl.pallas_call(
        functools.partial(
            finish, (float(amps_local * devices), float(samp_local * devices), float(bins))
        ),
        out_shape=(
            jax.ShapeDtypeStruct((samp_rows, LANES), f32),
            jax.ShapeDtypeStruct((1, bins // devices), f32),
            jax.ShapeDtypeStruct((1, 1), f32),
        ),
        in_specs=[vmem, vmem, vmem],
        out_specs=(vmem, vmem, vmem),
        name="finish",
    )(values, hist, totals)
    return probs.reshape(samp_local), mine.reshape(bins // devices), fid.reshape(())


def solution(mesh):
    return jax.shard_map(
        shards,
        mesh=mesh,
        in_specs=(P(None, "dev"), P(), P("dev", None), P("dev"), P()),
        out_specs=(P("dev"), P("dev"), P()),
        check_vma=False,
    )
```

```python
import functools
import itertools

import jax
import jax.numpy as jnp
from jax import lax
from jax.experimental import pallas as pl
from jax.experimental.pallas import tpu as pltpu
from jax.sharding import PartitionSpec as P

LANES = 128
SUBLANES = 8
TORUS = (4, 4, 4, 2)
f32 = jnp.float32
bf16 = jnp.bfloat16
i32 = jnp.int32


def iota(shape, dim):
    return lax.broadcasted_iota(i32, shape, dim)


def gate_rows(angles, qubits):
    sub = iota((SUBLANES, LANES), 0)

    def column(j):
        blocks = []
        for first in range(0, qubits, SUBLANES):
            block = jnp.zeros((SUBLANES, LANES), f32)
            for q in range(first, min(first + SUBLANES, qubits)):
                block = jnp.where(sub == q - first, angles[j, q], block)
            blocks.append(block)
        return jnp.concatenate(blocks, axis=0)

    theta, first, second = column(0), column(1), column(2)
    cosine, sine = jnp.cos(theta), jnp.sin(theta)
    joint = first + second
    return [
        cosine,
        jnp.zeros_like(cosine),
        -jnp.cos(second) * sine,
        -jnp.sin(second) * sine,
        jnp.cos(first) * sine,
        jnp.sin(first) * sine,
        jnp.cos(joint) * cosine,
        jnp.sin(joint) * cosine,
    ]


def leading_gate(xr, xi, bit, u):
    n, s, lanes = xr.shape
    shape = (n >> (bit + 1), 2, 1 << bit, s, lanes)
    xr, xi = xr.reshape(shape), xi.reshape(shape)
    ar, ai, br, bi = xr[:, 0], xi[:, 0], xr[:, 1], xi[:, 1]
    outs_r, outs_i = [], []
    for row in range(2):
        pr, pi, qr, qi = u[4 * row : 4 * row + 4]
        outs_r.append(pr * ar - pi * ai + (qr * br - qi * bi))
        outs_i.append(pr * ai + pi * ar + (qr * bi + qi * br))
    return (
        jnp.stack(outs_r, 1).reshape(n, s, lanes),
        jnp.stack(outs_i, 1).reshape(n, s, lanes),
    )


def sublane_gate(xr, xi, bit, u):
    step = 1 << bit
    high = ((iota((SUBLANES, LANES), 0) >> bit) & 1) == 1

    def swap(x):
        down = pltpu.roll(x, step, 1)
        if 2 * step == SUBLANES:
            return down
        return jnp.where(high[None], down, pltpu.roll(x, SUBLANES - step, 1))

    keep_r = jnp.where(high, u[6], u[0])[None]
    keep_i = jnp.where(high, u[7], u[1])[None]
    cross_r = jnp.where(high, u[4], u[2])[None]
    cross_i = jnp.where(high, u[5], u[3])[None]
    yr, yi = swap(xr), swap(xi)
    return (
        keep_r * xr - keep_i * xi + (cross_r * yr - cross_i * yi),
        keep_r * xi + keep_i * xr + (cross_r * yi + cross_i * yr),
    )


def lane_matrix(units):
    shape = (LANES, LANES)
    row, col = iota(shape, 0), iota(shape, 1)
    mr = mi = None
    for bit, u in enumerate(units):
        rb, cb = ((row >> bit) & 1) == 1, ((col >> bit) & 1) == 1
        gr = jnp.where(cb, jnp.where(rb, u[6], u[4]), jnp.where(rb, u[2], u[0]))
        gi = jnp.where(cb, jnp.where(rb, u[7], u[5]), jnp.where(rb, u[3], u[1]))
        if mr is None:
            mr, mi = gr, gi
        else:
            mr, mi = mr * gr - mi * gi, mr * gi + mi * gr
    return mr, mi


def row_matrix(units):
    shape = (LANES, LANES)
    row, col = iota(shape, 0), iota(shape, 1)
    mr = mi = None
    for bit, u in enumerate(units):
        rb, cb = ((row >> bit) & 1) == 1, ((col >> bit) & 1) == 1
        gr = jnp.where(rb, jnp.where(cb, u[6], u[4]), jnp.where(cb, u[2], u[0]))
        gi = jnp.where(rb, jnp.where(cb, u[7], u[5]), jnp.where(cb, u[3], u[1]))
        if mr is None:
            mr, mi = gr, gi
        else:
            mr, mi = mr * gr - mi * gi, mr * gi + mi * gr
    return mr, mi


def cut(x, depth):
    rows = x.shape[0]
    x = x.reshape(rows // SUBLANES, SUBLANES, LANES)
    per = SUBLANES // depth
    if per == 1:
        return x
    parts = [x[:, k * depth : (k + 1) * depth] for k in range(per)]
    return jnp.stack(parts, 1).reshape(rows // depth, depth, LANES)


def join(x):
    n, depth, _ = x.shape
    per = SUBLANES // depth
    if per > 1:
        x = x.reshape(n // per, per, depth, LANES)
        x = jnp.concatenate([x[:, k] for k in range(per)], axis=1)
    return x.reshape(n * depth, LANES)


def halves(x):
    top = x.astype(bf16)
    return top, (x - top.astype(f32)).astype(bf16)


def one_hot(row, count):
    wide = jnp.broadcast_to(row.astype(f32), (16, LANES)).astype(bf16)
    ids = iota((count, LANES), 0).astype(f32).astype(bf16).reshape(count // 16, 16, LANES)
    hot = jnp.where(ids == wide[None], jnp.ones((), bf16), jnp.zeros((), bf16))
    return hot.reshape(count, LANES)


def split_table(table):
    flipped = table.T
    top, rest = halves(flipped)
    return jnp.concatenate([top, rest], axis=0)


def lookup(table, upper, lower):
    rows = upper.shape[0]
    count = table.shape[1]
    hot = jnp.concatenate([one_hot(upper[r : r + 1], count) for r in range(rows)], axis=1)
    both = jnp.dot(table, hot, preferred_element_type=f32)
    sub = iota((SUBLANES, LANES), 0)
    found = []
    for r in range(rows):
        part = slice(r * LANES, (r + 1) * LANES)
        value = (both[:LANES, part] + both[LANES:, part]).reshape(LANES // SUBLANES, SUBLANES, LANES)
        low = jnp.broadcast_to(lower[r : r + 1], (SUBLANES, LANES))
        for bit in (6, 5, 4, 3):
            half = value.shape[0] // 2
            value = jnp.where((((low >> bit) & 1) == 1)[None], value[half:], value[:half])
        value = jnp.where(sub == (low & (SUBLANES - 1)), value[0], 0.0)
        found.append(jnp.sum(value, axis=0, keepdims=True))
    return jnp.concatenate(found, axis=0)


def lookup_lanes(plain, upper, lower):
    bits = plain.shape[0].bit_length() - 1
    high = [((upper >> bit) & 1) == 1 for bit in range(bits)]

    def pick(first, bit):
        if bit < 0:
            line = jnp.broadcast_to(plain[first : first + 1], (SUBLANES, LANES))
            return jnp.take_along_axis(line, lower, axis=1, mode="promise_in_bounds")
        zero = pick(first, bit - 1)
        return jnp.where(high[bit], pick(first + (1 << bit), bit - 1), zero)

    return pick(0, bits - 1)


def lookup_both(table, plain, upper, lower, lanes):
    dots = upper.shape[0] - lanes
    found = [lookup(table, upper[:dots], lower[:dots])]
    for first in range(dots, dots + lanes, SUBLANES):
        part = slice(first, first + SUBLANES)
        value = lookup_lanes(plain, upper[part], lower[part])
        found.append(jnp.where(upper[part] >= 0, value, 0.0))
    return jnp.concatenate(found, axis=0)


def routes(me):
    parts = []
    rest = me
    for size in reversed(TORUS):
        parts.insert(0, lax.rem(rest, size))
        rest = rest // size
    scale = 1
    tables = []
    for part, size in zip(reversed(parts), reversed(TORUS)):
        tables.insert(0, [lax.rem(part + step, size) * scale for step in range(size)])
        scale *= size
    steps = list(itertools.product(*[range(size) for size in TORUS]))
    steps.sort(key=lambda step: -sum(min(d, n - d) for d, n in zip(step[:3], TORUS[:3])))
    upper = {(a, b): tables[0][a] + tables[1][b] for a in range(TORUS[0]) for b in range(TORUS[1])}
    lower = {(a, b): tables[2][a] + tables[3][b] for a in range(TORUS[2]) for b in range(TORUS[3])}
    return [upper[step[:2]] + lower[step[2:]] for step in steps if any(step)]


def kernel(
    sizes,
    angles_hbm,
    marg_hbm,
    state_hbm,
    owner_hbm,
    low_hbm,
    probs_ref,
    hist_ref,
    fid_ref,
    amp_out,
    amp_in,
    wt_out,
    wt_in,
    ans_out,
    ans_in,
    his_ref,
    tot_out,
    tot_in,
    code_ref,
    rank_ref,
    req_ref,
    table_ref,
    plain_ref,
    global_ref,
    gates,
    angles,
    marg,
    state,
    owner_ref,
    low_ref,
    sends,
    recvs,
    loads,
):
    devices, depth, capacity_rows, marg_count = sizes
    me = lax.axis_index("dev")
    global_bits = devices.bit_length() - 1
    rows = state.shape[0] // 2
    row_bits = rows.bit_length() - 1
    local_bits = row_bits + 7
    codes = devices * capacity_rows

    peers = routes(me)
    inputs = [
        pltpu.make_async_copy(src, dst, loads.at[n])
        for n, (src, dst) in enumerate(
            (
                (angles_hbm, angles),
                (state_hbm, state),
                (owner_hbm, owner_ref),
                (low_hbm, low_ref),
                (marg_hbm, marg),
            )
        )
    ]
    for load in inputs:
        load.start()

    def copy(channel, src, dst, target):
        return pltpu.make_async_remote_copy(
            src_ref=src,
            dst_ref=dst,
            send_sem=sends.at[channel],
            recv_sem=recvs.at[channel],
            device_id=(target,),
            device_id_type=pl.DeviceIdType.MESH,
        )

    def scatter(channel, out, into):
        for target in peers:
            copy(channel, out.at[target], into.at[me], target).start()
        into[me] = out[me]

    def spread(channel, out, into):
        for target in peers:
            copy(channel, out.at[0], into.at[me], target).start()
        into[me] = out[0]

    def all_of(channel, into):
        many = into.at[pl.ds(0, devices - 1)]
        return copy(channel, many, many, peers[-1])

    barrier = pltpu.get_barrier_semaphore()

    for target in peers:
        pl.semaphore_signal(
            barrier, inc=1, device_id=(target,), device_id_type=pl.DeviceIdType.MESH
        )

    inputs[0].wait()
    for e, entry in enumerate(gate_rows(angles, global_bits + local_bits)):
        gates[e] = entry

    def unit(qubit):
        return [gates[e, qubit : qubit + 1] for e in range(8)]

    mr, mi = lane_matrix([unit(q) for q in range(7)])
    mixed = jnp.concatenate(
        [jnp.concatenate([mr, mi], axis=1), jnp.concatenate([-mi, mr], axis=1)], axis=0
    )
    inputs[1].wait()
    both = jnp.concatenate(
        [state[pl.ds(0, rows, stride=2)], state[pl.ds(1, rows, stride=2)]], axis=1
    )
    both = jnp.dot(both, mixed, precision=lax.Precision.HIGHEST, preferred_element_type=f32)
    xr = both[:, :LANES].reshape(rows // SUBLANES, SUBLANES, LANES)
    xi = both[:, LANES:].reshape(rows // SUBLANES, SUBLANES, LANES)
    for bit in range(3):
        xr, xi = sublane_gate(xr, xi, bit, unit(7 + bit))
    for bit in range(row_bits - 3):
        xr, xi = leading_gate(xr, xi, bit, unit(10 + bit))
    amp_out[:, 0] = cut(xr.reshape(rows, LANES), depth)
    amp_out[:, 1] = cut(xi.reshape(rows, LANES), depth)

    mr, mi = row_matrix([unit(local_bits + q) for q in range(global_bits)])
    mixed = jnp.concatenate(
        [jnp.concatenate([mr, -mi], axis=1), jnp.concatenate([mi, mr], axis=1)], axis=0
    )
    global_ref[0], global_ref[1] = halves(mixed)
    pl.semaphore_wait(barrier, devices - 1)
    scatter(0, amp_out, amp_in)

    samp_rows = owner_ref.shape[0]
    for load in inputs[2:]:
        load.wait()
    owner = owner_ref[...]
    owner_ids = iota((devices, LANES), 0)
    chunks = samp_rows // 2
    hot_rows = [(owner_ids == owner[r : r + 1]) for r in range(samp_rows)]
    pieces = [h.astype(f32).astype(bf16) for h in hot_rows]
    stacked = jnp.concatenate(
        [jnp.concatenate(pieces[2 * c : 2 * c + 2], axis=1) for c in range(chunks)], axis=0
    )
    tri_shape = (2 * LANES, 3 * LANES)
    tri_row, tri_col = iota(tri_shape, 0), iota(tri_shape, 1)
    tri = ((tri_row < tri_col) | (tri_col >= 2 * LANES)).astype(f32).astype(bf16)
    counts = jnp.dot(stacked, tri, preferred_element_type=f32)
    before = jnp.zeros((devices, LANES), f32)
    ranks = []
    for c in range(chunks):
        block = counts[c * devices : (c + 1) * devices]
        for h in range(2):
            spot = block[:, h * LANES : (h + 1) * LANES] + before
            mine = owner_ids == owner[2 * c + h : 2 * c + h + 1]
            ranks.append(jnp.sum(jnp.where(mine, spot, 0.0), axis=0, keepdims=True))
        before = before + block[:, 2 * LANES :]
    ranking = jnp.concatenate(ranks, axis=0).astype(i32)
    code_ref[...] = owner * capacity_rows + (ranking >> 7)
    rank_ref[...] = ranking & (LANES - 1)

    lane_ids = iota((LANES, LANES), 0)
    steps = samp_rows // SUBLANES

    def place(t, placed):
        window = pl.ds(pl.multiple_of(t * SUBLANES, SUBLANES), SUBLANES)
        code, rank, low = code_ref[window], rank_ref[window], low_ref[window] + 1
        low_top = (low >> 8).astype(f32)
        low_rest = (low & 255).astype(f32)
        hot = jnp.concatenate([one_hot(code[r : r + 1], codes) for r in range(SUBLANES)], axis=1)
        tops, rests = [], []
        for r in range(SUBLANES):
            here = lane_ids == rank[r : r + 1]
            tops.append(jnp.where(here, low_top[r : r + 1], 0.0).astype(bf16))
            rests.append(jnp.where(here, low_rest[r : r + 1], 0.0).astype(bf16))
        values = jnp.concatenate(
            [jnp.concatenate(tops, axis=1), jnp.concatenate(rests, axis=1)], axis=0
        )
        return placed + lax.dot_general(
            hot, values, (((1,), (1,)), ((), ())), preferred_element_type=f32
        )

    placed = lax.fori_loop(0, steps, place, jnp.zeros((codes, 2 * LANES), f32))
    wanted = placed[:, :LANES] * 256.0 + placed[:, LANES:] - 1.0
    wt_out[:, depth:] = cut(wanted, capacity_rows)

    all_of(0, amp_in).wait_recv()
    both = jnp.concatenate(
        [
            jnp.concatenate([amp_in[:, part, d] for d in range(depth)], axis=1)
            for part in range(2)
        ],
        axis=0,
    )
    top, rest = halves(both)
    both = jnp.dot(global_ref[0], top, preferred_element_type=f32) + (
        jnp.dot(global_ref[0], rest, preferred_element_type=f32)
        + jnp.dot(global_ref[1], top, preferred_element_type=f32)
    )
    xr, xi = both[:devices], both[devices:]
    weight = xr * xr + xi * xi
    weights = [weight[:, d * LANES : (d + 1) * LANES] for d in range(depth)]
    for d in range(depth):
        wt_out[:, d] = weights[d]
    scatter(1, wt_out, wt_in)

    weight = jnp.concatenate(weights, axis=0)
    norm_part = jnp.sum(weight, axis=0, keepdims=True)
    owner_bits = devices.bit_length() - 1
    code_shape = (rows, LANES)
    row_id = iota(code_shape, 0)
    row_value = (
        ((row_id & (devices - 1)) << local_bits)
        + me * (depth * LANES)
        + ((row_id >> owner_bits) << 7)
    )
    lane_value = iota((LANES, LANES), 0)
    row_code = jnp.zeros(code_shape, i32)
    lane_code = jnp.zeros((LANES, LANES), i32)
    lane_mask = jnp.zeros((), i32)
    for k in range(marg_count):
        qubit = marg[0, k]
        row_code = row_code + (((row_value >> qubit) & 1) << k)
        lane_code = lane_code + (((lane_value >> qubit) & 1) << k)
        lane_mask = lane_mask + jnp.where(qubit < 7, 1 << k, 0)
    bins = 2**marg_count
    top, rest = halves(weight)
    split = jnp.concatenate([top, rest], axis=0)
    @pl.loop(0, bins // LANES)
    def _(c):
        bin_id = c * LANES + iota((1, LANES), 1)
        lane_part = bin_id & lane_mask
        lane_hot = (lane_code == lane_part).astype(f32).astype(bf16)
        folded = jnp.dot(split, lane_hot, preferred_element_type=f32)
        folded = folded[:rows] + folded[rows:]
        picked = jnp.where(row_code == bin_id - lane_part, folded, 0.0)
        his_ref[pl.ds(c, 1)] = jnp.sum(picked, axis=0, keepdims=True)

    bin_share = devices * LANES // bins
    for c in range(bins // LANES):
        part = slice(c * bin_share, (c + 1) * bin_share)
        ans_out[part, capacity_rows] = jnp.broadcast_to(his_ref[c : c + 1], (bin_share, LANES))
    ans_out[:, capacity_rows + 1] = jnp.broadcast_to(norm_part, (devices, LANES))

    all_of(1, wt_in).wait_recv()
    plain_ref[0:rows] = join(wt_in[:, 0:depth])
    table_ref[:, 0:rows] = split_table(plain_ref[0:rows])
    req_ref[...] = join(wt_in[:, depth:]).astype(i32)
    group = 128 // capacity_rows
    groups = devices // group
    mine, spot = me // group, me % group

    def answer(turn):
        first = lax.rem(mine + turn, groups) * group
        window = pl.ds(pl.multiple_of(first * capacity_rows, SUBLANES), group * capacity_rows)
        wanted = req_ref[window]
        found = lookup_both(
            table_ref[:, 0:rows], plain_ref.at[0:rows], wanted >> 7, wanted & (LANES - 1), 48
        )
        ans_out[pl.ds(first, group), 0:capacity_rows] = cut(found, capacity_rows)
        return first, jnp.sum(found, axis=0, keepdims=True)

    def reply(first, count):
        for j in range(1, count + 1):
            target = first + lax.rem(spot + j, group)
            copy(2, ans_out.at[target], ans_in.at[me], target).start()

    def step(turn, total):
        first, part = answer(turn)
        reply(first, group)
        return total + part

    total = lax.fori_loop(1, groups, step, jnp.zeros((1, LANES), f32))
    first, part = answer(0)
    reply(first, group - 1)
    ans_in[me] = ans_out[me]
    tot_out[0] = total + part
    spread(3, tot_out, tot_in)

    all_of(2, ans_in).wait_recv()
    plain_ref[0:codes] = join(ans_in[:, 0:capacity_rows])
    table_ref[:, 0:codes] = split_table(plain_ref[0:codes])
    for first in range(0, samp_rows, 32):
        window = slice(first, first + 32)
        probs_ref[window] = lookup_both(
            table_ref[:, 0:codes], plain_ref.at[0:codes], code_ref[window], rank_ref[window], 8
        )
    hist_ref[...] = jnp.sum(ans_in[:, capacity_rows:], axis=0)
    all_of(3, tot_in).wait_recv()
    fid_ref[...] = jnp.sum(tot_in[...], axis=0)

    for channel, into in enumerate((amp_in, wt_in, ans_in, tot_in)):
        all_of(channel, into).wait_send()


def finish(sizes, values, hist, totals, probs_ref, mine_ref, fid_ref):
    amps_total, samples, bins = sizes
    mine = mine_ref.shape[1]
    start = lax.axis_index("dev") * mine
    total = jnp.sum(totals[...], axis=1, keepdims=True)
    norm = jnp.sum(hist[1:2], axis=1, keepdims=True)
    probs_ref[...] = amps_total * (values[...] / norm)
    line = jnp.broadcast_to(hist[0:1], (SUBLANES, LANES))
    line = pltpu.roll(line, (LANES - start % LANES) % LANES, 1)
    mine_ref[...] = bins * (line[0:1, :mine] / norm)
    fid_ref[...] = amps_total * (total / norm) / samples - 1.0


def shards(state, angles, sample_high, sample_low, marginal_qubits):
    devices = lax.axis_size("dev")
    amps_local = state.shape[1]
    samp_local = sample_low.shape[0]
    marg_count = marginal_qubits.shape[0]
    bins = 2**marg_count
    depth = amps_local // devices // LANES
    capacity_rows = 4 * samp_local // devices // LANES
    rows = amps_local // LANES
    samp_rows = samp_local // LANES
    sizes = (
        devices,
        depth,
        capacity_rows,
        marg_count,
    )
    vmem = pl.BlockSpec(memory_space=pltpu.VMEM)
    codes = devices * capacity_rows
    bin_rows = bins // LANES
    values, hist, totals = pl.pallas_call(
        functools.partial(kernel, sizes),
        out_shape=(
            jax.ShapeDtypeStruct((samp_rows, LANES), f32),
            jax.ShapeDtypeStruct((2, LANES), f32),
            jax.ShapeDtypeStruct((1, LANES), f32),
        ),
        in_specs=[pl.BlockSpec(memory_space=pltpu.HBM)] * 5,
        out_specs=(vmem, vmem, vmem),
        scratch_shapes=[
            pltpu.VMEM((devices, 2, depth, LANES), f32),
            pltpu.VMEM((devices, 2, depth, LANES), f32),
            pltpu.VMEM((devices, depth + capacity_rows, LANES), f32),
            pltpu.VMEM((devices, depth + capacity_rows, LANES), f32),
            pltpu.VMEM((devices, capacity_rows + 2, LANES), f32),
            pltpu.VMEM((devices, capacity_rows + 2, LANES), f32),
            pltpu.VMEM((bin_rows, LANES), f32),
            pltpu.VMEM((1, 1, LANES), f32),
            pltpu.VMEM((devices, 1, LANES), f32),
            pltpu.VMEM((samp_rows, LANES), i32),
            pltpu.VMEM((samp_rows, LANES), i32),
            pltpu.VMEM((codes, LANES), i32),
            pltpu.VMEM((2 * LANES, max(rows, codes)), bf16),
            pltpu.VMEM((max(rows, codes), LANES), f32),
            pltpu.VMEM((2, 2 * devices, 2 * devices), bf16),
            pltpu.VMEM((8, -(-angles.shape[0] // SUBLANES) * SUBLANES, LANES), f32),
            pltpu.SMEM((angles.shape[1], angles.shape[0]), f32),
            pltpu.SMEM((1, marg_count), i32),
            pltpu.VMEM((2 * rows, LANES), f32),
            pltpu.VMEM((samp_rows, LANES), i32),
            pltpu.VMEM((samp_rows, LANES), i32),
            pltpu.SemaphoreType.DMA((4,)),
            pltpu.SemaphoreType.DMA((4,)),
            pltpu.SemaphoreType.DMA((5,)),
        ],
        compiler_params=pltpu.CompilerParams(
            collective_id=0, has_side_effects=True, vmem_limit_bytes=24 << 20
        ),
        name="circuit",
    )(
        pltpu.with_memory_space_constraint(angles.T, pltpu.HBM),
        pltpu.with_memory_space_constraint(marginal_qubits.reshape(1, marg_count), pltpu.HBM),
        pltpu.with_memory_space_constraint(state.reshape(2, rows, LANES).transpose(1, 0, 2).reshape(2 * rows, LANES), pltpu.HBM),
        pltpu.with_memory_space_constraint(sample_high.reshape(samp_rows, LANES), pltpu.HBM),
        pltpu.with_memory_space_constraint(sample_low.reshape(samp_rows, LANES), pltpu.HBM),
    )
    probs, mine, fid = pl.pallas_call(
        functools.partial(
            finish, (float(amps_local * devices), float(samp_local * devices), float(bins))
        ),
        out_shape=(
            jax.ShapeDtypeStruct((samp_rows, LANES), f32),
            jax.ShapeDtypeStruct((1, bins // devices), f32),
            jax.ShapeDtypeStruct((1, 1), f32),
        ),
        in_specs=[vmem, vmem, vmem],
        out_specs=(vmem, vmem, vmem),
        compiler_params=pltpu.CompilerParams(vmem_limit_bytes=1 << 20),
        name="finish",
    )(values, hist, totals)
    return probs.reshape(samp_local), mine.reshape(bins // devices), fid.reshape(())


def solution(mesh):
    return jax.shard_map(
        shards,
        mesh=mesh,
        in_specs=(P(None, "dev"), P(), P("dev", None), P("dev"), P()),
        out_specs=(P("dev"), P("dev"), P()),
        check_vma=False,
    )
```

```python
import functools
import itertools

import jax
import jax.numpy as jnp
from jax import lax
from jax.experimental import pallas as pl
from jax.experimental.pallas import tpu as pltpu
from jax.sharding import PartitionSpec as P

LANES = 128
SUBLANES = 8
TORUS = (4, 4, 4, 2)
f32 = jnp.float32
bf16 = jnp.bfloat16
i32 = jnp.int32


def iota(shape, dim):
    return lax.broadcasted_iota(i32, shape, dim)


def gate_rows(angles, qubits):
    sub = iota((SUBLANES, LANES), 0)

    def column(j):
        blocks = []
        for first in range(0, qubits, SUBLANES):
            block = jnp.zeros((SUBLANES, LANES), f32)
            for q in range(first, min(first + SUBLANES, qubits)):
                block = jnp.where(sub == q - first, angles[j, q], block)
            blocks.append(block)
        return jnp.concatenate(blocks, axis=0)

    theta, first, second = column(0), column(1), column(2)
    cosine, sine = jnp.cos(theta), jnp.sin(theta)
    joint = first + second
    return [
        cosine,
        jnp.zeros_like(cosine),
        -jnp.cos(second) * sine,
        -jnp.sin(second) * sine,
        jnp.cos(first) * sine,
        jnp.sin(first) * sine,
        jnp.cos(joint) * cosine,
        jnp.sin(joint) * cosine,
    ]


def leading_gate(xr, xi, bit, u):
    n, s, lanes = xr.shape
    shape = (n >> (bit + 1), 2, 1 << bit, s, lanes)
    xr, xi = xr.reshape(shape), xi.reshape(shape)
    ar, ai, br, bi = xr[:, 0], xi[:, 0], xr[:, 1], xi[:, 1]
    outs_r, outs_i = [], []
    for row in range(2):
        pr, pi, qr, qi = u[4 * row : 4 * row + 4]
        outs_r.append(pr * ar - pi * ai + (qr * br - qi * bi))
        outs_i.append(pr * ai + pi * ar + (qr * bi + qi * br))
    return (
        jnp.stack(outs_r, 1).reshape(n, s, lanes),
        jnp.stack(outs_i, 1).reshape(n, s, lanes),
    )


def sublane_gate(xr, xi, bit, u):
    step = 1 << bit
    high = ((iota((SUBLANES, LANES), 0) >> bit) & 1) == 1

    def swap(x):
        down = pltpu.roll(x, step, 1)
        if 2 * step == SUBLANES:
            return down
        return jnp.where(high[None], down, pltpu.roll(x, SUBLANES - step, 1))

    keep_r = jnp.where(high, u[6], u[0])[None]
    keep_i = jnp.where(high, u[7], u[1])[None]
    cross_r = jnp.where(high, u[4], u[2])[None]
    cross_i = jnp.where(high, u[5], u[3])[None]
    yr, yi = swap(xr), swap(xi)
    return (
        keep_r * xr - keep_i * xi + (cross_r * yr - cross_i * yi),
        keep_r * xi + keep_i * xr + (cross_r * yi + cross_i * yr),
    )


def lane_matrix(units):
    shape = (LANES, LANES)
    row, col = iota(shape, 0), iota(shape, 1)
    mr = mi = None
    for bit, u in enumerate(units):
        rb, cb = ((row >> bit) & 1) == 1, ((col >> bit) & 1) == 1
        gr = jnp.where(cb, jnp.where(rb, u[6], u[4]), jnp.where(rb, u[2], u[0]))
        gi = jnp.where(cb, jnp.where(rb, u[7], u[5]), jnp.where(rb, u[3], u[1]))
        if mr is None:
            mr, mi = gr, gi
        else:
            mr, mi = mr * gr - mi * gi, mr * gi + mi * gr
    return mr, mi


def row_matrix(units):
    shape = (LANES, LANES)
    row, col = iota(shape, 0), iota(shape, 1)
    mr = mi = None
    for bit, u in enumerate(units):
        rb, cb = ((row >> bit) & 1) == 1, ((col >> bit) & 1) == 1
        gr = jnp.where(rb, jnp.where(cb, u[6], u[4]), jnp.where(cb, u[2], u[0]))
        gi = jnp.where(rb, jnp.where(cb, u[7], u[5]), jnp.where(cb, u[3], u[1]))
        if mr is None:
            mr, mi = gr, gi
        else:
            mr, mi = mr * gr - mi * gi, mr * gi + mi * gr
    return mr, mi


def cut(x, depth):
    rows = x.shape[0]
    x = x.reshape(rows // SUBLANES, SUBLANES, LANES)
    per = SUBLANES // depth
    if per == 1:
        return x
    parts = [x[:, k * depth : (k + 1) * depth] for k in range(per)]
    return jnp.stack(parts, 1).reshape(rows // depth, depth, LANES)


def join(x):
    n, depth, _ = x.shape
    per = SUBLANES // depth
    if per > 1:
        x = x.reshape(n // per, per, depth, LANES)
        x = jnp.concatenate([x[:, k] for k in range(per)], axis=1)
    return x.reshape(n * depth, LANES)


def halves(x):
    top = x.astype(bf16)
    return top, (x - top.astype(f32)).astype(bf16)


def marked(row, value, count):
    shape = (2 * SUBLANES, LANES)
    wide = jnp.broadcast_to(row.astype(f32), shape).astype(bf16)
    value = jnp.broadcast_to(value.astype(f32), shape).astype(bf16)
    ids = iota((count, LANES), 0).astype(f32).astype(bf16).reshape(count // 16, 16, LANES)
    return jnp.where(ids == wide[None], value[None], jnp.zeros((), bf16)).reshape(count, LANES)


def one_hot(row, count):
    wide = jnp.broadcast_to(row.astype(f32), (16, LANES)).astype(bf16)
    ids = iota((count, LANES), 0).astype(f32).astype(bf16).reshape(count // 16, 16, LANES)
    hot = jnp.where(ids == wide[None], jnp.ones((), bf16), jnp.zeros((), bf16))
    return hot.reshape(count, LANES)


def split_table(table):
    flipped = table.T
    top, rest = halves(flipped)
    return jnp.concatenate([top, rest], axis=0)


def lookup(table, upper, lower):
    rows = upper.shape[0]
    count = table.shape[1]
    hot = jnp.concatenate([one_hot(upper[r : r + 1], count) for r in range(rows)], axis=1)
    both = jnp.dot(table, hot, preferred_element_type=f32)
    sub = iota((SUBLANES, LANES), 0)
    found = []
    for r in range(rows):
        part = slice(r * LANES, (r + 1) * LANES)
        value = (both[:LANES, part] + both[LANES:, part]).reshape(LANES // SUBLANES, SUBLANES, LANES)
        low = jnp.broadcast_to(lower[r : r + 1], (SUBLANES, LANES))
        for bit in (6, 5, 4, 3):
            half = value.shape[0] // 2
            value = jnp.where((((low >> bit) & 1) == 1)[None], value[half:], value[:half])
        value = jnp.where(sub == (low & (SUBLANES - 1)), value[0], 0.0)
        found.append(jnp.sum(value, axis=0, keepdims=True))
    return jnp.concatenate(found, axis=0)


def lookup_lanes(plain, upper, lower):
    bits = plain.shape[0].bit_length() - 1
    high = [((upper >> bit) & 1) == 1 for bit in range(bits)]

    def pick(first, bit):
        if bit < 0:
            line = jnp.broadcast_to(plain[first : first + 1], (SUBLANES, LANES))
            return jnp.take_along_axis(line, lower, axis=1, mode="promise_in_bounds")
        zero = pick(first, bit - 1)
        return jnp.where(high[bit], pick(first + (1 << bit), bit - 1), zero)

    return pick(0, bits - 1)


def lookup_both(table, plain, upper, lower, lanes):
    dots = upper.shape[0] - lanes
    found = [lookup(table, upper[:dots], lower[:dots])]
    for first in range(dots, dots + lanes, SUBLANES):
        part = slice(first, first + SUBLANES)
        value = lookup_lanes(plain, upper[part], lower[part])
        found.append(jnp.where(upper[part] >= 0, value, 0.0))
    return jnp.concatenate(found, axis=0)


def routes(me):
    parts = []
    rest = me
    for size in reversed(TORUS):
        parts.insert(0, lax.rem(rest, size))
        rest = rest // size
    scale = 1
    tables = []
    for part, size in zip(reversed(parts), reversed(TORUS)):
        tables.insert(0, [lax.rem(part + step, size) * scale for step in range(size)])
        scale *= size
    steps = list(itertools.product(*[range(size) for size in TORUS]))
    steps.sort(key=lambda step: -sum(min(d, n - d) for d, n in zip(step[:3], TORUS[:3])))
    upper = {(a, b): tables[0][a] + tables[1][b] for a in range(TORUS[0]) for b in range(TORUS[1])}
    lower = {(a, b): tables[2][a] + tables[3][b] for a in range(TORUS[2]) for b in range(TORUS[3])}
    return [upper[step[:2]] + lower[step[2:]] for step in steps if any(step)]


def kernel(
    sizes,
    angles_hbm,
    marg_hbm,
    state_hbm,
    owner_hbm,
    low_hbm,
    probs_ref,
    hist_ref,
    fid_ref,
    amp_out,
    amp_in,
    wt_out,
    wt_in,
    req_out,
    req_in,
    ans_out,
    ans_in,
    his_out,
    his_in,
    tot_out,
    tot_in,
    code_ref,
    rank_ref,
    req_ref,
    table_ref,
    plain_ref,
    global_ref,
    gates,
    angles,
    marg,
    state,
    owner_ref,
    low_ref,
    sends,
    recvs,
    loads,
):
    devices, depth, capacity_rows, marg_count = sizes
    me = lax.axis_index("dev")
    global_bits = devices.bit_length() - 1
    rows = state.shape[0] // 2
    row_bits = rows.bit_length() - 1
    local_bits = row_bits + 7
    codes = devices * capacity_rows

    peers = routes(me)
    inputs = [
        pltpu.make_async_copy(src, dst, loads.at[n])
        for n, (src, dst) in enumerate(
            (
                (angles_hbm, angles),
                (state_hbm, state),
                (owner_hbm, owner_ref),
                (low_hbm, low_ref),
                (marg_hbm, marg),
            )
        )
    ]
    for load in inputs:
        load.start()

    def copy(channel, src, dst, target):
        return pltpu.make_async_remote_copy(
            src_ref=src,
            dst_ref=dst,
            send_sem=sends.at[channel],
            recv_sem=recvs.at[channel],
            device_id=(target,),
            device_id_type=pl.DeviceIdType.MESH,
        )

    def scatter(channel, out, into):
        for target in peers:
            copy(channel, out.at[target], into.at[me], target).start()
        into[me] = out[me]

    def spread(channel, out, into):
        for target in peers:
            copy(channel, out.at[0], into.at[me], target).start()
        into[me] = out[0]

    def all_of(channel, into):
        many = into.at[pl.ds(0, devices - 1)]
        return copy(channel, many, many, peers[-1])

    barrier = pltpu.get_barrier_semaphore()

    for target in peers:
        pl.semaphore_signal(
            barrier, inc=1, device_id=(target,), device_id_type=pl.DeviceIdType.MESH
        )

    inputs[0].wait()
    for e, entry in enumerate(gate_rows(angles, global_bits + local_bits)):
        gates[e] = entry

    def unit(qubit):
        return [gates[e, qubit : qubit + 1] for e in range(8)]

    mr, mi = lane_matrix([unit(q) for q in range(7)])
    mixed = jnp.concatenate(
        [jnp.concatenate([mr, mi], axis=1), jnp.concatenate([-mi, mr], axis=1)], axis=0
    )
    inputs[1].wait()
    both = jnp.concatenate(
        [state[pl.ds(0, rows, stride=2)], state[pl.ds(1, rows, stride=2)]], axis=1
    )
    both = jnp.dot(both, mixed, precision=lax.Precision.HIGHEST, preferred_element_type=f32)
    xr = both[:, :LANES].reshape(rows // SUBLANES, SUBLANES, LANES)
    xi = both[:, LANES:].reshape(rows // SUBLANES, SUBLANES, LANES)
    for bit in range(3):
        xr, xi = sublane_gate(xr, xi, bit, unit(7 + bit))
    for bit in range(row_bits - 3):
        xr, xi = leading_gate(xr, xi, bit, unit(10 + bit))
    amp_out[:, 0] = cut(xr.reshape(rows, LANES), depth)
    amp_out[:, 1] = cut(xi.reshape(rows, LANES), depth)

    mr, mi = row_matrix([unit(local_bits + q) for q in range(global_bits)])
    mixed = jnp.concatenate(
        [jnp.concatenate([mr, -mi], axis=1), jnp.concatenate([mi, mr], axis=1)], axis=0
    )
    global_ref[0], global_ref[1] = halves(mixed)
    pl.semaphore_wait(barrier, devices - 1)
    scatter(0, amp_out, amp_in)

    samp_rows = owner_ref.shape[0]
    for load in inputs[2:]:
        load.wait()
    owner = owner_ref[...]
    owner_ids = iota((devices, LANES), 0)
    chunks = samp_rows // 2
    pieces = [one_hot(owner[r : r + 1], devices) for r in range(samp_rows)]
    stacked = jnp.concatenate(
        [jnp.concatenate(pieces[2 * c : 2 * c + 2], axis=1) for c in range(chunks)], axis=0
    )
    tri_shape = (2 * LANES, 3 * LANES)
    tri_row, tri_col = iota(tri_shape, 0), iota(tri_shape, 1)
    tri = ((tri_row < tri_col) | (tri_col >= 2 * LANES)).astype(f32).astype(bf16)
    counts = jnp.dot(stacked, tri, preferred_element_type=f32)
    before = jnp.zeros((devices, LANES), f32)
    ranks = []
    for c in range(chunks):
        block = counts[c * devices : (c + 1) * devices]
        for h in range(2):
            spot = block[:, h * LANES : (h + 1) * LANES] + before
            mine = owner_ids == owner[2 * c + h : 2 * c + h + 1]
            ranks.append(jnp.sum(jnp.where(mine, spot, 0.0), axis=0, keepdims=True))
        before = before + block[:, 2 * LANES :]
    ranking = jnp.concatenate(ranks, axis=0).astype(i32)
    code = owner * capacity_rows + (ranking >> 7)
    rank = ranking & (LANES - 1)
    code_ref[...] = code
    rank_ref[...] = rank

    low = low_ref[...] + 1
    tops, rests = low >> 8, low & 255
    placed = jnp.zeros((codes, 2 * LANES), f32)
    for first in range(0, samp_rows, 16):
        line = [slice(r, r + 1) for r in range(first, first + 16)]
        hot = jnp.concatenate([one_hot(code[r], codes) for r in line], axis=1)
        values = [
            jnp.concatenate([marked(rank[r], part[r], LANES) for r in line], axis=1)
            for part in (tops, rests)
        ]
        placed = placed + lax.dot_general(
            hot,
            jnp.concatenate(values, axis=0),
            (((1,), (1,)), ((), ())),
            preferred_element_type=f32,
        )
    wanted = (placed[:, :LANES] * 256.0 + placed[:, LANES:]).astype(i32) - 1
    req_out[...] = cut(wanted, capacity_rows)
    scatter(5, req_out, req_in)

    all_of(0, amp_in).wait_recv()
    both = jnp.concatenate(
        [
            jnp.concatenate([amp_in[:, part, d] for d in range(depth)], axis=1)
            for part in range(2)
        ],
        axis=0,
    )
    top, rest = halves(both)
    both = jnp.dot(global_ref[0], top, preferred_element_type=f32) + (
        jnp.dot(global_ref[0], rest, preferred_element_type=f32)
        + jnp.dot(global_ref[1], top, preferred_element_type=f32)
    )
    xr, xi = both[:devices], both[devices:]
    weight = xr * xr + xi * xi
    weights = [weight[:, d * LANES : (d + 1) * LANES] for d in range(depth)]
    for d in range(depth):
        wt_out[:, d] = weights[d]
    scatter(1, wt_out, wt_in)

    weight = jnp.concatenate(weights, axis=0)
    norm_part = jnp.sum(weight, axis=0, keepdims=True)
    owner_bits = devices.bit_length() - 1
    code_shape = (rows, LANES)
    row_id = iota(code_shape, 0)
    row_value = (
        ((row_id & (devices - 1)) << local_bits)
        + me * (depth * LANES)
        + ((row_id >> owner_bits) << 7)
    )
    lane_value = iota((LANES, LANES), 0)
    row_code = jnp.zeros(code_shape, i32)
    lane_code = jnp.zeros((LANES, LANES), i32)
    lane_mask = jnp.zeros((), i32)
    for k in range(marg_count):
        qubit = marg[0, k]
        row_code = row_code + (((row_value >> qubit) & 1) << k)
        lane_code = lane_code + (((lane_value >> qubit) & 1) << k)
        lane_mask = lane_mask + jnp.where(qubit < 7, 1 << k, 0)
    bins = 2**marg_count
    top, rest = halves(weight)
    split = jnp.concatenate([top, rest], axis=0)
    @pl.loop(0, bins // LANES)
    def _(c):
        bin_id = c * LANES + iota((1, LANES), 1)
        lane_part = bin_id & lane_mask
        lane_hot = (lane_code == lane_part).astype(f32).astype(bf16)
        folded = jnp.dot(split, lane_hot, preferred_element_type=f32)
        folded = folded[:rows] + folded[rows:]
        picked = jnp.where(row_code == bin_id - lane_part, folded, 0.0)
        his_out[c] = jnp.sum(picked, axis=0, keepdims=True)

    bin_share = devices * LANES // bins
    for target in peers:
        copy(4, his_out.at[target // bin_share], his_in.at[me], target).start()
    his_in[me] = his_out[me // bin_share]

    all_of(5, req_in).wait_recv()
    req_ref[...] = join(req_in[...])
    all_of(1, wt_in).wait_recv()
    plain_ref[0:rows] = join(wt_in[...])
    table_ref[:, 0:rows] = split_table(plain_ref[0:rows])
    group = 64 // capacity_rows
    groups = devices // group
    mine, spot = me // group, me % group

    def answer(turn):
        first = lax.rem(mine + turn, groups) * group
        window = pl.ds(pl.multiple_of(first * capacity_rows, SUBLANES), group * capacity_rows)
        wanted = req_ref[window]
        found = lookup_both(
            table_ref[:, 0:rows], plain_ref.at[0:rows], wanted >> 7, wanted & (LANES - 1), 24
        )
        ans_out[pl.ds(first, group)] = cut(found, capacity_rows)
        return first, jnp.sum(found, axis=0, keepdims=True)

    def reply(first, count):
        for j in range(1, count + 1):
            target = first + lax.rem(spot + j, group)
            copy(2, ans_out.at[target], ans_in.at[me], target).start()

    total = jnp.zeros((1, LANES), f32)
    before = None
    for turn in [*range(1, groups), 0]:
        if before is not None:
            reply(before, group)
        before, part = answer(turn)
        total = total + part
    reply(before, group - 1)
    half = iota((1, LANES), 1) < LANES // 2
    packed = [jnp.broadcast_to(x, (SUBLANES, LANES)) for x in (total, norm_part)]
    packed = [x + pltpu.roll(x, LANES // 2, 1) for x in packed]
    tot_out[0] = jnp.where(half, packed[0][0:1], packed[1][0:1])
    spread(3, tot_out, tot_in)
    ans_in[me] = ans_out[me]

    all_of(2, ans_in).wait_recv()
    plain_ref[0:codes] = join(ans_in[...])
    table_ref[:, 0:codes] = split_table(plain_ref[0:codes])
    for first in range(0, samp_rows, 32):
        window = slice(first, first + 32)
        probs_ref[window] = lookup_both(
            table_ref[:, 0:codes], plain_ref.at[0:codes], code_ref[window], rank_ref[window], 8
        )
    all_of(4, his_in).wait_recv()
    hist_ref[...] = jnp.sum(his_in[...], axis=0)
    all_of(3, tot_in).wait_recv()
    fid_ref[...] = jnp.sum(tot_in[...], axis=0)

    for channel, into in enumerate((amp_in, wt_in, ans_in, tot_in, his_in, req_in)):
        all_of(channel, into).wait_send()


def finish(sizes, values, hist, totals, probs_ref, mine_ref, fid_ref):
    amps_total, samples, bins = sizes
    mine = mine_ref.shape[1]
    start = lax.axis_index("dev") * mine
    line = totals[...]
    half = iota(line.shape, 1) < LANES // 2
    total = jnp.sum(jnp.where(half, line, 0.0), axis=1, keepdims=True)
    norm = jnp.sum(jnp.where(half, 0.0, line), axis=1, keepdims=True)
    probs_ref[...] = amps_total * (values[...] / norm)
    line = jnp.broadcast_to(hist[0:1], (SUBLANES, LANES))
    line = pltpu.roll(line, (LANES - start % LANES) % LANES, 1)
    mine_ref[...] = bins * (line[0:1, :mine] / norm)
    fid_ref[...] = amps_total * (total / norm) / samples - 1.0


def shards(state, angles, sample_high, sample_low, marginal_qubits):
    devices = lax.axis_size("dev")
    amps_local = state.shape[1]
    samp_local = sample_low.shape[0]
    marg_count = marginal_qubits.shape[0]
    bins = 2**marg_count
    depth = amps_local // devices // LANES
    capacity_rows = 4 * samp_local // devices // LANES
    rows = amps_local // LANES
    samp_rows = samp_local // LANES
    sizes = (
        devices,
        depth,
        capacity_rows,
        marg_count,
    )
    vmem = pl.BlockSpec(memory_space=pltpu.VMEM)
    codes = devices * capacity_rows
    bin_rows = bins // LANES
    values, hist, totals = pl.pallas_call(
        functools.partial(kernel, sizes),
        out_shape=(
            jax.ShapeDtypeStruct((samp_rows, LANES), f32),
            jax.ShapeDtypeStruct((1, LANES), f32),
            jax.ShapeDtypeStruct((1, LANES), f32),
        ),
        in_specs=[pl.BlockSpec(memory_space=pltpu.HBM)] * 5,
        out_specs=(vmem, vmem, vmem),
        scratch_shapes=[
            pltpu.VMEM((devices, 2, depth, LANES), f32),
            pltpu.VMEM((devices, 2, depth, LANES), f32),
            pltpu.VMEM((devices, depth, LANES), f32),
            pltpu.VMEM((devices, depth, LANES), f32),
            pltpu.VMEM((devices, capacity_rows, LANES), i32),
            pltpu.VMEM((devices, capacity_rows, LANES), i32),
            pltpu.VMEM((devices, capacity_rows, LANES), f32),
            pltpu.VMEM((devices, capacity_rows, LANES), f32),
            pltpu.VMEM((bin_rows, 1, LANES), f32),
            pltpu.VMEM((devices, 1, LANES), f32),
            pltpu.VMEM((1, 1, LANES), f32),
            pltpu.VMEM((devices, 1, LANES), f32),
            pltpu.VMEM((samp_rows, LANES), i32),
            pltpu.VMEM((samp_rows, LANES), i32),
            pltpu.VMEM((codes, LANES), i32),
            pltpu.VMEM((2 * LANES, max(rows, codes)), bf16),
            pltpu.VMEM((max(rows, codes), LANES), f32),
            pltpu.VMEM((2, 2 * devices, 2 * devices), bf16),
            pltpu.VMEM((8, -(-angles.shape[0] // SUBLANES) * SUBLANES, LANES), f32),
            pltpu.SMEM((angles.shape[1], angles.shape[0]), f32),
            pltpu.SMEM((1, marg_count), i32),
            pltpu.VMEM((2 * rows, LANES), f32),
            pltpu.VMEM((samp_rows, LANES), i32),
            pltpu.VMEM((samp_rows, LANES), i32),
            pltpu.SemaphoreType.DMA((6,)),
            pltpu.SemaphoreType.DMA((6,)),
            pltpu.SemaphoreType.DMA((5,)),
        ],
        compiler_params=pltpu.CompilerParams(
            collective_id=0, has_side_effects=True, vmem_limit_bytes=24 << 20
        ),
        name="circuit",
    )(
        pltpu.with_memory_space_constraint(angles.T, pltpu.HBM),
        pltpu.with_memory_space_constraint(marginal_qubits.reshape(1, marg_count), pltpu.HBM),
        pltpu.with_memory_space_constraint(state.reshape(2, rows, LANES).transpose(1, 0, 2).reshape(2 * rows, LANES), pltpu.HBM),
        pltpu.with_memory_space_constraint(sample_high.reshape(samp_rows, LANES), pltpu.HBM),
        pltpu.with_memory_space_constraint(sample_low.reshape(samp_rows, LANES), pltpu.HBM),
    )
    probs, mine, fid = pl.pallas_call(
        functools.partial(
            finish, (float(amps_local * devices), float(samp_local * devices), float(bins))
        ),
        out_shape=(
            jax.ShapeDtypeStruct((samp_rows, LANES), f32),
            jax.ShapeDtypeStruct((1, bins // devices), f32),
            jax.ShapeDtypeStruct((1, 1), f32),
        ),
        in_specs=[vmem, vmem, vmem],
        out_specs=(vmem, vmem, vmem),
        compiler_params=pltpu.CompilerParams(vmem_limit_bytes=1 << 20),
        name="finish",
    )(values, hist, totals)
    return probs.reshape(samp_local), mine.reshape(bins // devices), fid.reshape(())


def solution(mesh):
    return jax.shard_map(
        shards,
        mesh=mesh,
        in_specs=(P(None, "dev"), P(), P("dev", None), P("dev"), P()),
        out_specs=(P("dev"), P("dev"), P()),
        check_vma=False,
    )
```

```python
import functools
import itertools

import jax
import jax.numpy as jnp
from jax import lax
from jax.experimental import pallas as pl
from jax.experimental.pallas import tpu as pltpu
from jax.sharding import PartitionSpec as P

LANES = 128
SUBLANES = 8
TORUS = (4, 4, 4, 2)
f32 = jnp.float32
bf16 = jnp.bfloat16
i32 = jnp.int32


def iota(shape, dim):
    return lax.broadcasted_iota(i32, shape, dim)


def gate_rows(angles, qubits):
    sub = iota((SUBLANES, LANES), 0)

    def column(j):
        blocks = []
        for first in range(0, qubits, SUBLANES):
            block = jnp.zeros((SUBLANES, LANES), f32)
            for q in range(first, min(first + SUBLANES, qubits)):
                block = jnp.where(sub == q - first, angles[j, q], block)
            blocks.append(block)
        return jnp.concatenate(blocks, axis=0)

    theta, first, second = column(0), column(1), column(2)
    cosine, sine = jnp.cos(theta), jnp.sin(theta)
    joint = first + second
    return [
        cosine,
        jnp.zeros_like(cosine),
        -jnp.cos(second) * sine,
        -jnp.sin(second) * sine,
        jnp.cos(first) * sine,
        jnp.sin(first) * sine,
        jnp.cos(joint) * cosine,
        jnp.sin(joint) * cosine,
    ]


def leading_gate(xr, xi, bit, u):
    n, s, lanes = xr.shape
    shape = (n >> (bit + 1), 2, 1 << bit, s, lanes)
    xr, xi = xr.reshape(shape), xi.reshape(shape)
    ar, ai, br, bi = xr[:, 0], xi[:, 0], xr[:, 1], xi[:, 1]
    outs_r, outs_i = [], []
    for row in range(2):
        pr, pi, qr, qi = u[4 * row : 4 * row + 4]
        outs_r.append(pr * ar - pi * ai + (qr * br - qi * bi))
        outs_i.append(pr * ai + pi * ar + (qr * bi + qi * br))
    return (
        jnp.stack(outs_r, 1).reshape(n, s, lanes),
        jnp.stack(outs_i, 1).reshape(n, s, lanes),
    )


def sublane_gate(xr, xi, bit, u):
    step = 1 << bit
    high = ((iota((SUBLANES, LANES), 0) >> bit) & 1) == 1

    def swap(x):
        down = pltpu.roll(x, step, 1)
        if 2 * step == SUBLANES:
            return down
        return jnp.where(high[None], down, pltpu.roll(x, SUBLANES - step, 1))

    keep_r = jnp.where(high, u[6], u[0])[None]
    keep_i = jnp.where(high, u[7], u[1])[None]
    cross_r = jnp.where(high, u[4], u[2])[None]
    cross_i = jnp.where(high, u[5], u[3])[None]
    yr, yi = swap(xr), swap(xi)
    return (
        keep_r * xr - keep_i * xi + (cross_r * yr - cross_i * yi),
        keep_r * xi + keep_i * xr + (cross_r * yi + cross_i * yr),
    )


def lane_matrix(units):
    shape = (LANES, LANES)
    row, col = iota(shape, 0), iota(shape, 1)
    mr = mi = None
    for bit, u in enumerate(units):
        rb, cb = ((row >> bit) & 1) == 1, ((col >> bit) & 1) == 1
        gr = jnp.where(cb, jnp.where(rb, u[6], u[4]), jnp.where(rb, u[2], u[0]))
        gi = jnp.where(cb, jnp.where(rb, u[7], u[5]), jnp.where(rb, u[3], u[1]))
        if mr is None:
            mr, mi = gr, gi
        else:
            mr, mi = mr * gr - mi * gi, mr * gi + mi * gr
    return mr, mi


def row_matrix(units):
    shape = (LANES, LANES)
    row, col = iota(shape, 0), iota(shape, 1)
    mr = mi = None
    for bit, u in enumerate(units):
        rb, cb = ((row >> bit) & 1) == 1, ((col >> bit) & 1) == 1
        gr = jnp.where(rb, jnp.where(cb, u[6], u[4]), jnp.where(cb, u[2], u[0]))
        gi = jnp.where(rb, jnp.where(cb, u[7], u[5]), jnp.where(cb, u[3], u[1]))
        if mr is None:
            mr, mi = gr, gi
        else:
            mr, mi = mr * gr - mi * gi, mr * gi + mi * gr
    return mr, mi


def cut(x, depth):
    rows = x.shape[0]
    x = x.reshape(rows // SUBLANES, SUBLANES, LANES)
    per = SUBLANES // depth
    if per == 1:
        return x
    parts = [x[:, k * depth : (k + 1) * depth] for k in range(per)]
    return jnp.stack(parts, 1).reshape(rows // depth, depth, LANES)


def join(x):
    n, depth, _ = x.shape
    per = SUBLANES // depth
    if per > 1:
        x = x.reshape(n // per, per, depth, LANES)
        x = jnp.concatenate([x[:, k] for k in range(per)], axis=1)
    return x.reshape(n * depth, LANES)


def halves(x):
    top = x.astype(bf16)
    return top, (x - top.astype(f32)).astype(bf16)


def marked(row, value, count):
    shape = (2 * SUBLANES, LANES)
    wide = jnp.broadcast_to(row.astype(f32), shape).astype(bf16)
    value = jnp.broadcast_to(value.astype(f32), shape).astype(bf16)
    ids = iota((count, LANES), 0).astype(f32).astype(bf16).reshape(count // 16, 16, LANES)
    return jnp.where(ids == wide[None], value[None], jnp.zeros((), bf16)).reshape(count, LANES)


def one_hot(row, count):
    wide = jnp.broadcast_to(row.astype(f32), (16, LANES)).astype(bf16)
    ids = iota((count, LANES), 0).astype(f32).astype(bf16).reshape(count // 16, 16, LANES)
    hot = jnp.where(ids == wide[None], jnp.ones((), bf16), jnp.zeros((), bf16))
    return hot.reshape(count, LANES)


def split_table(table):
    flipped = table.T
    top, rest = halves(flipped)
    return jnp.concatenate([top, rest], axis=0)


def pick_lane(value, lower):
    value = value.reshape(LANES // SUBLANES, SUBLANES, LANES)
    low = jnp.broadcast_to(lower, (SUBLANES, LANES))
    for bit in (6, 5, 4, 3):
        half = value.shape[0] // 2
        value = jnp.where((((low >> bit) & 1) == 1)[None], value[half:], value[:half])
    sub = iota((SUBLANES, LANES), 0)
    value = jnp.where(sub == (low & (SUBLANES - 1)), value[0], 0.0)
    return jnp.sum(value, axis=0, keepdims=True)


def rows_dot(table, upper):
    count = table.shape[1]
    hot = [one_hot(upper[r : r + 1], count) for r in range(upper.shape[0])]
    both = jnp.dot(table, jnp.concatenate(hot, axis=1), preferred_element_type=f32)
    return both[:LANES] + both[LANES:]


def lookup(table, upper, lower):
    both = rows_dot(table, upper)
    found = [
        pick_lane(both[:, r * LANES : (r + 1) * LANES], lower[r : r + 1])
        for r in range(upper.shape[0])
    ]
    return jnp.concatenate(found, axis=0)


def lookup_lanes(plain, upper, lower):
    bits = plain.shape[0].bit_length() - 1
    high = [((upper >> bit) & 1) == 1 for bit in range(bits)]

    def pick(first, bit):
        if bit < 0:
            line = jnp.broadcast_to(plain[first : first + 1], (SUBLANES, LANES))
            return jnp.take_along_axis(line, lower, axis=1, mode="promise_in_bounds")
        zero = pick(first, bit - 1)
        return jnp.where(high[bit], pick(first + (1 << bit), bit - 1), zero)

    return pick(0, bits - 1)


def lookup_both(table, plain, upper, lower, lanes):
    dots = upper.shape[0] - lanes
    found = [lookup(table, upper[:dots], lower[:dots])]
    for first in range(dots, dots + lanes, SUBLANES):
        part = slice(first, first + SUBLANES)
        value = lookup_lanes(plain, upper[part], lower[part])
        found.append(jnp.where(upper[part] >= 0, value, 0.0))
    return jnp.concatenate(found, axis=0)


def routes(me):
    parts = []
    rest = me
    for size in reversed(TORUS):
        parts.insert(0, lax.rem(rest, size))
        rest = rest // size
    scale = 1
    tables = []
    for part, size in zip(reversed(parts), reversed(TORUS)):
        tables.insert(0, [lax.rem(part + step, size) * scale for step in range(size)])
        scale *= size
    steps = list(itertools.product(*[range(size) for size in TORUS]))
    steps.sort(key=lambda step: -sum(min(d, n - d) for d, n in zip(step[:3], TORUS[:3])))
    upper = {(a, b): tables[0][a] + tables[1][b] for a in range(TORUS[0]) for b in range(TORUS[1])}
    lower = {(a, b): tables[2][a] + tables[3][b] for a in range(TORUS[2]) for b in range(TORUS[3])}
    return [upper[step[:2]] + lower[step[2:]] for step in steps if any(step)]


def kernel(
    sizes,
    angles_hbm,
    marg_hbm,
    state_hbm,
    owner_hbm,
    low_hbm,
    probs_ref,
    hist_ref,
    fid_ref,
    amp_out,
    amp_in,
    wt_out,
    wt_in,
    req_out,
    req_in,
    ans_out,
    ans_in,
    his_out,
    his_in,
    tot_out,
    tot_in,
    code_ref,
    rank_ref,
    req_ref,
    table_ref,
    plain_ref,
    both_ref,
    side_ref,
    global_ref,
    gates,
    angles,
    marg,
    state,
    owner_ref,
    low_ref,
    sends,
    recvs,
    loads,
):
    devices, depth, capacity_rows, marg_count = sizes
    me = lax.axis_index("dev")
    global_bits = devices.bit_length() - 1
    rows = state.shape[0] // 2
    row_bits = rows.bit_length() - 1
    local_bits = row_bits + 7
    codes = devices * capacity_rows

    peers = routes(me)
    inputs = [
        pltpu.make_async_copy(src, dst, loads.at[n])
        for n, (src, dst) in enumerate(
            (
                (angles_hbm, angles),
                (state_hbm, state),
                (owner_hbm, owner_ref),
                (low_hbm, low_ref),
                (marg_hbm, marg),
            )
        )
    ]
    for load in inputs:
        load.start()

    def copy(channel, src, dst, target):
        return pltpu.make_async_remote_copy(
            src_ref=src,
            dst_ref=dst,
            send_sem=sends.at[channel],
            recv_sem=recvs.at[channel],
            device_id=(target,),
            device_id_type=pl.DeviceIdType.MESH,
        )

    def scatter(channel, out, into):
        for target in peers:
            copy(channel, out.at[target], into.at[me], target).start()
        into[me] = out[me]

    def spread(channel, out, into):
        for target in peers:
            copy(channel, out.at[0], into.at[me], target).start()
        into[me] = out[0]

    def all_of(channel, into):
        many = into.at[pl.ds(0, devices - 1)]
        return copy(channel, many, many, peers[-1])

    barrier = pltpu.get_barrier_semaphore()

    for target in peers:
        pl.semaphore_signal(
            barrier, inc=1, device_id=(target,), device_id_type=pl.DeviceIdType.MESH
        )

    inputs[0].wait()
    for e, entry in enumerate(gate_rows(angles, global_bits + local_bits)):
        gates[e] = entry

    def unit(qubit):
        return [gates[e, qubit : qubit + 1] for e in range(8)]

    mr, mi = lane_matrix([unit(q) for q in range(7)])
    mixed = jnp.concatenate(
        [jnp.concatenate([mr, mi], axis=1), jnp.concatenate([-mi, mr], axis=1)], axis=0
    )
    inputs[1].wait()
    both = jnp.concatenate(
        [state[pl.ds(0, rows, stride=2)], state[pl.ds(1, rows, stride=2)]], axis=1
    )
    both = jnp.dot(both, mixed, precision=lax.Precision.HIGHEST, preferred_element_type=f32)
    xr = both[:, :LANES].reshape(rows // SUBLANES, SUBLANES, LANES)
    xi = both[:, LANES:].reshape(rows // SUBLANES, SUBLANES, LANES)
    for bit in range(3):
        xr, xi = sublane_gate(xr, xi, bit, unit(7 + bit))
    for bit in range(row_bits - 3):
        xr, xi = leading_gate(xr, xi, bit, unit(10 + bit))
    amp_out[:, 0] = cut(xr.reshape(rows, LANES), depth)
    amp_out[:, 1] = cut(xi.reshape(rows, LANES), depth)

    mr, mi = row_matrix([unit(local_bits + q) for q in range(global_bits)])
    mixed = jnp.concatenate(
        [jnp.concatenate([mr, -mi], axis=1), jnp.concatenate([mi, mr], axis=1)], axis=0
    )
    global_ref[0], global_ref[1] = halves(mixed)
    pl.semaphore_wait(barrier, devices - 1)
    scatter(0, amp_out, amp_in)

    samp_rows = owner_ref.shape[0]
    for load in inputs[2:]:
        load.wait()
    owner = owner_ref[...]
    owner_ids = iota((devices, LANES), 0)
    chunks = samp_rows // 2
    pieces = [one_hot(owner[r : r + 1], devices) for r in range(samp_rows)]
    stacked = jnp.concatenate(
        [jnp.concatenate(pieces[2 * c : 2 * c + 2], axis=1) for c in range(chunks)], axis=0
    )
    tri_shape = (2 * LANES, 3 * LANES)
    tri_row, tri_col = iota(tri_shape, 0), iota(tri_shape, 1)
    tri = ((tri_row < tri_col) | (tri_col >= 2 * LANES)).astype(f32).astype(bf16)
    counts = jnp.dot(stacked, tri, preferred_element_type=f32)
    before = jnp.zeros((devices, LANES), f32)
    ranks = []
    for c in range(chunks):
        block = counts[c * devices : (c + 1) * devices]
        for h in range(2):
            spot = block[:, h * LANES : (h + 1) * LANES] + before
            mine = owner_ids == owner[2 * c + h : 2 * c + h + 1]
            ranks.append(jnp.sum(jnp.where(mine, spot, 0.0), axis=0, keepdims=True))
        before = before + block[:, 2 * LANES :]
    ranking = jnp.concatenate(ranks, axis=0).astype(i32)
    code = owner * capacity_rows + (ranking >> 7)
    rank = ranking & (LANES - 1)
    code_ref[...] = code
    rank_ref[...] = rank

    low = low_ref[...] + 1
    tops, rests = low >> 8, low & 255
    placed = jnp.zeros((codes, 2 * LANES), f32)
    for first in range(0, samp_rows, 16):
        line = [slice(r, r + 1) for r in range(first, first + 16)]
        hot = jnp.concatenate([one_hot(code[r], codes) for r in line], axis=1)
        values = [
            jnp.concatenate([marked(rank[r], part[r], LANES) for r in line], axis=1)
            for part in (tops, rests)
        ]
        placed = placed + lax.dot_general(
            hot,
            jnp.concatenate(values, axis=0),
            (((1,), (1,)), ((), ())),
            preferred_element_type=f32,
        )
    wanted = (placed[:, :LANES] * 256.0 + placed[:, LANES:]).astype(i32) - 1
    req_out[...] = cut(wanted, capacity_rows)
    scatter(5, req_out, req_in)

    all_of(0, amp_in).wait_recv()
    both = jnp.concatenate(
        [
            jnp.concatenate([amp_in[:, part, d] for d in range(depth)], axis=1)
            for part in range(2)
        ],
        axis=0,
    )
    top, rest = halves(both)
    both = jnp.dot(global_ref[0], top, preferred_element_type=f32) + (
        jnp.dot(global_ref[0], rest, preferred_element_type=f32)
        + jnp.dot(global_ref[1], top, preferred_element_type=f32)
    )
    xr, xi = both[:devices], both[devices:]
    weight = xr * xr + xi * xi
    weights = [weight[:, d * LANES : (d + 1) * LANES] for d in range(depth)]
    for d in range(depth):
        wt_out[:, d] = weights[d]
    scatter(1, wt_out, wt_in)

    weight = jnp.concatenate(weights, axis=0)
    norm_part = jnp.sum(weight, axis=0, keepdims=True)
    owner_bits = devices.bit_length() - 1
    code_shape = (rows, LANES)
    row_id = iota(code_shape, 0)
    row_value = (
        ((row_id & (devices - 1)) << local_bits)
        + me * (depth * LANES)
        + ((row_id >> owner_bits) << 7)
    )
    lane_value = iota((LANES, LANES), 0)
    row_code = jnp.zeros(code_shape, i32)
    lane_code = jnp.zeros((LANES, LANES), i32)
    lane_mask = jnp.zeros((), i32)
    for k in range(marg_count):
        qubit = marg[0, k]
        row_code = row_code + (((row_value >> qubit) & 1) << k)
        lane_code = lane_code + (((lane_value >> qubit) & 1) << k)
        lane_mask = lane_mask + jnp.where(qubit < 7, 1 << k, 0)
    bins = 2**marg_count
    top, rest = halves(weight)
    split = jnp.concatenate([top, rest], axis=0)
    @pl.loop(0, bins // LANES)
    def _(c):
        bin_id = c * LANES + iota((1, LANES), 1)
        lane_part = bin_id & lane_mask
        lane_hot = (lane_code == lane_part).astype(f32).astype(bf16)
        folded = jnp.dot(split, lane_hot, preferred_element_type=f32)
        folded = folded[:rows] + folded[rows:]
        picked = jnp.where(row_code == bin_id - lane_part, folded, 0.0)
        his_out[c] = jnp.sum(picked, axis=0, keepdims=True)

    bin_share = devices * LANES // bins
    for target in peers:
        copy(4, his_out.at[target // bin_share], his_in.at[me], target).start()
    his_in[me] = his_out[me // bin_share]

    all_of(5, req_in).wait_recv()
    req_ref[...] = join(req_in[...])
    all_of(1, wt_in).wait_recv()
    plain_ref[0:rows] = join(wt_in[...])
    table_ref[:, 0:rows] = split_table(plain_ref[0:rows])
    group = 32 // capacity_rows
    groups = devices // group
    mine, spot = me // group, me % group

    dots = 32 - 8

    def place_of(turn):
        first = lax.rem(mine + turn, groups) * group
        start = pl.multiple_of(first * capacity_rows, SUBLANES)
        return first, req_ref[pl.ds(start, group * capacity_rows)]

    def begin(turn, slot):
        _, wanted = place_of(turn)
        upper, lower = wanted >> 7, wanted & (LANES - 1)
        both_ref[slot] = rows_dot(table_ref[:, 0:rows], upper[:dots])
        for first in range(dots, 32, SUBLANES):
            part = slice(first, first + SUBLANES)
            value = lookup_lanes(plain_ref.at[0:rows], upper[part], lower[part])
            side_ref[slot, first - dots : first - dots + SUBLANES] = jnp.where(
                upper[part] >= 0, value, 0.0
            )

    def answer(turn, slot):
        first, wanted = place_of(turn)
        lower = wanted & (LANES - 1)
        found = [
            pick_lane(both_ref[slot, :, r * LANES : (r + 1) * LANES], lower[r : r + 1])
            for r in range(dots)
        ]
        found = jnp.concatenate([*found, side_ref[slot]], axis=0)
        ans_out[pl.ds(first, group)] = cut(found, capacity_rows)
        return first, jnp.sum(found, axis=0, keepdims=True)

    def reply(first, count):
        for j in range(1, count + 1):
            target = first + lax.rem(spot + j, group)
            copy(2, ans_out.at[target], ans_in.at[me], target).start()

    total = jnp.zeros((1, LANES), f32)
    turns = [*range(1, groups), 0]
    begin(turns[0], 0)
    for n, turn in enumerate(turns):
        if n + 1 < groups:
            begin(turns[n + 1], (n + 1) % 2)
        before, extra = answer(turn, n % 2)
        total = total + extra
        if n + 1 < groups:
            reply(before, group)
    reply(before, group - 1)
    half = iota((1, LANES), 1) < LANES // 2
    packed = [jnp.broadcast_to(x, (SUBLANES, LANES)) for x in (total, norm_part)]
    packed = [x + pltpu.roll(x, LANES // 2, 1) for x in packed]
    tot_out[0] = jnp.where(half, packed[0][0:1], packed[1][0:1])
    spread(3, tot_out, tot_in)
    ans_in[me] = ans_out[me]

    all_of(2, ans_in).wait_recv()
    plain_ref[0:codes] = join(ans_in[...])
    table_ref[:, 0:codes] = split_table(plain_ref[0:codes])
    for first in range(0, samp_rows, 32):
        window = slice(first, first + 32)
        probs_ref[window] = lookup_both(
            table_ref[:, 0:codes], plain_ref.at[0:codes], code_ref[window], rank_ref[window], 8
        )
    all_of(4, his_in).wait_recv()
    hist_ref[...] = jnp.sum(his_in[...], axis=0)
    all_of(3, tot_in).wait_recv()
    fid_ref[...] = jnp.sum(tot_in[...], axis=0)

    for channel, into in enumerate((amp_in, wt_in, ans_in, tot_in, his_in, req_in)):
        all_of(channel, into).wait_send()


def finish(sizes, values, hist, totals, probs_ref, mine_ref, fid_ref):
    amps_total, samples, bins = sizes
    mine = mine_ref.shape[1]
    start = lax.axis_index("dev") * mine
    line = totals[...]
    half = iota(line.shape, 1) < LANES // 2
    total = jnp.sum(jnp.where(half, line, 0.0), axis=1, keepdims=True)
    norm = jnp.sum(jnp.where(half, 0.0, line), axis=1, keepdims=True)
    probs_ref[...] = amps_total * (values[...] / norm)
    line = jnp.broadcast_to(hist[0:1], (SUBLANES, LANES))
    line = pltpu.roll(line, (LANES - start % LANES) % LANES, 1)
    mine_ref[...] = bins * (line[0:1, :mine] / norm)
    fid_ref[...] = amps_total * (total / norm) / samples - 1.0


def shards(state, angles, sample_high, sample_low, marginal_qubits):
    devices = lax.axis_size("dev")
    amps_local = state.shape[1]
    samp_local = sample_low.shape[0]
    marg_count = marginal_qubits.shape[0]
    bins = 2**marg_count
    depth = amps_local // devices // LANES
    capacity_rows = 4 * samp_local // devices // LANES
    rows = amps_local // LANES
    samp_rows = samp_local // LANES
    sizes = (
        devices,
        depth,
        capacity_rows,
        marg_count,
    )
    vmem = pl.BlockSpec(memory_space=pltpu.VMEM)
    codes = devices * capacity_rows
    bin_rows = bins // LANES
    values, hist, totals = pl.pallas_call(
        functools.partial(kernel, sizes),
        out_shape=(
            jax.ShapeDtypeStruct((samp_rows, LANES), f32),
            jax.ShapeDtypeStruct((1, LANES), f32),
            jax.ShapeDtypeStruct((1, LANES), f32),
        ),
        in_specs=[pl.BlockSpec(memory_space=pltpu.HBM)] * 5,
        out_specs=(vmem, vmem, vmem),
        scratch_shapes=[
            pltpu.VMEM((devices, 2, depth, LANES), f32),
            pltpu.VMEM((devices, 2, depth, LANES), f32),
            pltpu.VMEM((devices, depth, LANES), f32),
            pltpu.VMEM((devices, depth, LANES), f32),
            pltpu.VMEM((devices, capacity_rows, LANES), i32),
            pltpu.VMEM((devices, capacity_rows, LANES), i32),
            pltpu.VMEM((devices, capacity_rows, LANES), f32),
            pltpu.VMEM((devices, capacity_rows, LANES), f32),
            pltpu.VMEM((bin_rows, 1, LANES), f32),
            pltpu.VMEM((devices, 1, LANES), f32),
            pltpu.VMEM((1, 1, LANES), f32),
            pltpu.VMEM((devices, 1, LANES), f32),
            pltpu.VMEM((samp_rows, LANES), i32),
            pltpu.VMEM((samp_rows, LANES), i32),
            pltpu.VMEM((codes, LANES), i32),
            pltpu.VMEM((2 * LANES, max(rows, codes)), bf16),
            pltpu.VMEM((max(rows, codes), LANES), f32),
            pltpu.VMEM((2, LANES, (32 - 8) * LANES), f32),
            pltpu.VMEM((2, 8, LANES), f32),
            pltpu.VMEM((2, 2 * devices, 2 * devices), bf16),
            pltpu.VMEM((8, -(-angles.shape[0] // SUBLANES) * SUBLANES, LANES), f32),
            pltpu.SMEM((angles.shape[1], angles.shape[0]), f32),
            pltpu.SMEM((1, marg_count), i32),
            pltpu.VMEM((2 * rows, LANES), f32),
            pltpu.VMEM((samp_rows, LANES), i32),
            pltpu.VMEM((samp_rows, LANES), i32),
            pltpu.SemaphoreType.DMA((6,)),
            pltpu.SemaphoreType.DMA((6,)),
            pltpu.SemaphoreType.DMA((5,)),
        ],
        compiler_params=pltpu.CompilerParams(
            collective_id=0, has_side_effects=True, vmem_limit_bytes=24 << 20
        ),
        name="circuit",
    )(
        pltpu.with_memory_space_constraint(angles.T, pltpu.HBM),
        pltpu.with_memory_space_constraint(marginal_qubits.reshape(1, marg_count), pltpu.HBM),
        pltpu.with_memory_space_constraint(state.reshape(2, rows, LANES).transpose(1, 0, 2).reshape(2 * rows, LANES), pltpu.HBM),
        pltpu.with_memory_space_constraint(sample_high.reshape(samp_rows, LANES), pltpu.HBM),
        pltpu.with_memory_space_constraint(sample_low.reshape(samp_rows, LANES), pltpu.HBM),
    )
    probs, mine, fid = pl.pallas_call(
        functools.partial(
            finish, (float(amps_local * devices), float(samp_local * devices), float(bins))
        ),
        out_shape=(
            jax.ShapeDtypeStruct((samp_rows, LANES), f32),
            jax.ShapeDtypeStruct((1, bins // devices), f32),
            jax.ShapeDtypeStruct((1, 1), f32),
        ),
        in_specs=[vmem, vmem, vmem],
        out_specs=(vmem, vmem, vmem),
        compiler_params=pltpu.CompilerParams(vmem_limit_bytes=1 << 20),
        name="finish",
    )(values, hist, totals)
    return probs.reshape(samp_local), mine.reshape(bins // devices), fid.reshape(())


def solution(mesh):
    return jax.shard_map(
        shards,
        mesh=mesh,
        in_specs=(P(None, "dev"), P(), P("dev", None), P("dev"), P()),
        out_specs=(P("dev"), P("dev"), P()),
        check_vma=False,
    )
```

```python
import functools
import itertools
import random

import jax
import jax.numpy as jnp
from jax import lax
from jax.experimental import pallas as pl
from jax.experimental.pallas import tpu as pltpu
from jax.sharding import PartitionSpec as P

LANES = 128
SUBLANES = 8
TORUS = (4, 4, 4, 2)
f32 = jnp.float32
bf16 = jnp.bfloat16
i32 = jnp.int32


def iota(shape, dim):
    return lax.broadcasted_iota(i32, shape, dim)


def gate_rows(angles, qubits):
    sub = iota((SUBLANES, LANES), 0)

    def column(j):
        blocks = []
        for first in range(0, qubits, SUBLANES):
            block = jnp.zeros((SUBLANES, LANES), f32)
            for q in range(first, min(first + SUBLANES, qubits)):
                block = jnp.where(sub == q - first, angles[j, q], block)
            blocks.append(block)
        return jnp.concatenate(blocks, axis=0)

    theta, first, second = column(0), column(1), column(2)
    cosine, sine = jnp.cos(theta), jnp.sin(theta)
    joint = first + second
    return [
        cosine,
        jnp.zeros_like(cosine),
        -jnp.cos(second) * sine,
        -jnp.sin(second) * sine,
        jnp.cos(first) * sine,
        jnp.sin(first) * sine,
        jnp.cos(joint) * cosine,
        jnp.sin(joint) * cosine,
    ]


def leading_gate(xr, xi, bit, u):
    n, s, lanes = xr.shape
    shape = (n >> (bit + 1), 2, 1 << bit, s, lanes)
    xr, xi = xr.reshape(shape), xi.reshape(shape)
    ar, ai, br, bi = xr[:, 0], xi[:, 0], xr[:, 1], xi[:, 1]
    outs_r, outs_i = [], []
    for row in range(2):
        pr, pi, qr, qi = u[4 * row : 4 * row + 4]
        outs_r.append(pr * ar - pi * ai + (qr * br - qi * bi))
        outs_i.append(pr * ai + pi * ar + (qr * bi + qi * br))
    return (
        jnp.stack(outs_r, 1).reshape(n, s, lanes),
        jnp.stack(outs_i, 1).reshape(n, s, lanes),
    )


def sublane_gate(xr, xi, bit, u):
    step = 1 << bit
    high = ((iota((SUBLANES, LANES), 0) >> bit) & 1) == 1

    def swap(x):
        down = pltpu.roll(x, step, 1)
        if 2 * step == SUBLANES:
            return down
        return jnp.where(high[None], down, pltpu.roll(x, SUBLANES - step, 1))

    keep_r = jnp.where(high, u[6], u[0])[None]
    keep_i = jnp.where(high, u[7], u[1])[None]
    cross_r = jnp.where(high, u[4], u[2])[None]
    cross_i = jnp.where(high, u[5], u[3])[None]
    yr, yi = swap(xr), swap(xi)
    return (
        keep_r * xr - keep_i * xi + (cross_r * yr - cross_i * yi),
        keep_r * xi + keep_i * xr + (cross_r * yi + cross_i * yr),
    )


def lane_matrix(units):
    shape = (LANES, LANES)
    row, col = iota(shape, 0), iota(shape, 1)
    mr = mi = None
    for bit, u in enumerate(units):
        rb, cb = ((row >> bit) & 1) == 1, ((col >> bit) & 1) == 1
        gr = jnp.where(cb, jnp.where(rb, u[6], u[4]), jnp.where(rb, u[2], u[0]))
        gi = jnp.where(cb, jnp.where(rb, u[7], u[5]), jnp.where(rb, u[3], u[1]))
        if mr is None:
            mr, mi = gr, gi
        else:
            mr, mi = mr * gr - mi * gi, mr * gi + mi * gr
    return mr, mi


def row_matrix(units):
    shape = (LANES, LANES)
    row, col = iota(shape, 0), iota(shape, 1)
    mr = mi = None
    for bit, u in enumerate(units):
        rb, cb = ((row >> bit) & 1) == 1, ((col >> bit) & 1) == 1
        gr = jnp.where(rb, jnp.where(cb, u[6], u[4]), jnp.where(cb, u[2], u[0]))
        gi = jnp.where(rb, jnp.where(cb, u[7], u[5]), jnp.where(cb, u[3], u[1]))
        if mr is None:
            mr, mi = gr, gi
        else:
            mr, mi = mr * gr - mi * gi, mr * gi + mi * gr
    return mr, mi


def cut(x, depth):
    rows = x.shape[0]
    x = x.reshape(rows // SUBLANES, SUBLANES, LANES)
    per = SUBLANES // depth
    if per == 1:
        return x
    parts = [x[:, k * depth : (k + 1) * depth] for k in range(per)]
    return jnp.stack(parts, 1).reshape(rows // depth, depth, LANES)


def join(x):
    n, depth, _ = x.shape
    per = SUBLANES // depth
    if per > 1:
        x = x.reshape(n // per, per, depth, LANES)
        x = jnp.concatenate([x[:, k] for k in range(per)], axis=1)
    return x.reshape(n * depth, LANES)


def halves(x):
    top = x.astype(bf16)
    return top, (x - top.astype(f32)).astype(bf16)


def marked(row, value, count):
    shape = (2 * SUBLANES, LANES)
    wide = jnp.broadcast_to(row.astype(f32), shape).astype(bf16)
    value = jnp.broadcast_to(value.astype(f32), shape).astype(bf16)
    ids = iota((count, LANES), 0).astype(f32).astype(bf16).reshape(count // 16, 16, LANES)
    return jnp.where(ids == wide[None], value[None], jnp.zeros((), bf16)).reshape(count, LANES)


def one_hot(row, count):
    wide = jnp.broadcast_to(row.astype(f32), (16, LANES)).astype(bf16)
    ids = iota((count, LANES), 0).astype(f32).astype(bf16).reshape(count // 16, 16, LANES)
    hot = jnp.where(ids == wide[None], jnp.ones((), bf16), jnp.zeros((), bf16))
    return hot.reshape(count, LANES)


def split_table(table):
    flipped = table.T
    top, rest = halves(flipped)
    return jnp.concatenate([top, rest], axis=0)


def pick_lane(value, lower):
    value = value.reshape(LANES // SUBLANES, SUBLANES, LANES)
    low = jnp.broadcast_to(lower, (SUBLANES, LANES))
    for bit in (6, 5, 4, 3):
        half = value.shape[0] // 2
        value = jnp.where((((low >> bit) & 1) == 1)[None], value[half:], value[:half])
    sub = iota((SUBLANES, LANES), 0)
    value = jnp.where(sub == (low & (SUBLANES - 1)), value[0], 0.0)
    return jnp.sum(value, axis=0, keepdims=True)


def rows_dot(table, upper):
    count = table.shape[1]
    hot = [one_hot(upper[r : r + 1], count) for r in range(upper.shape[0])]
    both = jnp.dot(table, jnp.concatenate(hot, axis=1), preferred_element_type=f32)
    return both[:LANES] + both[LANES:]


def lookup(table, upper, lower):
    both = rows_dot(table, upper)
    found = [
        pick_lane(both[:, r * LANES : (r + 1) * LANES], lower[r : r + 1])
        for r in range(upper.shape[0])
    ]
    return jnp.concatenate(found, axis=0)


def lookup_lanes(plain, upper, lower):
    bits = plain.shape[0].bit_length() - 1
    high = [((upper >> bit) & 1) == 1 for bit in range(bits)]

    def pick(first, bit):
        if bit < 0:
            line = jnp.broadcast_to(plain[first : first + 1], (SUBLANES, LANES))
            return jnp.take_along_axis(line, lower, axis=1, mode="promise_in_bounds")
        zero = pick(first, bit - 1)
        return jnp.where(high[bit], pick(first + (1 << bit), bit - 1), zero)

    return pick(0, bits - 1)


def lookup_both(table, plain, upper, lower, lanes):
    dots = upper.shape[0] - lanes
    found = [lookup(table, upper[:dots], lower[:dots])]
    for first in range(dots, dots + lanes, SUBLANES):
        part = slice(first, first + SUBLANES)
        value = lookup_lanes(plain, upper[part], lower[part])
        found.append(jnp.where(upper[part] >= 0, value, 0.0))
    return jnp.concatenate(found, axis=0)


def routes(me):
    parts = []
    rest = me
    for size in reversed(TORUS):
        parts.insert(0, lax.rem(rest, size))
        rest = rest // size
    scale = 1
    tables = []
    for part, size in zip(reversed(parts), reversed(TORUS)):
        tables.insert(0, [lax.rem(part + step, size) * scale for step in range(size)])
        scale *= size
    steps = [step for step in itertools.product(*[range(size) for size in TORUS]) if any(step)]
    random.Random(1).shuffle(steps)
    steps.sort(key=lambda step: -sum(min(d, n - d) for d, n in zip(step[:3], TORUS[:3])))
    upper = {(a, b): tables[0][a] + tables[1][b] for a in range(TORUS[0]) for b in range(TORUS[1])}
    lower = {(a, b): tables[2][a] + tables[3][b] for a in range(TORUS[2]) for b in range(TORUS[3])}
    return [upper[step[:2]] + lower[step[2:]] for step in steps]


def kernel(
    sizes,
    angles_hbm,
    marg_hbm,
    state_hbm,
    owner_hbm,
    low_hbm,
    probs_ref,
    hist_ref,
    fid_ref,
    amp_out,
    amp_in,
    wt_out,
    wt_in,
    req_out,
    req_in,
    ans_out,
    ans_in,
    his_out,
    his_in,
    tot_out,
    tot_in,
    code_ref,
    rank_ref,
    req_ref,
    table_ref,
    plain_ref,
    both_ref,
    side_ref,
    global_ref,
    gates,
    angles,
    marg,
    state,
    owner_ref,
    low_ref,
    sends,
    recvs,
    loads,
):
    devices, depth, capacity_rows, marg_count = sizes
    me = lax.axis_index("dev")
    global_bits = devices.bit_length() - 1
    rows = state.shape[0] // 2
    row_bits = rows.bit_length() - 1
    local_bits = row_bits + 7
    codes = devices * capacity_rows

    peers = routes(me)
    inputs = [
        pltpu.make_async_copy(src, dst, loads.at[n])
        for n, (src, dst) in enumerate(
            (
                (angles_hbm, angles),
                (state_hbm, state),
                (owner_hbm, owner_ref),
                (low_hbm, low_ref),
                (marg_hbm, marg),
            )
        )
    ]
    for load in inputs:
        load.start()

    def copy(channel, src, dst, target):
        return pltpu.make_async_remote_copy(
            src_ref=src,
            dst_ref=dst,
            send_sem=sends.at[channel],
            recv_sem=recvs.at[channel],
            device_id=(target,),
            device_id_type=pl.DeviceIdType.MESH,
        )

    def scatter(channel, out, into):
        for target in peers:
            copy(channel, out.at[target], into.at[me], target).start()
        into[me] = out[me]

    def spread(channel, out, into):
        for target in peers:
            copy(channel, out.at[0], into.at[me], target).start()
        into[me] = out[0]

    def all_of(channel, into):
        many = into.at[pl.ds(0, devices - 1)]
        return copy(channel, many, many, peers[-1])

    barrier = pltpu.get_barrier_semaphore()

    for target in peers:
        pl.semaphore_signal(
            barrier, inc=1, device_id=(target,), device_id_type=pl.DeviceIdType.MESH
        )

    inputs[0].wait()
    for e, entry in enumerate(gate_rows(angles, global_bits + local_bits)):
        gates[e] = entry

    def unit(qubit):
        return [gates[e, qubit : qubit + 1] for e in range(8)]

    mr, mi = lane_matrix([unit(q) for q in range(7)])
    mixed = jnp.concatenate(
        [jnp.concatenate([mr, mi], axis=1), jnp.concatenate([-mi, mr], axis=1)], axis=0
    )
    inputs[1].wait()
    both = jnp.concatenate(
        [state[pl.ds(0, rows, stride=2)], state[pl.ds(1, rows, stride=2)]], axis=1
    )
    both = jnp.dot(both, mixed, precision=lax.Precision.HIGHEST, preferred_element_type=f32)
    xr = both[:, :LANES].reshape(rows // SUBLANES, SUBLANES, LANES)
    xi = both[:, LANES:].reshape(rows // SUBLANES, SUBLANES, LANES)
    for bit in range(3):
        xr, xi = sublane_gate(xr, xi, bit, unit(7 + bit))
    for bit in range(row_bits - 3):
        xr, xi = leading_gate(xr, xi, bit, unit(10 + bit))
    amp_out[:, 0] = cut(xr.reshape(rows, LANES), depth)
    amp_out[:, 1] = cut(xi.reshape(rows, LANES), depth)

    mr, mi = row_matrix([unit(local_bits + q) for q in range(global_bits)])
    mixed = jnp.concatenate(
        [jnp.concatenate([mr, -mi], axis=1), jnp.concatenate([mi, mr], axis=1)], axis=0
    )
    global_ref[0], global_ref[1] = halves(mixed)
    pl.semaphore_wait(barrier, devices - 1)
    scatter(0, amp_out, amp_in)

    samp_rows = owner_ref.shape[0]
    for load in inputs[2:]:
        load.wait()
    owner = owner_ref[...]
    owner_ids = iota((devices, LANES), 0)
    chunks = samp_rows // 2
    pieces = [one_hot(owner[r : r + 1], devices) for r in range(samp_rows)]
    stacked = jnp.concatenate(
        [jnp.concatenate(pieces[2 * c : 2 * c + 2], axis=1) for c in range(chunks)], axis=0
    )
    tri_shape = (2 * LANES, 3 * LANES)
    tri_row, tri_col = iota(tri_shape, 0), iota(tri_shape, 1)
    tri = ((tri_row < tri_col) | (tri_col >= 2 * LANES)).astype(f32).astype(bf16)
    counts = jnp.dot(stacked, tri, preferred_element_type=f32)
    before = jnp.zeros((devices, LANES), f32)
    ranks = []
    for c in range(chunks):
        block = counts[c * devices : (c + 1) * devices]
        for h in range(2):
            spot = block[:, h * LANES : (h + 1) * LANES] + before
            mine = owner_ids == owner[2 * c + h : 2 * c + h + 1]
            ranks.append(jnp.sum(jnp.where(mine, spot, 0.0), axis=0, keepdims=True))
        before = before + block[:, 2 * LANES :]
    ranking = jnp.concatenate(ranks, axis=0).astype(i32)
    code = owner * capacity_rows + (ranking >> 7)
    rank = ranking & (LANES - 1)
    code_ref[...] = code
    rank_ref[...] = rank

    low = low_ref[...] + 1
    tops, rests = low >> 8, low & 255
    placed = jnp.zeros((codes, 2 * LANES), f32)
    for first in range(0, samp_rows, 16):
        line = [slice(r, r + 1) for r in range(first, first + 16)]
        hot = jnp.concatenate([one_hot(code[r], codes) for r in line], axis=1)
        values = [
            jnp.concatenate([marked(rank[r], part[r], LANES) for r in line], axis=1)
            for part in (tops, rests)
        ]
        placed = placed + lax.dot_general(
            hot,
            jnp.concatenate(values, axis=0),
            (((1,), (1,)), ((), ())),
            preferred_element_type=f32,
        )
    wanted = (placed[:, :LANES] * 256.0 + placed[:, LANES:]).astype(i32) - 1
    req_out[...] = cut(wanted, capacity_rows)
    scatter(5, req_out, req_in)

    all_of(0, amp_in).wait_recv()
    both = jnp.concatenate(
        [
            jnp.concatenate([amp_in[:, part, d] for d in range(depth)], axis=1)
            for part in range(2)
        ],
        axis=0,
    )
    top, rest = halves(both)
    both = jnp.dot(global_ref[0], top, preferred_element_type=f32) + (
        jnp.dot(global_ref[0], rest, preferred_element_type=f32)
        + jnp.dot(global_ref[1], top, preferred_element_type=f32)
    )
    xr, xi = both[:devices], both[devices:]
    weight = xr * xr + xi * xi
    weights = [weight[:, d * LANES : (d + 1) * LANES] for d in range(depth)]
    for d in range(depth):
        wt_out[:, d] = weights[d]
    scatter(1, wt_out, wt_in)

    weight = jnp.concatenate(weights, axis=0)
    norm_part = jnp.sum(weight, axis=0, keepdims=True)
    owner_bits = devices.bit_length() - 1
    code_shape = (rows, LANES)
    row_id = iota(code_shape, 0)
    row_value = (
        ((row_id & (devices - 1)) << local_bits)
        + me * (depth * LANES)
        + ((row_id >> owner_bits) << 7)
    )
    lane_value = iota((LANES, LANES), 0)
    row_code = jnp.zeros(code_shape, i32)
    lane_code = jnp.zeros((LANES, LANES), i32)
    lane_mask = jnp.zeros((), i32)
    for k in range(marg_count):
        qubit = marg[0, k]
        row_code = row_code + (((row_value >> qubit) & 1) << k)
        lane_code = lane_code + (((lane_value >> qubit) & 1) << k)
        lane_mask = lane_mask + jnp.where(qubit < 7, 1 << k, 0)
    bins = 2**marg_count
    top, rest = halves(weight)
    split = jnp.concatenate([top, rest], axis=0)
    @pl.loop(0, bins // LANES)
    def _(c):
        bin_id = c * LANES + iota((1, LANES), 1)
        lane_part = bin_id & lane_mask
        lane_hot = (lane_code == lane_part).astype(f32).astype(bf16)
        folded = jnp.dot(split, lane_hot, preferred_element_type=f32)
        folded = folded[:rows] + folded[rows:]
        picked = jnp.where(row_code == bin_id - lane_part, folded, 0.0)
        his_out[c] = jnp.sum(picked, axis=0, keepdims=True)

    bin_share = devices * LANES // bins
    for target in peers:
        copy(4, his_out.at[target // bin_share], his_in.at[me], target).start()
    his_in[me] = his_out[me // bin_share]

    all_of(5, req_in).wait_recv()
    req_ref[...] = join(req_in[...])
    all_of(1, wt_in).wait_recv()
    plain_ref[0:rows] = join(wt_in[...])
    table_ref[:, 0:rows] = split_table(plain_ref[0:rows])
    group = 32 // capacity_rows
    groups = devices // group
    mine, spot = me // group, me % group

    dots = 32 - 8

    def place_of(turn):
        first = lax.rem(mine + turn, groups) * group
        start = pl.multiple_of(first * capacity_rows, SUBLANES)
        return first, req_ref[pl.ds(start, group * capacity_rows)]

    def begin(turn, slot):
        _, wanted = place_of(turn)
        upper, lower = wanted >> 7, wanted & (LANES - 1)
        both_ref[slot] = rows_dot(table_ref[:, 0:rows], upper[:dots])
        for first in range(dots, 32, SUBLANES):
            part = slice(first, first + SUBLANES)
            value = lookup_lanes(plain_ref.at[0:rows], upper[part], lower[part])
            side_ref[slot, first - dots : first - dots + SUBLANES] = jnp.where(
                upper[part] >= 0, value, 0.0
            )

    def answer(turn, slot):
        first, wanted = place_of(turn)
        lower = wanted & (LANES - 1)
        found = [
            pick_lane(both_ref[slot, :, r * LANES : (r + 1) * LANES], lower[r : r + 1])
            for r in range(dots)
        ]
        found = jnp.concatenate([*found, side_ref[slot]], axis=0)
        ans_out[pl.ds(first, group)] = cut(found, capacity_rows)
        return first, jnp.sum(found, axis=0, keepdims=True)

    def reply(first, count):
        for j in range(1, count + 1):
            target = first + lax.rem(spot + j, group)
            copy(2, ans_out.at[target], ans_in.at[me], target).start()

    total = jnp.zeros((1, LANES), f32)
    turns = [*range(1, groups), 0]
    begin(turns[0], 0)
    for n, turn in enumerate(turns):
        if n + 1 < groups:
            begin(turns[n + 1], (n + 1) % 2)
        before, extra = answer(turn, n % 2)
        total = total + extra
        if n + 1 < groups:
            reply(before, group)
    reply(before, group - 1)
    half = iota((1, LANES), 1) < LANES // 2
    packed = [jnp.broadcast_to(x, (SUBLANES, LANES)) for x in (total, norm_part)]
    packed = [x + pltpu.roll(x, LANES // 2, 1) for x in packed]
    tot_out[0] = jnp.where(half, packed[0][0:1], packed[1][0:1])
    spread(3, tot_out, tot_in)
    ans_in[me] = ans_out[me]

    all_of(2, ans_in).wait_recv()
    plain_ref[0:codes] = join(ans_in[...])
    table_ref[:, 0:codes] = split_table(plain_ref[0:codes])
    for first in range(0, samp_rows, 32):
        window = slice(first, first + 32)
        probs_ref[window] = lookup_both(
            table_ref[:, 0:codes], plain_ref.at[0:codes], code_ref[window], rank_ref[window], 8
        )
    all_of(4, his_in).wait_recv()
    hist_ref[...] = jnp.sum(his_in[...], axis=0)
    all_of(3, tot_in).wait_recv()
    fid_ref[...] = jnp.sum(tot_in[...], axis=0)

    for channel, into in enumerate((amp_in, wt_in, ans_in, tot_in, his_in, req_in)):
        all_of(channel, into).wait_send()


def finish(sizes, values, hist, totals, probs_ref, mine_ref, fid_ref):
    amps_total, samples, bins = sizes
    mine = mine_ref.shape[1]
    start = lax.axis_index("dev") * mine
    line = totals[...]
    half = iota(line.shape, 1) < LANES // 2
    total = jnp.sum(jnp.where(half, line, 0.0), axis=1, keepdims=True)
    norm = jnp.sum(jnp.where(half, 0.0, line), axis=1, keepdims=True)
    probs_ref[...] = amps_total * (values[...] / norm)
    line = jnp.broadcast_to(hist[0:1], (SUBLANES, LANES))
    line = pltpu.roll(line, (LANES - start % LANES) % LANES, 1)
    mine_ref[...] = bins * (line[0:1, :mine] / norm)
    fid_ref[...] = amps_total * (total / norm) / samples - 1.0


def shards(state, angles, sample_high, sample_low, marginal_qubits):
    devices = lax.axis_size("dev")
    amps_local = state.shape[1]
    samp_local = sample_low.shape[0]
    marg_count = marginal_qubits.shape[0]
    bins = 2**marg_count
    depth = amps_local // devices // LANES
    capacity_rows = 4 * samp_local // devices // LANES
    rows = amps_local // LANES
    samp_rows = samp_local // LANES
    sizes = (
        devices,
        depth,
        capacity_rows,
        marg_count,
    )
    vmem = pl.BlockSpec(memory_space=pltpu.VMEM)
    codes = devices * capacity_rows
    bin_rows = bins // LANES
    values, hist, totals = pl.pallas_call(
        functools.partial(kernel, sizes),
        out_shape=(
            jax.ShapeDtypeStruct((samp_rows, LANES), f32),
            jax.ShapeDtypeStruct((1, LANES), f32),
            jax.ShapeDtypeStruct((1, LANES), f32),
        ),
        in_specs=[pl.BlockSpec(memory_space=pltpu.HBM)] * 5,
        out_specs=(vmem, vmem, vmem),
        scratch_shapes=[
            pltpu.VMEM((devices, 2, depth, LANES), f32),
            pltpu.VMEM((devices, 2, depth, LANES), f32),
            pltpu.VMEM((devices, depth, LANES), f32),
            pltpu.VMEM((devices, depth, LANES), f32),
            pltpu.VMEM((devices, capacity_rows, LANES), i32),
            pltpu.VMEM((devices, capacity_rows, LANES), i32),
            pltpu.VMEM((devices, capacity_rows, LANES), f32),
            pltpu.VMEM((devices, capacity_rows, LANES), f32),
            pltpu.VMEM((bin_rows, 1, LANES), f32),
            pltpu.VMEM((devices, 1, LANES), f32),
            pltpu.VMEM((1, 1, LANES), f32),
            pltpu.VMEM((devices, 1, LANES), f32),
            pltpu.VMEM((samp_rows, LANES), i32),
            pltpu.VMEM((samp_rows, LANES), i32),
            pltpu.VMEM((codes, LANES), i32),
            pltpu.VMEM((2 * LANES, max(rows, codes)), bf16),
            pltpu.VMEM((max(rows, codes), LANES), f32),
            pltpu.VMEM((2, LANES, (32 - 8) * LANES), f32),
            pltpu.VMEM((2, 8, LANES), f32),
            pltpu.VMEM((2, 2 * devices, 2 * devices), bf16),
            pltpu.VMEM((8, -(-angles.shape[0] // SUBLANES) * SUBLANES, LANES), f32),
            pltpu.SMEM((angles.shape[1], angles.shape[0]), f32),
            pltpu.SMEM((1, marg_count), i32),
            pltpu.VMEM((2 * rows, LANES), f32),
            pltpu.VMEM((samp_rows, LANES), i32),
            pltpu.VMEM((samp_rows, LANES), i32),
            pltpu.SemaphoreType.DMA((6,)),
            pltpu.SemaphoreType.DMA((6,)),
            pltpu.SemaphoreType.DMA((5,)),
        ],
        compiler_params=pltpu.CompilerParams(
            collective_id=0, has_side_effects=True, vmem_limit_bytes=24 << 20
        ),
        name="circuit",
    )(
        pltpu.with_memory_space_constraint(angles.T, pltpu.HBM),
        pltpu.with_memory_space_constraint(marginal_qubits.reshape(1, marg_count), pltpu.HBM),
        pltpu.with_memory_space_constraint(state.reshape(2, rows, LANES).transpose(1, 0, 2).reshape(2 * rows, LANES), pltpu.HBM),
        pltpu.with_memory_space_constraint(sample_high.reshape(samp_rows, LANES), pltpu.HBM),
        pltpu.with_memory_space_constraint(sample_low.reshape(samp_rows, LANES), pltpu.HBM),
    )
    probs, mine, fid = pl.pallas_call(
        functools.partial(
            finish, (float(amps_local * devices), float(samp_local * devices), float(bins))
        ),
        out_shape=(
            jax.ShapeDtypeStruct((samp_rows, LANES), f32),
            jax.ShapeDtypeStruct((1, bins // devices), f32),
            jax.ShapeDtypeStruct((1, 1), f32),
        ),
        in_specs=[vmem, vmem, vmem],
        out_specs=(vmem, vmem, vmem),
        compiler_params=pltpu.CompilerParams(vmem_limit_bytes=1 << 20),
        name="finish",
    )(values, hist, totals)
    return probs.reshape(samp_local), mine.reshape(bins // devices), fid.reshape(())


def solution(mesh):
    return jax.shard_map(
        shards,
        mesh=mesh,
        in_specs=(P(None, "dev"), P(), P("dev", None), P("dev"), P()),
        out_specs=(P("dev"), P("dev"), P()),
        check_vma=False,
    )
```

```python
import functools
import itertools
import random

import jax
import jax.numpy as jnp
from jax import lax
from jax.experimental import pallas as pl
from jax.experimental.pallas import tpu as pltpu
from jax.sharding import PartitionSpec as P

LANES = 128
SUBLANES = 8
TORUS = (4, 4, 4, 2)
f32 = jnp.float32
bf16 = jnp.bfloat16
i32 = jnp.int32


def iota(shape, dim):
    return lax.broadcasted_iota(i32, shape, dim)


def gate_rows(angles, qubits):
    sub = iota((SUBLANES, LANES), 0)

    def column(j):
        blocks = []
        for first in range(0, qubits, SUBLANES):
            block = jnp.zeros((SUBLANES, LANES), f32)
            for q in range(first, min(first + SUBLANES, qubits)):
                block = jnp.where(sub == q - first, angles[j, q], block)
            blocks.append(block)
        return jnp.concatenate(blocks, axis=0)

    theta, first, second = column(0), column(1), column(2)
    cosine, sine = jnp.cos(theta), jnp.sin(theta)
    joint = first + second
    return [
        cosine,
        jnp.zeros_like(cosine),
        -jnp.cos(second) * sine,
        -jnp.sin(second) * sine,
        jnp.cos(first) * sine,
        jnp.sin(first) * sine,
        jnp.cos(joint) * cosine,
        jnp.sin(joint) * cosine,
    ]


def leading_gate(xr, xi, bit, u):
    n, s, lanes = xr.shape
    shape = (n >> (bit + 1), 2, 1 << bit, s, lanes)
    xr, xi = xr.reshape(shape), xi.reshape(shape)
    ar, ai, br, bi = xr[:, 0], xi[:, 0], xr[:, 1], xi[:, 1]
    outs_r, outs_i = [], []
    for row in range(2):
        pr, pi, qr, qi = u[4 * row : 4 * row + 4]
        outs_r.append(pr * ar - pi * ai + (qr * br - qi * bi))
        outs_i.append(pr * ai + pi * ar + (qr * bi + qi * br))
    return (
        jnp.stack(outs_r, 1).reshape(n, s, lanes),
        jnp.stack(outs_i, 1).reshape(n, s, lanes),
    )


def sublane_gate(xr, xi, bit, u):
    step = 1 << bit
    high = ((iota((SUBLANES, LANES), 0) >> bit) & 1) == 1

    def swap(x):
        down = pltpu.roll(x, step, 1)
        if 2 * step == SUBLANES:
            return down
        return jnp.where(high[None], down, pltpu.roll(x, SUBLANES - step, 1))

    keep_r = jnp.where(high, u[6], u[0])[None]
    keep_i = jnp.where(high, u[7], u[1])[None]
    cross_r = jnp.where(high, u[4], u[2])[None]
    cross_i = jnp.where(high, u[5], u[3])[None]
    yr, yi = swap(xr), swap(xi)
    return (
        keep_r * xr - keep_i * xi + (cross_r * yr - cross_i * yi),
        keep_r * xi + keep_i * xr + (cross_r * yi + cross_i * yr),
    )


def lane_matrix(units):
    shape = (LANES, LANES)
    row, col = iota(shape, 0), iota(shape, 1)
    mr = mi = None
    for bit, u in enumerate(units):
        rb, cb = ((row >> bit) & 1) == 1, ((col >> bit) & 1) == 1
        gr = jnp.where(cb, jnp.where(rb, u[6], u[4]), jnp.where(rb, u[2], u[0]))
        gi = jnp.where(cb, jnp.where(rb, u[7], u[5]), jnp.where(rb, u[3], u[1]))
        if mr is None:
            mr, mi = gr, gi
        else:
            mr, mi = mr * gr - mi * gi, mr * gi + mi * gr
    return mr, mi


def row_matrix(units):
    shape = (LANES, LANES)
    row, col = iota(shape, 0), iota(shape, 1)
    mr = mi = None
    for bit, u in enumerate(units):
        rb, cb = ((row >> bit) & 1) == 1, ((col >> bit) & 1) == 1
        gr = jnp.where(rb, jnp.where(cb, u[6], u[4]), jnp.where(cb, u[2], u[0]))
        gi = jnp.where(rb, jnp.where(cb, u[7], u[5]), jnp.where(cb, u[3], u[1]))
        if mr is None:
            mr, mi = gr, gi
        else:
            mr, mi = mr * gr - mi * gi, mr * gi + mi * gr
    return mr, mi


def cut(x, depth):
    rows = x.shape[0]
    x = x.reshape(rows // SUBLANES, SUBLANES, LANES)
    per = SUBLANES // depth
    if per == 1:
        return x
    parts = [x[:, k * depth : (k + 1) * depth] for k in range(per)]
    return jnp.stack(parts, 1).reshape(rows // depth, depth, LANES)


def join(x):
    n, depth, _ = x.shape
    per = SUBLANES // depth
    if per > 1:
        x = x.reshape(n // per, per, depth, LANES)
        x = jnp.concatenate([x[:, k] for k in range(per)], axis=1)
    return x.reshape(n * depth, LANES)


def halves(x):
    top = x.astype(bf16)
    return top, (x - top.astype(f32)).astype(bf16)


def marked(row, value, count):
    shape = (2 * SUBLANES, LANES)
    wide = jnp.broadcast_to(row.astype(f32), shape).astype(bf16)
    value = jnp.broadcast_to(value.astype(f32), shape).astype(bf16)
    ids = iota((count, LANES), 0).astype(f32).astype(bf16).reshape(count // 16, 16, LANES)
    return jnp.where(ids == wide[None], value[None], jnp.zeros((), bf16)).reshape(count, LANES)


def one_hot(row, count):
    wide = jnp.broadcast_to(row.astype(f32), (16, LANES)).astype(bf16)
    ids = iota((count, LANES), 0).astype(f32).astype(bf16).reshape(count // 16, 16, LANES)
    hot = jnp.where(ids == wide[None], jnp.ones((), bf16), jnp.zeros((), bf16))
    return hot.reshape(count, LANES)


def split_table(table):
    flipped = table.T
    top, rest = halves(flipped)
    return jnp.concatenate([top, rest], axis=0)


def pick_lane(value, lower):
    value = value.reshape(LANES // SUBLANES, SUBLANES, LANES)
    low = jnp.broadcast_to(lower, (SUBLANES, LANES))
    for bit in (6, 5, 4, 3):
        half = value.shape[0] // 2
        value = jnp.where((((low >> bit) & 1) == 1)[None], value[half:], value[:half])
    sub = iota((SUBLANES, LANES), 0)
    value = jnp.where(sub == (low & (SUBLANES - 1)), value[0], 0.0)
    return jnp.sum(value, axis=0, keepdims=True)


def rows_dot(table, upper):
    count = table.shape[1]
    hot = [one_hot(upper[r : r + 1], count) for r in range(upper.shape[0])]
    both = jnp.dot(table, jnp.concatenate(hot, axis=1), preferred_element_type=f32)
    return both[:LANES] + both[LANES:]


def lookup(table, upper, lower):
    both = rows_dot(table, upper)
    found = [
        pick_lane(both[:, r * LANES : (r + 1) * LANES], lower[r : r + 1])
        for r in range(upper.shape[0])
    ]
    return jnp.concatenate(found, axis=0)


def lookup_lanes(plain, upper, lower):
    bits = plain.shape[0].bit_length() - 1
    high = [((upper >> bit) & 1) == 1 for bit in range(bits)]

    def pick(first, bit):
        if bit < 0:
            line = jnp.broadcast_to(plain[first : first + 1], (SUBLANES, LANES))
            return jnp.take_along_axis(line, lower, axis=1, mode="promise_in_bounds")
        zero = pick(first, bit - 1)
        return jnp.where(high[bit], pick(first + (1 << bit), bit - 1), zero)

    return pick(0, bits - 1)


def lookup_both(table, plain, upper, lower, lanes):
    dots = upper.shape[0] - lanes
    found = [lookup(table, upper[:dots], lower[:dots])]
    for first in range(dots, dots + lanes, SUBLANES):
        part = slice(first, first + SUBLANES)
        value = lookup_lanes(plain, upper[part], lower[part])
        found.append(jnp.where(upper[part] >= 0, value, 0.0))
    return jnp.concatenate(found, axis=0)


def routes(me):
    parts = []
    rest = me
    for size in reversed(TORUS):
        parts.insert(0, lax.rem(rest, size))
        rest = rest // size
    scale = 1
    tables = []
    for part, size in zip(reversed(parts), reversed(TORUS)):
        tables.insert(0, [lax.rem(part + step, size) * scale for step in range(size)])
        scale *= size
    steps = [step for step in itertools.product(*[range(size) for size in TORUS]) if any(step)]
    random.Random(1).shuffle(steps)
    steps.sort(key=lambda step: -sum(min(d, n - d) for d, n in zip(step[:3], TORUS[:3])))
    upper = {(a, b): tables[0][a] + tables[1][b] for a in range(TORUS[0]) for b in range(TORUS[1])}
    lower = {(a, b): tables[2][a] + tables[3][b] for a in range(TORUS[2]) for b in range(TORUS[3])}
    return [upper[step[:2]] + lower[step[2:]] for step in steps]


def kernel(
    sizes,
    angles_hbm,
    marg_hbm,
    state_hbm,
    owner_hbm,
    low_hbm,
    probs_ref,
    hist_ref,
    fid_ref,
    amp_out,
    amp_in,
    wt_out,
    wt_in,
    req_out,
    req_in,
    ans_out,
    ans_in,
    his_out,
    his_in,
    tot_out,
    tot_in,
    code_ref,
    rank_ref,
    req_ref,
    table_ref,
    plain_ref,
    both_ref,
    side_ref,
    global_ref,
    gates,
    angles,
    marg,
    state,
    owner_ref,
    low_ref,
    sends,
    recvs,
    loads,
):
    devices, depth, capacity_rows, marg_count = sizes
    me = lax.axis_index("dev")
    global_bits = devices.bit_length() - 1
    rows = state.shape[0] // 2
    row_bits = rows.bit_length() - 1
    local_bits = row_bits + 7
    codes = devices * capacity_rows

    peers = routes(me)
    inputs = [
        pltpu.make_async_copy(src, dst, loads.at[n])
        for n, (src, dst) in enumerate(
            (
                (angles_hbm, angles),
                (state_hbm, state),
                (owner_hbm, owner_ref),
                (low_hbm, low_ref),
                (marg_hbm, marg),
            )
        )
    ]
    for load in inputs:
        load.start()

    def copy(channel, src, dst, target):
        return pltpu.make_async_remote_copy(
            src_ref=src,
            dst_ref=dst,
            send_sem=sends.at[channel],
            recv_sem=recvs.at[channel],
            device_id=(target,),
            device_id_type=pl.DeviceIdType.MESH,
        )

    def scatter(channel, out, into):
        for target in peers:
            copy(channel, out.at[target], into.at[me], target).start()
        into[me] = out[me]

    def spread(channel, out, into):
        for target in peers:
            copy(channel, out.at[0], into.at[me], target).start()
        into[me] = out[0]

    def all_of(channel, into):
        many = into.at[pl.ds(0, devices - 1)]
        return copy(channel, many, many, peers[-1])

    barrier = pltpu.get_barrier_semaphore()

    for target in peers:
        pl.semaphore_signal(
            barrier, inc=1, device_id=(target,), device_id_type=pl.DeviceIdType.MESH
        )

    inputs[0].wait()
    for e, entry in enumerate(gate_rows(angles, global_bits + local_bits)):
        gates[e] = entry

    def unit(qubit):
        return [gates[e, qubit : qubit + 1] for e in range(8)]

    mr, mi = lane_matrix([unit(q) for q in range(7)])
    mixed = jnp.concatenate(
        [jnp.concatenate([mr, mi], axis=1), jnp.concatenate([-mi, mr], axis=1)], axis=0
    )
    inputs[1].wait()
    both = jnp.concatenate(
        [state[pl.ds(0, rows, stride=2)], state[pl.ds(1, rows, stride=2)]], axis=1
    )
    both = jnp.dot(both, mixed, precision=lax.Precision.HIGHEST, preferred_element_type=f32)
    xr = both[:, :LANES].reshape(rows // SUBLANES, SUBLANES, LANES)
    xi = both[:, LANES:].reshape(rows // SUBLANES, SUBLANES, LANES)
    for bit in range(3):
        xr, xi = sublane_gate(xr, xi, bit, unit(7 + bit))
    for bit in range(row_bits - 3):
        xr, xi = leading_gate(xr, xi, bit, unit(10 + bit))
    amp_out[:, 0] = cut(xr.reshape(rows, LANES), depth)
    amp_out[:, 1] = cut(xi.reshape(rows, LANES), depth)

    mr, mi = row_matrix([unit(local_bits + q) for q in range(global_bits)])
    mixed = jnp.concatenate(
        [jnp.concatenate([mr, -mi], axis=1), jnp.concatenate([mi, mr], axis=1)], axis=0
    )
    global_ref[0], global_ref[1] = halves(mixed)
    pl.semaphore_wait(barrier, devices - 1)
    scatter(0, amp_out, amp_in)

    samp_rows = owner_ref.shape[0]
    for load in inputs[2:]:
        load.wait()
    owner = owner_ref[...]
    owner_ids = iota((devices, LANES), 0)
    chunks = samp_rows // 2
    pieces = [one_hot(owner[r : r + 1], devices) for r in range(samp_rows)]
    stacked = jnp.concatenate(
        [jnp.concatenate(pieces[2 * c : 2 * c + 2], axis=1) for c in range(chunks)], axis=0
    )
    tri_shape = (2 * LANES, 3 * LANES)
    tri_row, tri_col = iota(tri_shape, 0), iota(tri_shape, 1)
    tri = ((tri_row < tri_col) | (tri_col >= 2 * LANES)).astype(f32).astype(bf16)
    counts = jnp.dot(stacked, tri, preferred_element_type=f32)
    before = jnp.zeros((devices, LANES), f32)
    ranks = []
    for c in range(chunks):
        block = counts[c * devices : (c + 1) * devices]
        for h in range(2):
            spot = block[:, h * LANES : (h + 1) * LANES] + before
            mine = owner_ids == owner[2 * c + h : 2 * c + h + 1]
            ranks.append(jnp.sum(jnp.where(mine, spot, 0.0), axis=0, keepdims=True))
        before = before + block[:, 2 * LANES :]
    ranking = jnp.concatenate(ranks, axis=0).astype(i32)
    code = owner * capacity_rows + (ranking >> 7)
    rank = ranking & (LANES - 1)
    code_ref[...] = code
    rank_ref[...] = rank

    low = low_ref[...] + 1
    tops, rests = low >> 8, low & 255
    placed = jnp.zeros((codes, 2 * LANES), f32)
    for first in range(0, samp_rows, 16):
        line = [slice(r, r + 1) for r in range(first, first + 16)]
        hot = jnp.concatenate([one_hot(code[r], codes) for r in line], axis=1)
        values = [
            jnp.concatenate([marked(rank[r], part[r], LANES) for r in line], axis=1)
            for part in (tops, rests)
        ]
        placed = placed + lax.dot_general(
            hot,
            jnp.concatenate(values, axis=0),
            (((1,), (1,)), ((), ())),
            preferred_element_type=f32,
        )
    wanted = (placed[:, :LANES] * 256.0 + placed[:, LANES:]).astype(i32) - 1
    req_out[...] = cut(wanted, capacity_rows)
    scatter(5, req_out, req_in)

    all_of(0, amp_in).wait_recv()
    both = jnp.concatenate(
        [
            jnp.concatenate([amp_in[:, part, d] for d in range(depth)], axis=1)
            for part in range(2)
        ],
        axis=0,
    )
    top, rest = halves(both)
    both = jnp.dot(global_ref[0], top, preferred_element_type=f32) + (
        jnp.dot(global_ref[0], rest, preferred_element_type=f32)
        + jnp.dot(global_ref[1], top, preferred_element_type=f32)
    )
    xr, xi = both[:devices], both[devices:]
    weight = xr * xr + xi * xi
    weights = [weight[:, d * LANES : (d + 1) * LANES] for d in range(depth)]
    for d in range(depth):
        wt_out[:, d] = weights[d]
    scatter(1, wt_out, wt_in)

    weight = jnp.concatenate(weights, axis=0)
    norm_part = jnp.sum(weight, axis=0, keepdims=True)
    owner_bits = devices.bit_length() - 1
    code_shape = (rows, LANES)
    row_id = iota(code_shape, 0)
    row_value = (
        ((row_id & (devices - 1)) << local_bits)
        + me * (depth * LANES)
        + ((row_id >> owner_bits) << 7)
    )
    lane_value = iota((LANES, LANES), 0)
    row_code = jnp.zeros(code_shape, i32)
    lane_code = jnp.zeros((LANES, LANES), i32)
    lane_mask = jnp.zeros((), i32)
    for k in range(marg_count):
        qubit = marg[0, k]
        row_code = row_code + (((row_value >> qubit) & 1) << k)
        lane_code = lane_code + (((lane_value >> qubit) & 1) << k)
        lane_mask = lane_mask + jnp.where(qubit < 7, 1 << k, 0)
    bins = 2**marg_count
    top, rest = halves(weight)
    split = jnp.concatenate([top, rest], axis=0)
    @pl.loop(0, bins // LANES)
    def _(c):
        bin_id = c * LANES + iota((1, LANES), 1)
        lane_part = bin_id & lane_mask
        lane_hot = (lane_code == lane_part).astype(f32).astype(bf16)
        folded = jnp.dot(split, lane_hot, preferred_element_type=f32)
        folded = folded[:rows] + folded[rows:]
        picked = jnp.where(row_code == bin_id - lane_part, folded, 0.0)
        his_out[c] = jnp.sum(picked, axis=0, keepdims=True)

    bin_share = devices * LANES // bins
    for target in peers:
        copy(4, his_out.at[target // bin_share], his_in.at[me], target).start()
    his_in[me] = his_out[me // bin_share]

    all_of(5, req_in).wait_recv()
    req_ref[...] = join(req_in[...])
    all_of(1, wt_in).wait_recv()
    plain_ref[0:rows] = join(wt_in[...])
    table_ref[:, 0:rows] = split_table(plain_ref[0:rows])
    group = 32 // capacity_rows
    groups = devices // group
    mine, spot = me // group, me % group

    dots = 32 - 8

    def place_of(turn):
        first = lax.rem(mine + turn, groups) * group
        start = pl.multiple_of(first * capacity_rows, SUBLANES)
        return first, req_ref[pl.ds(start, group * capacity_rows)]

    def begin(turn, slot):
        _, wanted = place_of(turn)
        upper, lower = wanted >> 7, wanted & (LANES - 1)
        both_ref[slot] = rows_dot(table_ref[:, 0:rows], upper[:dots])
        for first in range(dots, 32, SUBLANES):
            part = slice(first, first + SUBLANES)
            value = lookup_lanes(plain_ref.at[0:rows], upper[part], lower[part])
            side_ref[slot, first - dots : first - dots + SUBLANES] = jnp.where(
                upper[part] >= 0, value, 0.0
            )

    def answer(turn, slot):
        first, wanted = place_of(turn)
        lower = wanted & (LANES - 1)
        found = [
            pick_lane(both_ref[slot, :, r * LANES : (r + 1) * LANES], lower[r : r + 1])
            for r in range(dots)
        ]
        found = jnp.concatenate([*found, side_ref[slot]], axis=0)
        ans_out[pl.ds(first, group)] = cut(found, capacity_rows)
        return first, jnp.sum(found, axis=0, keepdims=True)

    def reply(first, count):
        for j in range(1, count + 1):
            target = first + lax.rem(spot + j, group)
            copy(2, ans_out.at[target], ans_in.at[me], target).start()

    total = jnp.zeros((1, LANES), f32)
    turns = sorted(range(groups), key=lambda turn: -min(turn, groups - turn))
    begin(turns[0], 0)
    for n, turn in enumerate(turns):
        if n + 1 < groups:
            begin(turns[n + 1], (n + 1) % 2)
        before, extra = answer(turn, n % 2)
        total = total + extra
        if n + 1 < groups:
            reply(before, group)
    reply(before, group - 1)
    half = iota((1, LANES), 1) < LANES // 2
    packed = [jnp.broadcast_to(x, (SUBLANES, LANES)) for x in (total, norm_part)]
    packed = [x + pltpu.roll(x, LANES // 2, 1) for x in packed]
    tot_out[0] = jnp.where(half, packed[0][0:1], packed[1][0:1])
    spread(3, tot_out, tot_in)
    ans_in[me] = ans_out[me]

    all_of(2, ans_in).wait_recv()
    plain_ref[0:codes] = join(ans_in[...])
    table_ref[:, 0:codes] = split_table(plain_ref[0:codes])
    for first in range(0, samp_rows, 32):
        window = slice(first, first + 32)
        probs_ref[window] = lookup_both(
            table_ref[:, 0:codes], plain_ref.at[0:codes], code_ref[window], rank_ref[window], 8
        )
    all_of(4, his_in).wait_recv()
    hist_ref[...] = jnp.sum(his_in[...], axis=0)
    all_of(3, tot_in).wait_recv()
    fid_ref[...] = jnp.sum(tot_in[...], axis=0)

    for channel, into in enumerate((amp_in, wt_in, ans_in, tot_in, his_in, req_in)):
        all_of(channel, into).wait_send()


def finish(sizes, values, hist, totals, probs_ref, mine_ref, fid_ref):
    amps_total, samples, bins = sizes
    mine = mine_ref.shape[1]
    start = lax.axis_index("dev") * mine
    line = totals[...]
    half = iota(line.shape, 1) < LANES // 2
    total = jnp.sum(jnp.where(half, line, 0.0), axis=1, keepdims=True)
    norm = jnp.sum(jnp.where(half, 0.0, line), axis=1, keepdims=True)
    probs_ref[...] = amps_total * (values[...] / norm)
    line = jnp.broadcast_to(hist[0:1], (SUBLANES, LANES))
    line = pltpu.roll(line, (LANES - start % LANES) % LANES, 1)
    mine_ref[...] = bins * (line[0:1, :mine] / norm)
    fid_ref[...] = amps_total * (total / norm) / samples - 1.0


def shards(state, angles, sample_high, sample_low, marginal_qubits):
    devices = lax.axis_size("dev")
    amps_local = state.shape[1]
    samp_local = sample_low.shape[0]
    marg_count = marginal_qubits.shape[0]
    bins = 2**marg_count
    depth = amps_local // devices // LANES
    capacity_rows = 4 * samp_local // devices // LANES
    rows = amps_local // LANES
    samp_rows = samp_local // LANES
    sizes = (
        devices,
        depth,
        capacity_rows,
        marg_count,
    )
    vmem = pl.BlockSpec(memory_space=pltpu.VMEM)
    codes = devices * capacity_rows
    bin_rows = bins // LANES
    values, hist, totals = pl.pallas_call(
        functools.partial(kernel, sizes),
        out_shape=(
            jax.ShapeDtypeStruct((samp_rows, LANES), f32),
            jax.ShapeDtypeStruct((1, LANES), f32),
            jax.ShapeDtypeStruct((1, LANES), f32),
        ),
        in_specs=[pl.BlockSpec(memory_space=pltpu.HBM)] * 5,
        out_specs=(vmem, vmem, vmem),
        scratch_shapes=[
            pltpu.VMEM((devices, 2, depth, LANES), f32),
            pltpu.VMEM((devices, 2, depth, LANES), f32),
            pltpu.VMEM((devices, depth, LANES), f32),
            pltpu.VMEM((devices, depth, LANES), f32),
            pltpu.VMEM((devices, capacity_rows, LANES), i32),
            pltpu.VMEM((devices, capacity_rows, LANES), i32),
            pltpu.VMEM((devices, capacity_rows, LANES), f32),
            pltpu.VMEM((devices, capacity_rows, LANES), f32),
            pltpu.VMEM((bin_rows, 1, LANES), f32),
            pltpu.VMEM((devices, 1, LANES), f32),
            pltpu.VMEM((1, 1, LANES), f32),
            pltpu.VMEM((devices, 1, LANES), f32),
            pltpu.VMEM((samp_rows, LANES), i32),
            pltpu.VMEM((samp_rows, LANES), i32),
            pltpu.VMEM((codes, LANES), i32),
            pltpu.VMEM((2 * LANES, max(rows, codes)), bf16),
            pltpu.VMEM((max(rows, codes), LANES), f32),
            pltpu.VMEM((2, LANES, (32 - 8) * LANES), f32),
            pltpu.VMEM((2, 8, LANES), f32),
            pltpu.VMEM((2, 2 * devices, 2 * devices), bf16),
            pltpu.VMEM((8, -(-angles.shape[0] // SUBLANES) * SUBLANES, LANES), f32),
            pltpu.SMEM((angles.shape[1], angles.shape[0]), f32),
            pltpu.SMEM((1, marg_count), i32),
            pltpu.VMEM((2 * rows, LANES), f32),
            pltpu.VMEM((samp_rows, LANES), i32),
            pltpu.VMEM((samp_rows, LANES), i32),
            pltpu.SemaphoreType.DMA((6,)),
            pltpu.SemaphoreType.DMA((6,)),
            pltpu.SemaphoreType.DMA((5,)),
        ],
        compiler_params=pltpu.CompilerParams(
            collective_id=0, has_side_effects=True, vmem_limit_bytes=24 << 20
        ),
        name="circuit",
    )(
        pltpu.with_memory_space_constraint(angles.T, pltpu.HBM),
        pltpu.with_memory_space_constraint(marginal_qubits.reshape(1, marg_count), pltpu.HBM),
        pltpu.with_memory_space_constraint(state.reshape(2, rows, LANES).transpose(1, 0, 2).reshape(2 * rows, LANES), pltpu.HBM),
        pltpu.with_memory_space_constraint(sample_high.reshape(samp_rows, LANES), pltpu.HBM),
        pltpu.with_memory_space_constraint(sample_low.reshape(samp_rows, LANES), pltpu.HBM),
    )
    probs, mine, fid = pl.pallas_call(
        functools.partial(
            finish, (float(amps_local * devices), float(samp_local * devices), float(bins))
        ),
        out_shape=(
            jax.ShapeDtypeStruct((samp_rows, LANES), f32),
            jax.ShapeDtypeStruct((1, bins // devices), f32),
            jax.ShapeDtypeStruct((1, 1), f32),
        ),
        in_specs=[vmem, vmem, vmem],
        out_specs=(vmem, vmem, vmem),
        compiler_params=pltpu.CompilerParams(vmem_limit_bytes=1 << 20),
        name="finish",
    )(values, hist, totals)
    return probs.reshape(samp_local), mine.reshape(bins // devices), fid.reshape(())


def solution(mesh):
    return jax.shard_map(
        shards,
        mesh=mesh,
        in_specs=(P(None, "dev"), P(), P("dev", None), P("dev"), P()),
        out_specs=(P("dev"), P("dev"), P()),
        check_vma=False,
    )
```

```python
import functools
import itertools
import random

import jax
import jax.numpy as jnp
from jax import lax
from jax.experimental import pallas as pl
from jax.experimental.pallas import tpu as pltpu
from jax.sharding import PartitionSpec as P

LANES = 128
SUBLANES = 8
TORUS = (4, 4, 4, 2)
f32 = jnp.float32
bf16 = jnp.bfloat16
i32 = jnp.int32


def iota(shape, dim):
    return lax.broadcasted_iota(i32, shape, dim)


def gate_rows(angles, qubits):
    sub = iota((SUBLANES, LANES), 0)

    def column(j):
        blocks = []
        for first in range(0, qubits, SUBLANES):
            block = jnp.zeros((SUBLANES, LANES), f32)
            for q in range(first, min(first + SUBLANES, qubits)):
                block = jnp.where(sub == q - first, angles[j, q], block)
            blocks.append(block)
        return jnp.concatenate(blocks, axis=0)

    theta, first, second = column(0), column(1), column(2)
    cosine, sine = jnp.cos(theta), jnp.sin(theta)
    joint = first + second
    return [
        cosine,
        jnp.zeros_like(cosine),
        -jnp.cos(second) * sine,
        -jnp.sin(second) * sine,
        jnp.cos(first) * sine,
        jnp.sin(first) * sine,
        jnp.cos(joint) * cosine,
        jnp.sin(joint) * cosine,
    ]


def leading_gate(xr, xi, bit, u):
    n, s, lanes = xr.shape
    shape = (n >> (bit + 1), 2, 1 << bit, s, lanes)
    xr, xi = xr.reshape(shape), xi.reshape(shape)
    ar, ai, br, bi = xr[:, 0], xi[:, 0], xr[:, 1], xi[:, 1]
    outs_r, outs_i = [], []
    for row in range(2):
        pr, pi, qr, qi = u[4 * row : 4 * row + 4]
        outs_r.append(pr * ar - pi * ai + (qr * br - qi * bi))
        outs_i.append(pr * ai + pi * ar + (qr * bi + qi * br))
    return (
        jnp.stack(outs_r, 1).reshape(n, s, lanes),
        jnp.stack(outs_i, 1).reshape(n, s, lanes),
    )


def sublane_gate(xr, xi, bit, u):
    step = 1 << bit
    high = ((iota((SUBLANES, LANES), 0) >> bit) & 1) == 1

    def swap(x):
        down = pltpu.roll(x, step, 1)
        if 2 * step == SUBLANES:
            return down
        return jnp.where(high[None], down, pltpu.roll(x, SUBLANES - step, 1))

    keep_r = jnp.where(high, u[6], u[0])[None]
    keep_i = jnp.where(high, u[7], u[1])[None]
    cross_r = jnp.where(high, u[4], u[2])[None]
    cross_i = jnp.where(high, u[5], u[3])[None]
    yr, yi = swap(xr), swap(xi)
    return (
        keep_r * xr - keep_i * xi + (cross_r * yr - cross_i * yi),
        keep_r * xi + keep_i * xr + (cross_r * yi + cross_i * yr),
    )


def lane_matrix(units):
    shape = (LANES, LANES)
    row, col = iota(shape, 0), iota(shape, 1)
    mr = mi = None
    for bit, u in enumerate(units):
        rb, cb = ((row >> bit) & 1) == 1, ((col >> bit) & 1) == 1
        gr = jnp.where(cb, jnp.where(rb, u[6], u[4]), jnp.where(rb, u[2], u[0]))
        gi = jnp.where(cb, jnp.where(rb, u[7], u[5]), jnp.where(rb, u[3], u[1]))
        if mr is None:
            mr, mi = gr, gi
        else:
            mr, mi = mr * gr - mi * gi, mr * gi + mi * gr
    return mr, mi


def row_matrix(units):
    shape = (LANES, LANES)
    row, col = iota(shape, 0), iota(shape, 1)
    mr = mi = None
    for bit, u in enumerate(units):
        rb, cb = ((row >> bit) & 1) == 1, ((col >> bit) & 1) == 1
        gr = jnp.where(rb, jnp.where(cb, u[6], u[4]), jnp.where(cb, u[2], u[0]))
        gi = jnp.where(rb, jnp.where(cb, u[7], u[5]), jnp.where(cb, u[3], u[1]))
        if mr is None:
            mr, mi = gr, gi
        else:
            mr, mi = mr * gr - mi * gi, mr * gi + mi * gr
    return mr, mi


def cut(x, depth):
    rows = x.shape[0]
    x = x.reshape(rows // SUBLANES, SUBLANES, LANES)
    per = SUBLANES // depth
    if per == 1:
        return x
    parts = [x[:, k * depth : (k + 1) * depth] for k in range(per)]
    return jnp.stack(parts, 1).reshape(rows // depth, depth, LANES)


def join(x):
    n, depth, _ = x.shape
    per = SUBLANES // depth
    if per > 1:
        x = x.reshape(n // per, per, depth, LANES)
        x = jnp.concatenate([x[:, k] for k in range(per)], axis=1)
    return x.reshape(n * depth, LANES)


def halves(x):
    top = x.astype(bf16)
    return top, (x - top.astype(f32)).astype(bf16)


def marked(row, value, count):
    shape = (2 * SUBLANES, LANES)
    wide = jnp.broadcast_to(row.astype(f32), shape).astype(bf16)
    value = jnp.broadcast_to(value.astype(f32), shape).astype(bf16)
    ids = iota((count, LANES), 0).astype(f32).astype(bf16).reshape(count // 16, 16, LANES)
    return jnp.where(ids == wide[None], value[None], jnp.zeros((), bf16)).reshape(count, LANES)


def one_hot(row, count):
    wide = jnp.broadcast_to(row.astype(f32), (16, LANES)).astype(bf16)
    ids = iota((count, LANES), 0).astype(f32).astype(bf16).reshape(count // 16, 16, LANES)
    hot = jnp.where(ids == wide[None], jnp.ones((), bf16), jnp.zeros((), bf16))
    return hot.reshape(count, LANES)


def split_table(table):
    flipped = table.T
    top, rest = halves(flipped)
    return jnp.concatenate([top, rest], axis=0)


def pick_lane(value, lower):
    value = value.reshape(LANES // SUBLANES, SUBLANES, LANES)
    low = jnp.broadcast_to(lower, (SUBLANES, LANES))
    for bit in (6, 5, 4, 3):
        half = value.shape[0] // 2
        value = jnp.where((((low >> bit) & 1) == 1)[None], value[half:], value[:half])
    sub = iota((SUBLANES, LANES), 0)
    value = jnp.where(sub == (low & (SUBLANES - 1)), value[0], 0.0)
    return jnp.sum(value, axis=0, keepdims=True)


def rows_dot(table, upper):
    count = table.shape[1]
    hot = [one_hot(upper[r : r + 1], count) for r in range(upper.shape[0])]
    both = jnp.dot(table, jnp.concatenate(hot, axis=1), preferred_element_type=f32)
    return both[:LANES] + both[LANES:]


def lookup_lanes(plain, upper, lower):
    bits = plain.shape[0].bit_length() - 1
    high = [((upper >> bit) & 1) == 1 for bit in range(bits)]

    def pick(first, bit):
        if bit < 0:
            line = jnp.broadcast_to(plain[first : first + 1], (SUBLANES, LANES))
            return jnp.take_along_axis(line, lower, axis=1, mode="promise_in_bounds")
        zero = pick(first, bit - 1)
        return jnp.where(high[bit], pick(first + (1 << bit), bit - 1), zero)

    return pick(0, bits - 1)


def routes(me):
    parts = []
    rest = me
    for size in reversed(TORUS):
        parts.insert(0, lax.rem(rest, size))
        rest = rest // size
    scale = 1
    tables = []
    for part, size in zip(reversed(parts), reversed(TORUS)):
        tables.insert(0, [lax.rem(part + step, size) * scale for step in range(size)])
        scale *= size
    steps = [step for step in itertools.product(*[range(size) for size in TORUS]) if any(step)]
    random.Random(1).shuffle(steps)
    steps.sort(key=lambda step: -sum(min(d, n - d) for d, n in zip(step[:3], TORUS[:3])))
    upper = {(a, b): tables[0][a] + tables[1][b] for a in range(TORUS[0]) for b in range(TORUS[1])}
    lower = {(a, b): tables[2][a] + tables[3][b] for a in range(TORUS[2]) for b in range(TORUS[3])}
    return [upper[step[:2]] + lower[step[2:]] for step in steps]


def kernel(
    sizes,
    angles_hbm,
    marg_hbm,
    state_hbm,
    owner_hbm,
    low_hbm,
    probs_ref,
    hist_ref,
    fid_ref,
    amp_out,
    amp_in,
    wt_out,
    wt_in,
    req_out,
    req_in,
    ans_out,
    ans_in,
    his_out,
    his_in,
    tot_out,
    tot_in,
    code_ref,
    rank_ref,
    req_ref,
    table_ref,
    plain_ref,
    both_ref,
    side_ref,
    global_ref,
    gates,
    angles,
    marg,
    state,
    owner_ref,
    low_ref,
    sends,
    recvs,
    loads,
):
    devices, depth, capacity_rows, marg_count = sizes
    me = lax.axis_index("dev")
    global_bits = devices.bit_length() - 1
    rows = state.shape[0] // 2
    row_bits = rows.bit_length() - 1
    local_bits = row_bits + 7
    codes = devices * capacity_rows

    peers = routes(me)
    inputs = [
        pltpu.make_async_copy(src, dst, loads.at[n])
        for n, (src, dst) in enumerate(
            (
                (angles_hbm, angles),
                (state_hbm, state),
                (owner_hbm, owner_ref),
                (low_hbm, low_ref),
                (marg_hbm, marg),
            )
        )
    ]
    for load in inputs:
        load.start()

    def copy(channel, src, dst, target):
        return pltpu.make_async_remote_copy(
            src_ref=src,
            dst_ref=dst,
            send_sem=sends.at[channel],
            recv_sem=recvs.at[channel],
            device_id=(target,),
            device_id_type=pl.DeviceIdType.MESH,
        )

    def scatter(channel, out, into):
        for target in peers:
            copy(channel, out.at[target], into.at[me], target).start()
        into[me] = out[me]

    def spread(channel, out, into):
        for target in peers:
            copy(channel, out.at[0], into.at[me], target).start()
        into[me] = out[0]

    def all_of(channel, into):
        many = into.at[pl.ds(0, devices - 1)]
        return copy(channel, many, many, peers[-1])

    barrier = pltpu.get_barrier_semaphore()

    for target in peers:
        pl.semaphore_signal(
            barrier, inc=1, device_id=(target,), device_id_type=pl.DeviceIdType.MESH
        )

    inputs[0].wait()
    for e, entry in enumerate(gate_rows(angles, global_bits + local_bits)):
        gates[e] = entry

    def unit(qubit):
        return [gates[e, qubit : qubit + 1] for e in range(8)]

    mr, mi = lane_matrix([unit(q) for q in range(7)])
    mixed = jnp.concatenate(
        [jnp.concatenate([mr, mi], axis=1), jnp.concatenate([-mi, mr], axis=1)], axis=0
    )
    inputs[1].wait()
    both = jnp.concatenate(
        [state[pl.ds(0, rows, stride=2)], state[pl.ds(1, rows, stride=2)]], axis=1
    )
    both = jnp.dot(both, mixed, precision=lax.Precision.HIGHEST, preferred_element_type=f32)
    xr = both[:, :LANES].reshape(rows // SUBLANES, SUBLANES, LANES)
    xi = both[:, LANES:].reshape(rows // SUBLANES, SUBLANES, LANES)
    for bit in range(3):
        xr, xi = sublane_gate(xr, xi, bit, unit(7 + bit))
    for bit in range(row_bits - 3):
        xr, xi = leading_gate(xr, xi, bit, unit(10 + bit))
    amp_out[:, 0] = cut(xr.reshape(rows, LANES), depth)
    amp_out[:, 1] = cut(xi.reshape(rows, LANES), depth)

    mr, mi = row_matrix([unit(local_bits + q) for q in range(global_bits)])
    mixed = jnp.concatenate(
        [jnp.concatenate([mr, -mi], axis=1), jnp.concatenate([mi, mr], axis=1)], axis=0
    )
    global_ref[0], global_ref[1] = halves(mixed)
    pl.semaphore_wait(barrier, devices - 1)
    scatter(0, amp_out, amp_in)

    samp_rows = owner_ref.shape[0]
    for load in inputs[2:]:
        load.wait()
    owner = owner_ref[...]
    owner_ids = iota((devices, LANES), 0)
    chunks = samp_rows // 2
    pieces = [one_hot(owner[r : r + 1], devices) for r in range(samp_rows)]
    stacked = jnp.concatenate(
        [jnp.concatenate(pieces[2 * c : 2 * c + 2], axis=1) for c in range(chunks)], axis=0
    )
    tri_shape = (2 * LANES, 3 * LANES)
    tri_row, tri_col = iota(tri_shape, 0), iota(tri_shape, 1)
    tri = ((tri_row < tri_col) | (tri_col >= 2 * LANES)).astype(f32).astype(bf16)
    counts = jnp.dot(stacked, tri, preferred_element_type=f32)
    before = jnp.zeros((devices, LANES), f32)
    ranks = []
    for c in range(chunks):
        block = counts[c * devices : (c + 1) * devices]
        for h in range(2):
            spot = block[:, h * LANES : (h + 1) * LANES] + before
            mine = owner_ids == owner[2 * c + h : 2 * c + h + 1]
            ranks.append(jnp.sum(jnp.where(mine, spot, 0.0), axis=0, keepdims=True))
        before = before + block[:, 2 * LANES :]
    ranking = jnp.concatenate(ranks, axis=0).astype(i32)
    code = owner * capacity_rows + (ranking >> 7)
    rank = ranking & (LANES - 1)
    code_ref[...] = code
    rank_ref[...] = rank

    low = low_ref[...] + 1
    tops, rests = low >> 8, low & 255
    placed = jnp.zeros((codes, 2 * LANES), f32)
    for first in range(0, samp_rows, 16):
        line = [slice(r, r + 1) for r in range(first, first + 16)]
        hot = jnp.concatenate([one_hot(code[r], codes) for r in line], axis=1)
        values = [
            jnp.concatenate([marked(rank[r], part[r], LANES) for r in line], axis=1)
            for part in (tops, rests)
        ]
        placed = placed + lax.dot_general(
            hot,
            jnp.concatenate(values, axis=0),
            (((1,), (1,)), ((), ())),
            preferred_element_type=f32,
        )
    wanted = (placed[:, :LANES] * 256.0 + placed[:, LANES:]).astype(i32) - 1
    req_out[...] = cut(wanted, capacity_rows)
    scatter(5, req_out, req_in)

    all_of(0, amp_in).wait_recv()
    both = jnp.concatenate(
        [
            jnp.concatenate([amp_in[:, part, d] for d in range(depth)], axis=1)
            for part in range(2)
        ],
        axis=0,
    )
    top, rest = halves(both)
    both = jnp.dot(global_ref[0], top, preferred_element_type=f32) + (
        jnp.dot(global_ref[0], rest, preferred_element_type=f32)
        + jnp.dot(global_ref[1], top, preferred_element_type=f32)
    )
    xr, xi = both[:devices], both[devices:]
    weight = xr * xr + xi * xi
    weights = [weight[:, d * LANES : (d + 1) * LANES] for d in range(depth)]
    for d in range(depth):
        wt_out[:, d] = weights[d]
    scatter(1, wt_out, wt_in)

    weight = jnp.concatenate(weights, axis=0)
    norm_part = jnp.sum(weight, axis=0, keepdims=True)
    owner_bits = devices.bit_length() - 1
    code_shape = (rows, LANES)
    row_id = iota(code_shape, 0)
    row_value = (
        ((row_id & (devices - 1)) << local_bits)
        + me * (depth * LANES)
        + ((row_id >> owner_bits) << 7)
    )
    lane_value = iota((LANES, LANES), 0)
    row_code = jnp.zeros(code_shape, i32)
    lane_code = jnp.zeros((LANES, LANES), i32)
    lane_mask = jnp.zeros((), i32)
    for k in range(marg_count):
        qubit = marg[0, k]
        row_code = row_code + (((row_value >> qubit) & 1) << k)
        lane_code = lane_code + (((lane_value >> qubit) & 1) << k)
        lane_mask = lane_mask + jnp.where(qubit < 7, 1 << k, 0)
    bins = 2**marg_count
    top, rest = halves(weight)
    split = jnp.concatenate([top, rest], axis=0)
    @pl.loop(0, bins // LANES)
    def _(c):
        bin_id = c * LANES + iota((1, LANES), 1)
        lane_part = bin_id & lane_mask
        lane_hot = (lane_code == lane_part).astype(f32).astype(bf16)
        folded = jnp.dot(split, lane_hot, preferred_element_type=f32)
        folded = folded[:rows] + folded[rows:]
        picked = jnp.where(row_code == bin_id - lane_part, folded, 0.0)
        his_out[c] = jnp.sum(picked, axis=0, keepdims=True)

    bin_share = devices * LANES // bins
    for target in peers:
        copy(4, his_out.at[target // bin_share], his_in.at[me], target).start()
    his_in[me] = his_out[me // bin_share]

    all_of(5, req_in).wait_recv()
    req_ref[...] = join(req_in[...])
    all_of(1, wt_in).wait_recv()
    plain_ref[0:rows] = join(wt_in[...])
    table_ref[:, 0:rows] = split_table(plain_ref[0:rows])
    group = 32 // capacity_rows
    groups = devices // group
    mine, spot = me // group, me % group

    dots = 32 - 8

    def place_of(turn):
        first = lax.rem(mine + turn, groups) * group
        start = pl.multiple_of(first * capacity_rows, SUBLANES)
        return first, req_ref[pl.ds(start, group * capacity_rows)]

    def begin(turn, slot):
        _, wanted = place_of(turn)
        upper, lower = wanted >> 7, wanted & (LANES - 1)
        both_ref[slot] = rows_dot(table_ref[:, 0:rows], upper[:dots])
        for first in range(dots, 32, SUBLANES):
            part = slice(first, first + SUBLANES)
            value = lookup_lanes(plain_ref.at[0:rows], upper[part], lower[part])
            side_ref[slot, first - dots : first - dots + SUBLANES] = jnp.where(
                upper[part] >= 0, value, 0.0
            )

    def answer(turn, slot):
        first, wanted = place_of(turn)
        lower = wanted & (LANES - 1)
        found = [
            pick_lane(both_ref[slot, :, r * LANES : (r + 1) * LANES], lower[r : r + 1])
            for r in range(dots)
        ]
        found = jnp.concatenate([*found, side_ref[slot]], axis=0)
        ans_out[pl.ds(first, group)] = cut(found, capacity_rows)
        return first, jnp.sum(found, axis=0, keepdims=True)

    def reply(first, count):
        for j in range(1, count + 1):
            target = first + lax.rem(spot + j, group)
            copy(2, ans_out.at[target], ans_in.at[me], target).start()

    total = jnp.zeros((1, LANES), f32)
    turns = [*range(1, groups), 0]
    begin(turns[0], 0)
    for n, turn in enumerate(turns):
        if n + 1 < groups:
            begin(turns[n + 1], (n + 1) % 2)
        before, extra = answer(turn, n % 2)
        total = total + extra
        if n + 1 < groups:
            reply(before, group)
    reply(before, group - 1)
    half = iota((1, LANES), 1) < LANES // 2
    packed = [jnp.broadcast_to(x, (SUBLANES, LANES)) for x in (total, norm_part)]
    packed = [x + pltpu.roll(x, LANES // 2, 1) for x in packed]
    tot_out[0] = jnp.where(half, packed[0][0:1], packed[1][0:1])
    spread(3, tot_out, tot_in)
    ans_in[me] = ans_out[me]

    all_of(2, ans_in).wait_recv()
    plain_ref[0:codes] = join(ans_in[...])
    table_ref[:, 0:codes] = split_table(plain_ref[0:codes])
    def fetch(block, slot):
        window = slice(block * 32, (block + 1) * 32)
        upper, lower = code_ref[window], rank_ref[window]
        both_ref[slot] = rows_dot(table_ref[:, 0:codes], upper[:dots])
        side_ref[slot] = lookup_lanes(plain_ref.at[0:codes], upper[dots:], lower[dots:])

    def settle(block, slot):
        lower = rank_ref[block * 32 : (block + 1) * 32]
        found = [
            pick_lane(both_ref[slot, :, r * LANES : (r + 1) * LANES], lower[r : r + 1])
            for r in range(dots)
        ]
        probs_ref[block * 32 : (block + 1) * 32] = jnp.concatenate([*found, side_ref[slot]], axis=0)

    blocks = samp_rows // 32
    fetch(0, 0)
    for block in range(blocks):
        if block + 1 < blocks:
            fetch(block + 1, (block + 1) % 2)
        settle(block, block % 2)
    all_of(4, his_in).wait_recv()
    hist_ref[...] = jnp.sum(his_in[...], axis=0)
    all_of(3, tot_in).wait_recv()
    fid_ref[...] = jnp.sum(tot_in[...], axis=0)

    for channel, into in enumerate((amp_in, wt_in, ans_in, tot_in, his_in, req_in)):
        all_of(channel, into).wait_send()


def finish(sizes, values, hist, totals, probs_ref, mine_ref, fid_ref):
    amps_total, samples, bins = sizes
    mine = mine_ref.shape[1]
    start = lax.axis_index("dev") * mine
    line = totals[...]
    half = iota(line.shape, 1) < LANES // 2
    total = jnp.sum(jnp.where(half, line, 0.0), axis=1, keepdims=True)
    norm = jnp.sum(jnp.where(half, 0.0, line), axis=1, keepdims=True)
    probs_ref[...] = amps_total * (values[...] / norm)
    line = jnp.broadcast_to(hist[0:1], (SUBLANES, LANES))
    line = pltpu.roll(line, (LANES - start % LANES) % LANES, 1)
    mine_ref[...] = bins * (line[0:1, :mine] / norm)
    fid_ref[...] = amps_total * (total / norm) / samples - 1.0


def shards(state, angles, sample_high, sample_low, marginal_qubits):
    devices = lax.axis_size("dev")
    amps_local = state.shape[1]
    samp_local = sample_low.shape[0]
    marg_count = marginal_qubits.shape[0]
    bins = 2**marg_count
    depth = amps_local // devices // LANES
    capacity_rows = 4 * samp_local // devices // LANES
    rows = amps_local // LANES
    samp_rows = samp_local // LANES
    sizes = (
        devices,
        depth,
        capacity_rows,
        marg_count,
    )
    vmem = pl.BlockSpec(memory_space=pltpu.VMEM)
    codes = devices * capacity_rows
    bin_rows = bins // LANES
    values, hist, totals = pl.pallas_call(
        functools.partial(kernel, sizes),
        out_shape=(
            jax.ShapeDtypeStruct((samp_rows, LANES), f32),
            jax.ShapeDtypeStruct((1, LANES), f32),
            jax.ShapeDtypeStruct((1, LANES), f32),
        ),
        in_specs=[pl.BlockSpec(memory_space=pltpu.HBM)] * 5,
        out_specs=(vmem, vmem, vmem),
        scratch_shapes=[
            pltpu.VMEM((devices, 2, depth, LANES), f32),
            pltpu.VMEM((devices, 2, depth, LANES), f32),
            pltpu.VMEM((devices, depth, LANES), f32),
            pltpu.VMEM((devices, depth, LANES), f32),
            pltpu.VMEM((devices, capacity_rows, LANES), i32),
            pltpu.VMEM((devices, capacity_rows, LANES), i32),
            pltpu.VMEM((devices, capacity_rows, LANES), f32),
            pltpu.VMEM((devices, capacity_rows, LANES), f32),
            pltpu.VMEM((bin_rows, 1, LANES), f32),
            pltpu.VMEM((devices, 1, LANES), f32),
            pltpu.VMEM((1, 1, LANES), f32),
            pltpu.VMEM((devices, 1, LANES), f32),
            pltpu.VMEM((samp_rows, LANES), i32),
            pltpu.VMEM((samp_rows, LANES), i32),
            pltpu.VMEM((codes, LANES), i32),
            pltpu.VMEM((2 * LANES, max(rows, codes)), bf16),
            pltpu.VMEM((max(rows, codes), LANES), f32),
            pltpu.VMEM((2, LANES, (32 - 8) * LANES), f32),
            pltpu.VMEM((2, 8, LANES), f32),
            pltpu.VMEM((2, 2 * devices, 2 * devices), bf16),
            pltpu.VMEM((8, -(-angles.shape[0] // SUBLANES) * SUBLANES, LANES), f32),
            pltpu.SMEM((angles.shape[1], angles.shape[0]), f32),
            pltpu.SMEM((1, marg_count), i32),
            pltpu.VMEM((2 * rows, LANES), f32),
            pltpu.VMEM((samp_rows, LANES), i32),
            pltpu.VMEM((samp_rows, LANES), i32),
            pltpu.SemaphoreType.DMA((6,)),
            pltpu.SemaphoreType.DMA((6,)),
            pltpu.SemaphoreType.DMA((5,)),
        ],
        compiler_params=pltpu.CompilerParams(
            collective_id=0, has_side_effects=True, vmem_limit_bytes=24 << 20
        ),
        name="circuit",
    )(
        pltpu.with_memory_space_constraint(angles.T, pltpu.HBM),
        pltpu.with_memory_space_constraint(marginal_qubits.reshape(1, marg_count), pltpu.HBM),
        pltpu.with_memory_space_constraint(state.reshape(2, rows, LANES).transpose(1, 0, 2).reshape(2 * rows, LANES), pltpu.HBM),
        pltpu.with_memory_space_constraint(sample_high.reshape(samp_rows, LANES), pltpu.HBM),
        pltpu.with_memory_space_constraint(sample_low.reshape(samp_rows, LANES), pltpu.HBM),
    )
    probs, mine, fid = pl.pallas_call(
        functools.partial(
            finish, (float(amps_local * devices), float(samp_local * devices), float(bins))
        ),
        out_shape=(
            jax.ShapeDtypeStruct((samp_rows, LANES), f32),
            jax.ShapeDtypeStruct((1, bins // devices), f32),
            jax.ShapeDtypeStruct((1, 1), f32),
        ),
        in_specs=[vmem, vmem, vmem],
        out_specs=(vmem, vmem, vmem),
        compiler_params=pltpu.CompilerParams(vmem_limit_bytes=1 << 20),
        name="finish",
    )(values, hist, totals)
    return probs.reshape(samp_local), mine.reshape(bins // devices), fid.reshape(())


def solution(mesh):
    return jax.shard_map(
        shards,
        mesh=mesh,
        in_specs=(P(None, "dev"), P(), P("dev", None), P("dev"), P()),
        out_specs=(P("dev"), P("dev"), P()),
        check_vma=False,
    )
```
